32 devices in a mesh: row: 4 (over x, core), col: 8 (over z, y).
Axes of the slice: x: 2, y: 2, z: 4, core: 2. Of those that a mesh axis runs over, the one named last changes fastest.
Arguments:
- voltage: float32 [512, 2048], P('row', 'col'), may hold values from -6 to 6
- currents: float32 [2, 512, 2048], P(None, 'row', 'col'), may hold values from -6 to 6
- resistance: float32 [2, 512, 2048], P(None, 'row', 'col'), may hold values from 0.05 to 0.5
- inverse_cap: float32 [512, 2048], P('row', 'col'), may hold values from 0.05 to 0.5
- shunt_conductance: float32 [512, 2048], P('row', 'col'), may hold values from 0.1 to 1
- tap_index: int32 [512, 2048], P('row', 'col'), may hold values from 0 to 8
- pad_mask: int32 [512, 2048], P('row', 'col'), may hold values 0 or 1
- waveforms: float32 [2, 8], replicated, may hold values from -8 to 8
- k_window: bfloat16 [2, 33, 33], replicated, may hold values from -0.1 to 0.4
Outputs:
- voltage_out: float32 [512, 2048], P('row', 'col')
- current_out: float32 [2, 512, 2048], P(None, 'row', 'col')
The draws below stay inside these ranges and needn't reach their ends.
All inputs are finite; a program needn't handle non-finite values. No bound on the sum of `pad_mask` on one device may be relied on, other than what follows from the above.
Results may differ from the reference program's by a relative error of at most 0.0023.
Values may be sent and summed in bfloat16 or wider, within the bound.
No kernel may reach another device: no remote copies, remote signals or barrier semaphores. Data moves between devices by JAX's collectives and lax.ppermute only.
A program may use at most 64 MiB of HBM per device.

```python
import math
import jax
import jax.numpy as jnp
from jax import lax

CY = 256
HALF = 16
STEPS = 2
NW = 8
NX = 512
NY = 2048


def draw_k_window(key, part):
    window_span = 2 * HALF + 1
    noise = jax.random.normal(key, (2, window_span, window_span), jnp.float32) * 0.012
    noise = jnp.clip(noise, -0.09, 0.09)
    center = jnp.zeros((2, window_span, window_span), jnp.float32).at[:, HALF, HALF].set(0.3)
    return (noise + center).astype(jnp.bfloat16)


def with_ends(values, key, least, top_value):
    spot = [jax.random.randint(jax.random.fold_in(key, axis), (), 0, length) for axis, length in enumerate(values.shape)]
    main_axis = values.shape.index(max(values.shape))
    neighbour = spot[:main_axis] + [(spot[main_axis] + 1) % values.shape[main_axis]] + spot[main_axis + 1:]
    return values.at[tuple(spot)].set(least).at[tuple(neighbour)].set(top_value)


def block_scale(own_key, shape, cuts, low, high):
    loudness, own = 1.0, jax.random.fold_in(own_key, 6)
    for position, parts in cuts:
        draws = jnp.exp(jax.random.uniform(jax.random.fold_in(own, position), (parts,), jnp.float32, low / len(cuts), high / len(cuts)))
        loudness = loudness * jnp.repeat(draws, shape[position] // parts).reshape([-1 if axis == position else 1 for axis in range(len(shape))])
    return loudness


def bell_draw(rng, shape, scale, reach, split=(), held_as=jnp.bfloat16):
    drawn = scale * jax.random.normal(rng, shape, jnp.float32)
    if split:
        drawn = drawn * block_scale(rng, shape, split, -0.22, 0.18)
    return jnp.clip(drawn, -reach, reach).astype(held_as)


def setup_inputs(seed: int = 0) -> dict:
    arg_keys = jax.random.split(jax.random.key(seed), 10)
    return {
        "voltage": bell_draw(arg_keys[0], (NX, NY), 1.0, 6.0, ((0, 4), (1, 8)), jnp.float32),
        "currents": bell_draw(arg_keys[1], (2, NX, NY), 1.0, 6.0, ((1, 4), (2, 8)), jnp.float32),
        "resistance": jnp.clip(jnp.exp(math.log(0.5) - 2.3025851 * jax.random.uniform(arg_keys[2], (2, NX, NY), jnp.float32) ** block_scale(arg_keys[2], (2, NX, NY), ((1, 4), (2, 8)), -0.2, 0.2)), 0.05, 0.5),
        "inverse_cap": jnp.clip(jnp.exp(math.log(0.5) - 2.3025851 * jax.random.uniform(arg_keys[3], (NX, NY), jnp.float32) ** block_scale(arg_keys[3], (NX, NY), ((0, 4), (1, 8)), -0.2, 0.2)), 0.05, 0.5),
        "shunt_conductance": jnp.clip(jnp.exp(math.log(1.0) - 2.3025851 * jax.random.uniform(arg_keys[4], (NX, NY), jnp.float32) ** block_scale(arg_keys[4], (NX, NY), ((0, 4), (1, 8)), -0.2, 0.2)), 0.1, 1.0),
        "tap_index": with_ends(jax.random.randint(arg_keys[5], (NX, NY), 0, NW + 1), jax.random.fold_in(arg_keys[5], 1), 0, NW).astype(jnp.int32),
        "pad_mask": with_ends((jax.random.randint(arg_keys[6], (NX, NY), 0, 16) < 1).astype(jnp.int32), jax.random.fold_in(arg_keys[6], 1), 0, 1),
        "waveforms": bell_draw(arg_keys[7], (STEPS, NW), 2.0, 8.0, (), jnp.float32),
        "k_window": draw_k_window(jax.random.fold_in(arg_keys[9], 71), 0),
    }


def toeplitz_rows(kernel_row, width_in, width_out):
    window_span = kernel_row.shape[1]
    in_index = jnp.arange(width_in, dtype=jnp.int32)[:, None]
    out_index = jnp.arange(width_out, dtype=jnp.int32)[None, :]
    offsets_col = in_index - out_index
    inside = (offsets_col >= 0) & (offsets_col < window_span)
    entries = jnp.take(kernel_row, jnp.clip(offsets_col, 0, window_span - 1), axis=1)
    return jnp.where(inside[None], entries, jnp.zeros_like(entries))


def window_apply(padded, kernel, row_count, col_count):
    window_span = kernel.shape[1]

    def accumulate(offset, running):
        row_slab = lax.dynamic_slice_in_dim(padded, offset, row_count, 1)
        kernel_row = lax.dynamic_index_in_dim(kernel, offset, 1, keepdims=False)
        matrix = toeplitz_rows(kernel_row, col_count + window_span - 1, col_count)
        return running + jnp.einsum("crj,cjk->crk", row_slab, matrix, preferred_element_type=jnp.float32)

    start = jnp.zeros((2, row_count, col_count), jnp.float32)
    return lax.fori_loop(0, window_span, accumulate, start)


def loads_of(tap_index, wave_row):
    running = jnp.zeros(tap_index.shape, jnp.float32)
    for which in range(NW):
        running = running + jnp.where(tap_index == which, wave_row[which], jnp.float32(0.0))
    return running


def reference(voltage, currents, resistance, inverse_cap, shunt_conductance, tap_index, pad_mask, waveforms, k_window):
    blocks = NY // CY
    for step_index in range(STEPS):
        shifted = jnp.pad(voltage, ((0, 1), (0, 1)))
        drop_pair = jnp.stack([voltage - shifted[1:, :-1], voltage - shifted[:-1, 1:]])
        driving = (drop_pair - resistance * currents).astype(jnp.bfloat16)
        padded = jnp.pad(driving, ((0, 0), (HALF, HALF), (HALF, HALF)))

        def one_block(block):
            col_slab = lax.dynamic_slice(padded, (jnp.int32(0), jnp.int32(0), block * CY), (2, NX + 2 * HALF, CY + 2 * HALF))
            return window_apply(col_slab, k_window, NX, CY)

        pieces = lax.map(one_block, jnp.arange(blocks, dtype=jnp.int32))
        update = jnp.transpose(pieces, (1, 2, 0, 3)).reshape(2, NX, NY)
        currents = currents + update
        before_x = jnp.pad(currents[0], ((1, 0), (0, 0)))[:-1]
        before_y = jnp.pad(currents[1], ((0, 0), (1, 0)))[:, :-1]
        divergence = currents[0] - before_x + currents[1] - before_y
        load = loads_of(tap_index, waveforms[step_index])
        voltage = voltage + inverse_cap * (load - divergence - shunt_conductance * voltage)
        voltage = jnp.where(pad_mask == 1, jnp.float32(0.0), voltage)
    return voltage, currents
```

```python
import functools

import jax
import jax.numpy as jnp
from jax import lax
from jax.experimental import pallas as pl
from jax.experimental.pallas import tpu as pltpu
from jax.sharding import PartitionSpec as P

F32 = jnp.float32
BF16 = jnp.bfloat16
LANES = 128
TILE = 16
VMEM = pl.BlockSpec(memory_space=pltpu.VMEM)
SMEM = pl.BlockSpec(memory_space=pltpu.SMEM)


class Sizes:
    def __init__(self, rows, cols, span, waves):
        self.rows, self.cols, self.span, self.waves = rows, cols, span, waves
        self.half = (span - 1) // 2
        self.far = 2 * self.half + 2
        self.near = self.half + 2
        self.lanes = cols + LANES
        self.frame = rows + 5 * TILE
        self.pairs = (span + 1) // 2
        self.up_d = 3 * TILE
        self.up_f = 2 * TILE
        self.payload = 2 * self.up_d + 6 * self.up_f + TILE
        far, near = self.far, self.near
        self.slots = (
            ((far, 0), (far, far), (near, 2 * far), (near, 2 * far + near)),
            ((near, 0), (near, near), (near, 2 * near), (near, 3 * near), (far, 4 * near)),
        )


def lane_of(shape):
    return lax.broadcasted_iota(jnp.int32, shape, len(shape) - 1)


def row_of(shape):
    return lax.broadcasted_iota(jnp.int32, shape, 0)


def tables_kernel(k_ref, t_ref, pad_ref, *, s):
    zero = jnp.zeros((LANES, LANES), F32)
    for c in range(2):
        pad_ref[...] = zero
        pad_ref[0 : s.span, 0 : s.span] = k_ref[c].astype(F32)
        turned = pad_ref[...].T
        for b in range(2 * s.pairs):
            p, q = divmod(b, 2)
            row = jnp.broadcast_to(turned[b : b + 1, :], (96, LANES))
            band = pltpu.roll(row, 0, 1, stride=1, stride_axis=0)
            t_ref[c, p, :, q * LANES : (q + 1) * LANES] = band.astype(BF16)


def first_kernel(v_ref, i_ref, r_ref, cap_ref, shunt_ref, tap_ref, pad_ref, wave_ref,
                 d_ref, a_ref, b_ref, c_ref, e_ref, one_ref, two_ref, *, s):
    even = lax.rem(lax.axis_index("col"), 2) == 0
    volt = v_ref[...]
    cap, shunt, tap = cap_ref[...], shunt_ref[...], tap_ref[...]
    keep = pad_ref[...] != 1
    loads = []
    for step in range(2):
        total = jnp.zeros(volt.shape, F32)
        for n in range(s.waves):
            total = jnp.where(tap == n, wave_ref[step, n], total)
        loads.append(total)
    b = jnp.where(keep, cap, 0.0)
    c = jnp.where(keep, 1.0, 0.0) - b * shunt
    a = c * volt + b * loads[0]
    a_ref[...], b_ref[...], c_ref[...], e_ref[...] = a, b, c, b * loads[1]
    rows, cols = volt.shape
    below = jnp.where(row_of(volt.shape) == rows - 1, 0.0, pltpu.roll(volt, rows - 1, 0))
    beside = jnp.where(lane_of(volt.shape) == cols - 1, 0.0, pltpu.roll(volt, cols - 1, 1))
    d0 = ((volt - below) - r_ref[0] * i_ref[0]).astype(BF16)
    d1 = ((volt - beside) - r_ref[1] * i_ref[1]).astype(BF16)
    d_ref[0], d_ref[1] = d0, d1
    groups = ((d0.astype(F32), d1.astype(F32), i_ref[0], i_ref[1]), (r_ref[0], r_ref[1], a, b, volt))
    lane = lane_of((rows, LANES))
    for tile, (slots, fields) in enumerate(zip(s.slots, groups)):
        left = jnp.zeros((rows, LANES), F32)
        right = jnp.zeros((rows, LANES), F32)
        for (n, off), field in zip(slots, fields):
            x = jnp.where(lane < n, field[:, :LANES], 0.0)
            y = jnp.where(lane >= LANES - n, field[:, cols - LANES :], 0.0)
            left = left + (pltpu.roll(x, off, 1) if off else x)
            right = right + (pltpu.roll(y, LANES - off, 1) if off else y)
        at = slice(tile * LANES, (tile + 1) * LANES)
        one_ref[:, at] = jnp.where(even, right, left).astype(BF16)
        two_ref[:, at] = jnp.where(even, left, right).astype(BF16)


def second_kernel(d_ref, v_ref, i_ref, r_ref, a_ref, b_ref, one_ref, two_ref,
                  df_ref, t_ref, up_ref, down_ref, *, s):
    even = lax.rem(lax.axis_index("col"), 2) == 0
    rows, cols = v_ref.shape
    lane = lane_of((rows, LANES))
    sides = []
    for tile, slots in enumerate(s.slots):
        at = slice(tile * LANES, (tile + 1) * LANES)
        one, two = one_ref[:, at].astype(F32), two_ref[:, at].astype(F32)
        from_right = jnp.where(even, one, two)
        from_left = jnp.where(even, two, one)
        for n, off in slots:
            x = pltpu.roll(from_right, LANES - off, 1) if off else from_right
            y = pltpu.roll(from_left, off, 1) if off else from_left
            sides.append(jnp.where(lane < n, x, jnp.where(lane >= LANES - n, y, 0.0)))
    d0s, d1s, i0s, i1s, r0s, r1s, as_, bs, vs = sides
    edge = lane == LANES - 1
    next_side = pltpu.roll(vs, LANES - 1, 1)
    next_own = pltpu.roll(v_ref[:, :LANES], LANES - 1, 1)
    d1 = d_ref[1]
    tail = d1[:, cols - LANES :].astype(F32)
    tail = jnp.where(edge, tail - next_side, tail).astype(BF16)
    d1s = jnp.where(edge, jnp.where(r1s > 0, d1s - next_own, 0.0), d1s).astype(BF16)
    df_ref[0, :, :cols] = d_ref[0]
    df_ref[0, :, cols:] = d0s.astype(BF16)
    df_ref[1, :, : cols - LANES] = d1[:, : cols - LANES]
    df_ref[1, :, cols - LANES : cols] = tail
    df_ref[1, :, cols:] = d1s
    for n, x in enumerate((i0s, i1s, r0s, r1s, as_, bs, vs)):
        t_ref[n] = x.astype(BF16)
    for ref, dstart, fstart in ((up_ref, 0, 0), (down_ref, rows - s.up_d, rows - s.up_f)):
        at = 0
        for c in range(2):
            ref[at : at + s.up_d, :] = df_ref[c, dstart : dstart + s.up_d, :]
            at += s.up_d
        own = (i_ref.at[0], i_ref.at[1], r_ref.at[0], r_ref.at[1], a_ref, b_ref)
        for n, field in enumerate(own):
            ref[at : at + s.up_f, :cols] = field[fstart : fstart + s.up_f, :].astype(BF16)
            ref[at : at + s.up_f, cols:] = t_ref[n, fstart : fstart + s.up_f, :]
            at += s.up_f
        ref[at : at + TILE, :cols] = v_ref[0:TILE, :].astype(BF16)
        ref[at : at + TILE, cols:] = t_ref[6, 0:TILE, :]


def convolve(d_ref, t_ref, c, s, strips):
    tiles = s.frame // TILE
    lanes = s.lanes
    first = [t % tiles for t in range(-3, 5)]
    second = list(range(3, 11))
    acc = [jnp.zeros((96, 2 * LANES), F32) for _ in range(3 if strips else 2)]
    for p in range(s.pairs):
        rhs1, rhs2, rhs3 = [], [], []
        for b in (2 * p, 2 * p + 1):
            shift = (s.half - b) % lanes
            x = d_ref[c]
            x = pltpu.roll(x, shift, 1) if shift else x
            rhs1 += [x[t * TILE : (t + 1) * TILE, : s.cols] for t in first]
            rhs2 += [x[t * TILE : (t + 1) * TILE, : s.cols] for t in second]
            rhs3 += [jnp.concatenate([x[t * TILE : (t + 1) * TILE, s.cols :], x[u * TILE : (u + 1) * TILE, s.cols :]], 1)
                     for t, u in zip(first, second)]
        lhs = t_ref[c, p]
        for n, rhs in enumerate((rhs1, rhs2, rhs3)[: len(acc)]):
            acc[n] = acc[n] + jnp.dot(lhs, jnp.concatenate(rhs, 0), preferred_element_type=F32)
    return acc


def last_kernel(df_ref, v_ref, i_ref, r_ref, a_ref, b_ref, c_ref, e_ref, side_ref, tab_ref, one_ref, two_ref,
                vo_ref, io_ref, d_ref, if_ref, rf_ref, af_ref, bf_ref, vf_ref, *, s):
    even = lax.rem(lax.axis_index("row"), 2) == 0
    rows, cols, frame, lanes = s.rows, s.cols, s.frame, s.lanes
    low = jnp.where(even, one_ref[...], two_ref[...])
    high = jnp.where(even, two_ref[...], one_ref[...])
    ud, uf = s.up_d, s.up_f
    own = (i_ref.at[0], i_ref.at[1], r_ref.at[0], r_ref.at[1], a_ref, b_ref)
    frames = (if_ref.at[0], if_ref.at[1], rf_ref.at[0], rf_ref.at[1], af_ref, bf_ref)
    for n, (src, dst) in enumerate(zip(own, frames)):
        at = 2 * ud + n * uf
        dst[0:rows, :cols] = src[...]
        dst[0:rows, cols:] = side_ref[n].astype(F32)
        dst[rows : rows + uf, :] = low[at : at + uf, :].astype(F32)
        dst[rows + uf : frame - uf, :] = jnp.zeros((frame - rows - 2 * uf, lanes), F32)
        dst[frame - uf : frame, :] = high[at : at + uf, :].astype(F32)
    at = 2 * ud + 6 * uf
    v_next = low[at : at + TILE, :].astype(F32)[0:1, :]
    v_first = jnp.concatenate([v_ref[0:8, :][0:1, :], side_ref[6, 0:TILE, :].astype(F32)[0:1, :]], 1)
    gap = rows + 2 * TILE
    shape = (TILE, lanes)
    for c in range(2):
        d_ref[c, 0:rows, :] = df_ref[c]
        d_ref[c, rows:gap, :] = low[c * ud : c * ud + 2 * TILE, :]
        d_ref[c, gap + TILE :, :] = high[c * ud + TILE : (c + 1) * ud, :]
        d_ref[c, gap : gap + TILE, :] = jnp.where(
            row_of(shape) < TILE // 2,
            low[c * ud + 2 * TILE : (c + 1) * ud, :].astype(F32),
            high[c * ud : c * ud + TILE, :].astype(F32)).astype(BF16)
    last = row_of(shape) == TILE - 1
    x = d_ref[0, rows - TILE : rows, :].astype(F32)
    d_ref[0, rows - TILE : rows, :] = jnp.where(last, x - v_next, x).astype(BF16)
    x = d_ref[0, frame - TILE :, :].astype(F32)
    inside = rf_ref[0, frame - TILE :, :] > 0
    d_ref[0, frame - TILE :, :] = jnp.where(last, jnp.where(inside, x - v_first, 0.0), x).astype(BF16)

    for c in range(2):
        one, two, side = convolve(d_ref, tab_ref, c, s, True)
        for dst0, src0, n in ((0, 32, 64), (frame - 32, 0, 32)):
            old = if_ref[c, dst0 : dst0 + n, :]
            add = jnp.concatenate([one[src0 : src0 + n], side[src0 : src0 + n, :LANES]], 1)
            if_ref[c, dst0 : dst0 + n, :] = jnp.where(rf_ref[c, dst0 : dst0 + n, :] > 0, old + add, 0.0)
        old = if_ref[c, 64 : 64 + 96, :]
        add = jnp.concatenate([two, side[:, LANES:]], 1)
        if_ref[c, 64 : 64 + 96, :] = jnp.where(rf_ref[c, 64 : 64 + 96, :] > 0, old + add, 0.0)
    i0, i1 = if_ref[0], if_ref[1]
    div = i0 - pltpu.roll(i0, 1, 0) + i1 - pltpu.roll(i1, 1, 1)
    volt = af_ref[...] - bf_ref[...] * div
    vf_ref[...] = volt
    drop0 = volt - pltpu.roll(volt, frame - 1, 0)
    drop1 = volt - pltpu.roll(volt, lanes - 1, 1)
    r0, r1 = rf_ref[0], rf_ref[1]
    d_ref[0] = jnp.where(r0 > 0, drop0 - r0 * i0, 0.0).astype(BF16)
    d_ref[1] = jnp.where(r1 > 0, drop1 - r1 * i1, 0.0).astype(BF16)

    one, two = convolve(d_ref, tab_ref, 0, s, False)
    above = (if_ref[0, frame - 8 :, :cols] + one[24:32])[7:8]
    above = jnp.where(rf_ref[0, frame - 8 :, :cols][7:8] > 0, above, 0.0)
    io_ref[0, 0:64, :] = if_ref[0, 0:64, :cols] + one[32:]
    io_ref[0, 64:128, :] = if_ref[0, 64:128, :cols] + two[:64]
    one, two, side = convolve(d_ref, tab_ref, 1, s, True)
    io_ref[1, 0:64, :] = if_ref[1, 0:64, :cols] + one[32:]
    io_ref[1, 64:128, :] = if_ref[1, 64:128, :cols] + two[:64]
    side = jnp.concatenate([side[32:, :LANES], side[:64, LANES:]], 0)
    side = jnp.where(rf_ref[1, 0:rows, cols:] > 0, if_ref[1, 0:rows, cols:] + side, 0.0)
    i0, i1 = io_ref[0], io_ref[1]
    up = jnp.where(row_of((rows, cols)) == 0, above, pltpu.roll(i0, 1, 0))
    left = pltpu.roll(jnp.concatenate([i1, side], 1), 1, 1)[:, :cols]
    div = i0 - up + i1 - left
    vo_ref[...] = c_ref[...] * vf_ref[0:rows, :cols] + e_ref[...] - b_ref[...] * div


def swap(x, axis, odd):
    n = lax.axis_size(axis)
    pairs = []
    for i in range(odd, n - 1, 2):
        pairs += [(i, i + 1), (i + 1, i)]
    return lax.ppermute(x, axis, pairs)


def call(kernel, outs, ins, scratch=(), specs=None):
    return pl.pallas_call(
        kernel,
        out_shape=outs,
        in_specs=specs or [VMEM] * len(ins),
        out_specs=jax.tree.map(lambda _: VMEM, outs),
        scratch_shapes=scratch,
    )(*ins)


def local(voltage, currents, resistance, inverse_cap, shunt, tap, pad, waveforms, k_window):
    rows, cols = voltage.shape
    s = Sizes(rows, cols, k_window.shape[1], waveforms.shape[1])
    sds = jax.ShapeDtypeStruct
    block = sds((rows, cols), F32)
    half = sds((rows, 2 * LANES), BF16)
    d, a, b, c, e, one, two = call(
        functools.partial(first_kernel, s=s),
        (sds((2, rows, cols), BF16), block, block, block, block, half, half),
        (voltage, currents, resistance, inverse_cap, shunt, tap, pad, waveforms),
        specs=[VMEM] * 7 + [SMEM])
    tables = call(
        functools.partial(tables_kernel, s=s),
        sds((2, s.pairs, 96, 2 * LANES), BF16), (k_window,),
        scratch=[pltpu.VMEM((LANES, LANES), F32)])
    one, two = swap(one, "col", 0), swap(two, "col", 1)
    pay = sds((s.payload, s.lanes), BF16)
    df, side, up, down = call(
        functools.partial(second_kernel, s=s),
        (sds((2, rows, s.lanes), BF16), sds((7, rows, LANES), BF16), pay, pay),
        (d, voltage, currents, resistance, a, b, one, two))
    even = lax.rem(lax.axis_index("row"), 2) == 0
    one, two = jnp.where(even, down, up), jnp.where(even, up, down)
    one, two = swap(one, "row", 0), swap(two, "row", 1)
    f = pltpu.VMEM((s.frame, s.lanes), F32)
    f2 = pltpu.VMEM((2, s.frame, s.lanes), F32)
    return call(
        functools.partial(last_kernel, s=s),
        (block, sds((2, rows, cols), F32)),
        (df, voltage, currents, resistance, a, b, c, e, side, tables, one, two),
        scratch=[pltpu.VMEM((2, s.frame, s.lanes), BF16), f2, f2, f, f, f])


def solution(mesh):
    grid = P("row", "col")
    pair = P(None, "row", "col")
    return jax.shard_map(
        local,
        mesh=mesh,
        in_specs=(grid, pair, pair, grid, grid, grid, grid, P(), P()),
        out_specs=(grid, pair),
        check_vma=False,
    )
```

```python
import functools

import jax
import jax.numpy as jnp
from jax import lax
from jax.experimental import pallas as pl
from jax.experimental.pallas import tpu as pltpu
from jax.sharding import PartitionSpec as P

F32 = jnp.float32
BF16 = jnp.bfloat16
LANES = 128
TILE = 16
VMEM = pl.BlockSpec(memory_space=pltpu.VMEM)
FAR = pl.BlockSpec(memory_space=pltpu.HBM)


class Sizes:
    def __init__(self, rows, cols, span, waves):
        self.rows, self.cols, self.span, self.waves = rows, cols, span, waves
        self.half = (span - 1) // 2
        self.far = 2 * self.half + 2
        self.near = self.half + 2
        self.lanes = cols + LANES
        self.frame = rows + 5 * TILE
        self.pairs = (span + 1) // 2
        self.up_d = 3 * TILE
        self.up_f = 2 * TILE
        self.payload = 2 * self.up_d + 6 * self.up_f + TILE
        far, near = self.far, self.near
        self.slots = (
            ((far, 0), (far, far), (near, 2 * far), (near, 2 * far + near)),
            ((near, 0), (near, near), (near, 2 * near), (near, 3 * near), (far, 4 * near)),
        )


def lane_of(shape):
    return lax.broadcasted_iota(jnp.int32, shape, len(shape) - 1)


def row_of(shape):
    return lax.broadcasted_iota(jnp.int32, shape, 0)


def tables_kernel(k_ref, t_ref, pad_ref, *, s):
    zero = jnp.zeros((LANES, LANES), F32)
    for c in range(2):
        pad_ref[...] = zero
        pad_ref[0 : s.span, 0 : s.span] = k_ref[:, c, :].astype(F32)
        turned = pad_ref[...].T
        for b in range(2 * s.pairs):
            p, q = divmod(b, 2)
            row = jnp.broadcast_to(turned[b : b + 1, :], (96, LANES))
            band = pltpu.roll(row, 0, 1, stride=1, stride_axis=0)
            t_ref[c, p, :, q * LANES : (q + 1) * LANES] = band.astype(BF16)


def first_kernel(v_hbm, i_hbm, r_hbm, cap_hbm, shunt_hbm, tap_hbm, pad_hbm, wave_hbm, k_hbm,
                 d_ref, a_ref, b_ref, c_ref, e_ref, one_ref, two_ref, v_ref, i_ref, r_ref, k_ref,
                 cap_ref, shunt_ref, tap_ref, pad_ref, wave_ref, sems, *, s):
    sources = (wave_hbm, tap_hbm, pad_hbm, cap_hbm, shunt_hbm, v_hbm, i_hbm, r_hbm, k_hbm)
    targets = (wave_ref, tap_ref, pad_ref, cap_ref, shunt_ref, v_ref, i_ref, r_ref, k_ref)
    copies = [pltpu.make_async_copy(x, y, sems.at[n]) for n, (x, y) in enumerate(zip(sources, targets))]
    for copy in copies:
        copy.start()
    for copy in copies:
        copy.wait()
    even = lax.rem(lax.axis_index("col"), 2) == 0
    volt = v_ref[...]
    cap, shunt, tap = cap_ref[...], shunt_ref[...], tap_ref[...]
    keep = pad_ref[...] != 1
    loads = []
    for step in range(2):
        total = jnp.zeros(volt.shape, F32)
        for n in range(s.waves):
            total = jnp.where(tap == n, wave_ref[step, n], total)
        loads.append(total)
    b = jnp.where(keep, cap, 0.0)
    c = jnp.where(keep, 1.0, 0.0) - b * shunt
    a = c * volt + b * loads[0]
    a_ref[...], b_ref[...], c_ref[...], e_ref[...] = a, b, c, b * loads[1]
    rows, cols = volt.shape
    below = jnp.where(row_of(volt.shape) == rows - 1, 0.0, pltpu.roll(volt, rows - 1, 0))
    beside = jnp.where(lane_of(volt.shape) == cols - 1, 0.0, pltpu.roll(volt, cols - 1, 1))
    d0 = ((volt - below) - r_ref[0] * i_ref[0]).astype(BF16)
    d1 = ((volt - beside) - r_ref[1] * i_ref[1]).astype(BF16)
    d_ref[0], d_ref[1] = d0, d1
    groups = ((d0.astype(F32), d1.astype(F32), i_ref[0], i_ref[1]), (r_ref[0], r_ref[1], a, b, volt))
    lane = lane_of((rows, LANES))
    for tile, (slots, fields) in enumerate(zip(s.slots, groups)):
        left = jnp.zeros((rows, LANES), F32)
        right = jnp.zeros((rows, LANES), F32)
        for (n, off), field in zip(slots, fields):
            x = jnp.where(lane < n, field[:, :LANES], 0.0)
            y = jnp.where(lane >= LANES - n, field[:, cols - LANES :], 0.0)
            left = left + (pltpu.roll(x, off, 1) if off else x)
            right = right + (pltpu.roll(y, LANES - off, 1) if off else y)
        at = slice(tile * LANES, (tile + 1) * LANES)
        one_ref[:, at] = jnp.where(even, right, left).astype(BF16)
        two_ref[:, at] = jnp.where(even, left, right).astype(BF16)


def second_kernel(d_ref, v_ref, i_ref, r_ref, a_ref, b_ref, one_ref, two_ref, tab_ref,
                  df_ref, t_ref, up_ref, down_ref, *, s):
    even = lax.rem(lax.axis_index("col"), 2) == 0
    rows, cols = v_ref.shape
    lane = lane_of((rows, LANES))
    sides = []
    for tile, slots in enumerate(s.slots):
        at = slice(tile * LANES, (tile + 1) * LANES)
        one, two = one_ref[:, at].astype(F32), two_ref[:, at].astype(F32)
        from_right = jnp.where(even, one, two)
        from_left = jnp.where(even, two, one)
        for n, off in slots:
            x = pltpu.roll(from_right, LANES - off, 1) if off else from_right
            y = pltpu.roll(from_left, off, 1) if off else from_left
            sides.append(jnp.where(lane < n, x, jnp.where(lane >= LANES - n, y, 0.0)))
    d0s, d1s, i0s, i1s, r0s, r1s, as_, bs, vs = sides
    edge = lane == LANES - 1
    next_side = pltpu.roll(vs, LANES - 1, 1)
    next_own = pltpu.roll(v_ref[:, :LANES], LANES - 1, 1)
    d1 = d_ref[1]
    tail = d1[:, cols - LANES :].astype(F32)
    tail = jnp.where(edge, tail - next_side, tail).astype(BF16)
    d1s = jnp.where(edge, jnp.where(r1s > 0, d1s - next_own, 0.0), d1s).astype(BF16)
    df_ref[0, :, :cols] = d_ref[0]
    df_ref[0, :, cols:] = d0s.astype(BF16)
    df_ref[1, :, : cols - LANES] = d1[:, : cols - LANES]
    df_ref[1, :, cols - LANES : cols] = tail
    df_ref[1, :, cols:] = d1s
    for n, x in enumerate((i0s, i1s, r0s, r1s, as_, bs, vs)):
        t_ref[n] = x.astype(BF16)
    above = lax.rem(lax.axis_index("row"), 2) == 0

    def pack(ref, dstart, fstart):
        at = 0
        for c in range(2):
            ref[at : at + s.up_d, :] = df_ref[c, dstart : dstart + s.up_d, :]
            at += s.up_d
        own = (i_ref.at[0], i_ref.at[1], r_ref.at[0], r_ref.at[1], a_ref, b_ref)
        for n, field in enumerate(own):
            ref[at : at + s.up_f, :cols] = field[fstart : fstart + s.up_f, :].astype(BF16)
            ref[at : at + s.up_f, cols:] = t_ref[n, fstart : fstart + s.up_f, :]
            at += s.up_f
        ref[at : at + TILE, :cols] = v_ref[0:TILE, :].astype(BF16)
        ref[at : at + TILE, cols:] = t_ref[6, 0:TILE, :]

    @pl.when(above)
    def _():
        pack(up_ref, rows - s.up_d, rows - s.up_f)
        pack(down_ref, 0, 0)

    @pl.when(jnp.logical_not(above))
    def _():
        pack(up_ref, 0, 0)
        pack(down_ref, rows - s.up_d, rows - s.up_f)


def convolve(d_ref, t_ref, c, s, strips):
    tiles = s.frame // TILE
    lanes = s.lanes
    first = [t % tiles for t in range(-3, 5)]
    second = list(range(3, 11))
    acc = [jnp.zeros((96, 2 * LANES), F32) for _ in range(3 if strips else 2)]
    for p in range(s.pairs):
        rhs1, rhs2, rhs3 = [], [], []
        for b in (2 * p, 2 * p + 1):
            shift = (s.half - b) % lanes
            x = d_ref[c]
            x = pltpu.roll(x, shift, 1) if shift else x
            rhs1 += [x[t * TILE : (t + 1) * TILE, : s.cols] for t in first]
            rhs2 += [x[t * TILE : (t + 1) * TILE, : s.cols] for t in second]
            rhs3 += [jnp.concatenate([x[t * TILE : (t + 1) * TILE, s.cols :], x[u * TILE : (u + 1) * TILE, s.cols :]], 1)
                     for t, u in zip(first, second)]
        lhs = t_ref[c, p]
        for n, rhs in enumerate((rhs1, rhs2, rhs3)[: len(acc)]):
            acc[n] = acc[n] + jnp.dot(lhs, jnp.concatenate(rhs, 0), preferred_element_type=F32)
    return acc


def last_kernel(df_ref, v_ref, i_ref, r_ref, a_ref, b_ref, c_ref, e_ref, side_ref, tab_ref, one_ref, two_ref,
                vo_ref, io_ref, d_ref, if_ref, rf_ref, af_ref, bf_ref, vf_ref, *, s):
    even = lax.rem(lax.axis_index("row"), 2) == 0
    rows, cols, frame, lanes = s.rows, s.cols, s.frame, s.lanes
    low = jnp.where(even, one_ref[...], two_ref[...])
    high = jnp.where(even, two_ref[...], one_ref[...])
    ud, uf = s.up_d, s.up_f
    own = (i_ref.at[0], i_ref.at[1], r_ref.at[0], r_ref.at[1], a_ref, b_ref)
    frames = (if_ref.at[0], if_ref.at[1], rf_ref.at[0], rf_ref.at[1], af_ref, bf_ref)
    for n, (src, dst) in enumerate(zip(own, frames)):
        at = 2 * ud + n * uf
        dst[0:rows, :cols] = src[...]
        dst[0:rows, cols:] = side_ref[n].astype(F32)
        dst[rows : rows + uf, :] = low[at : at + uf, :].astype(F32)
        dst[rows + uf : frame - uf, :] = jnp.zeros((frame - rows - 2 * uf, lanes), F32)
        dst[frame - uf : frame, :] = high[at : at + uf, :].astype(F32)
    at = 2 * ud + 6 * uf
    v_next = low[at : at + TILE, :].astype(F32)[0:1, :]
    v_first = jnp.concatenate([v_ref[0:8, :][0:1, :], side_ref[6, 0:TILE, :].astype(F32)[0:1, :]], 1)
    gap = rows + 2 * TILE
    shape = (TILE, lanes)
    for c in range(2):
        d_ref[c, 0:rows, :] = df_ref[c]
        d_ref[c, rows:gap, :] = low[c * ud : c * ud + 2 * TILE, :]
        d_ref[c, gap + TILE :, :] = high[c * ud + TILE : (c + 1) * ud, :]
        d_ref[c, gap : gap + TILE, :] = jnp.where(
            row_of(shape) < TILE // 2,
            low[c * ud + 2 * TILE : (c + 1) * ud, :].astype(F32),
            high[c * ud : c * ud + TILE, :].astype(F32)).astype(BF16)
    last = row_of(shape) == TILE - 1
    x = d_ref[0, rows - TILE : rows, :].astype(F32)
    d_ref[0, rows - TILE : rows, :] = jnp.where(last, x - v_next, x).astype(BF16)
    x = d_ref[0, frame - TILE :, :].astype(F32)
    inside = rf_ref[0, frame - TILE :, :] > 0
    d_ref[0, frame - TILE :, :] = jnp.where(last, jnp.where(inside, x - v_first, 0.0), x).astype(BF16)

    for c in range(2):
        one, two, side = convolve(d_ref, tab_ref, c, s, True)
        for dst0, src0, n in ((0, 32, 64), (frame - 32, 0, 32)):
            old = if_ref[c, dst0 : dst0 + n, :]
            add = jnp.concatenate([one[src0 : src0 + n], side[src0 : src0 + n, :LANES]], 1)
            if_ref[c, dst0 : dst0 + n, :] = jnp.where(rf_ref[c, dst0 : dst0 + n, :] > 0, old + add, 0.0)
        old = if_ref[c, 64 : 64 + 96, :]
        add = jnp.concatenate([two, side[:, LANES:]], 1)
        if_ref[c, 64 : 64 + 96, :] = jnp.where(rf_ref[c, 64 : 64 + 96, :] > 0, old + add, 0.0)
    i0, i1 = if_ref[0], if_ref[1]
    div = i0 - pltpu.roll(i0, 1, 0) + i1 - pltpu.roll(i1, 1, 1)
    volt = af_ref[...] - bf_ref[...] * div
    vf_ref[...] = volt
    drop0 = volt - pltpu.roll(volt, frame - 1, 0)
    drop1 = volt - pltpu.roll(volt, lanes - 1, 1)
    r0, r1 = rf_ref[0], rf_ref[1]
    d_ref[0] = jnp.where(r0 > 0, drop0 - r0 * i0, 0.0).astype(BF16)
    d_ref[1] = jnp.where(r1 > 0, drop1 - r1 * i1, 0.0).astype(BF16)

    one, two = convolve(d_ref, tab_ref, 0, s, False)
    above = (if_ref[0, frame - 8 :, :cols] + one[24:32])[7:8]
    above = jnp.where(rf_ref[0, frame - 8 :, :cols][7:8] > 0, above, 0.0)
    io_ref[0, 0:64, :] = if_ref[0, 0:64, :cols] + one[32:]
    io_ref[0, 64:128, :] = if_ref[0, 64:128, :cols] + two[:64]
    one, two, side = convolve(d_ref, tab_ref, 1, s, True)
    io_ref[1, 0:64, :] = if_ref[1, 0:64, :cols] + one[32:]
    io_ref[1, 64:128, :] = if_ref[1, 64:128, :cols] + two[:64]
    side = jnp.concatenate([side[32:, :LANES], side[:64, LANES:]], 0)
    side = jnp.where(rf_ref[1, 0:rows, cols:] > 0, if_ref[1, 0:rows, cols:] + side, 0.0)
    i0, i1 = io_ref[0], io_ref[1]
    up = jnp.where(row_of((rows, cols)) == 0, above, pltpu.roll(i0, 1, 0))
    left = pltpu.roll(jnp.concatenate([i1, side], 1), 1, 1)[:, :cols]
    div = i0 - up + i1 - left
    vo_ref[...] = c_ref[...] * vf_ref[0:rows, :cols] + e_ref[...] - b_ref[...] * div


def swap(x, axis, odd):
    n = lax.axis_size(axis)
    pairs = []
    for i in range(odd, n - 1, 2):
        pairs += [(i, i + 1), (i + 1, i)]
    return lax.ppermute(x, axis, pairs)


def near(x):
    return pltpu.with_memory_space_constraint(x, pltpu.VMEM)


def call(kernel, outs, ins, scratch=(), specs=None, limit=16):
    return pl.pallas_call(
        kernel,
        compiler_params=pltpu.CompilerParams(vmem_limit_bytes=limit << 20),
        out_shape=outs,
        in_specs=specs or [VMEM] * len(ins),
        out_specs=jax.tree.map(lambda _: VMEM, outs),
        scratch_shapes=scratch,
    )(*ins)


def local(voltage, currents, resistance, inverse_cap, shunt, tap, pad, waveforms, k_window):
    rows, cols = voltage.shape
    s = Sizes(rows, cols, k_window.shape[1], waveforms.shape[1])
    sds = pltpu.VMEM
    k_window = k_window.transpose(1, 0, 2)
    block = sds((rows, cols), F32)
    half = sds((rows, 2 * LANES), BF16)
    d, a, b, c, e, one, two, v_near, i_near, r_near, k_near = call(
        functools.partial(first_kernel, s=s),
        (sds((2, rows, cols), BF16), block, block, block, block, half, half,
         block, sds((2, rows, cols), F32), sds((2, rows, cols), F32), sds(k_window.shape, BF16)),
        [pltpu.with_memory_space_constraint(x, pltpu.HBM)
         for x in (voltage, currents, resistance, inverse_cap, shunt, tap, pad, waveforms, k_window)],
        specs=[FAR] * 9,
        scratch=[pltpu.VMEM((rows, cols), F32)] * 2 + [pltpu.VMEM((rows, cols), jnp.int32)] * 2
        + [pltpu.SMEM(waveforms.shape, F32), pltpu.SemaphoreType.DMA((9,))])
    tables = call(
        functools.partial(tables_kernel, s=s),
        sds((2, s.pairs, 96, 2 * LANES), BF16), (k_near,),
        scratch=[pltpu.VMEM((LANES, LANES), F32)])
    one, two = near(swap(one, "col", 0)), near(swap(two, "col", 1))
    pay = sds((s.payload, s.lanes), BF16)
    df, side, one, two = call(
        functools.partial(second_kernel, s=s),
        (sds((2, rows, s.lanes), BF16), sds((7, rows, LANES), BF16), pay, pay),
        (d, v_near, i_near, r_near, a, b, one, two, tables))
    one, two = near(swap(one, "row", 0)), near(swap(two, "row", 1))
    f = pltpu.VMEM((s.frame, s.lanes), F32)
    f2 = pltpu.VMEM((2, s.frame, s.lanes), F32)
    return call(
        functools.partial(last_kernel, s=s),
        (jax.ShapeDtypeStruct((rows, cols), F32), jax.ShapeDtypeStruct((2, rows, cols), F32)),
        (df, v_near, i_near, r_near, a, b, c, e, side, tables, one, two),
        scratch=[pltpu.VMEM((2, s.frame, s.lanes), BF16), f2, f2, f, f, f])


def solution(mesh):
    grid = P("row", "col")
    pair = P(None, "row", "col")
    return jax.shard_map(
        local,
        mesh=mesh,
        in_specs=(grid, pair, pair, grid, grid, grid, grid, P(), P()),
        out_specs=(grid, pair),
        check_vma=False,
    )
```

```python
import functools

import jax
import jax.numpy as jnp
from jax import lax
from jax.experimental import pallas as pl
from jax.experimental.pallas import tpu as pltpu
from jax.sharding import PartitionSpec as P


F32 = jnp.float32
BF16 = jnp.bfloat16
LANES = 128
TILE = 16
VMEM = pl.BlockSpec(memory_space=pltpu.VMEM)
FAR = pl.BlockSpec(memory_space=pltpu.HBM)


class Sizes:
    def __init__(self, rows, cols, span, waves):
        self.rows, self.cols, self.span, self.waves = rows, cols, span, waves
        self.half = (span - 1) // 2
        self.far = 2 * self.half + 2
        self.near = self.half + 2
        self.lanes = cols + LANES
        self.frame = rows + 5 * TILE
        self.group = -(-span // 3)
        self.pairs = (self.group + 1) // 2
        self.fields = rows + 3 * TILE
        self.up_d = 2 * self.half
        self.up_f = self.half
        self.payload = 2 * self.up_d + 6 * self.up_f + TILE
        far, near = self.far, self.near
        self.slots = (
            ((far, 0), (far, far), (near, 2 * far), (near, 2 * far + near)),
            ((near, 0), (near, near), (near, 2 * near), (near, 3 * near), (far, 4 * near)),
        )


def lane_of(shape):
    return lax.broadcasted_iota(jnp.int32, shape, len(shape) - 1)


def row_of(shape):
    return lax.broadcasted_iota(jnp.int32, shape, 0)


def tables_kernel(k_ref, t_ref, pad_ref, *, s):
    zero = jnp.zeros((LANES, LANES), F32)
    for c in range(2):
        pad_ref[...] = zero
        pad_ref[0 : s.span, 0 : s.span] = k_ref[:, c, :].astype(F32)
        turned = pad_ref[...].T
        for r in range(2 * s.pairs):
            p, at = divmod(r, 2)
            for q in range(3):
                if r < s.group:
                    b = s.group * q + r
                    row = jnp.broadcast_to(turned[b : b + 1, :], (96, LANES))
                    band = pltpu.roll(row, 0, 1, stride=1, stride_axis=0).astype(BF16)
                else:
                    band = jnp.zeros((96, LANES), BF16)
                t_ref[c, p, q * 96 : (q + 1) * 96, at * LANES : (at + 1) * LANES] = band


def first_kernel(v_hbm, i_hbm, r_hbm, cap_hbm, shunt_hbm, tap_hbm, pad_hbm, wave_hbm, k_hbm,
                 d_ref, a_ref, b_ref, c_ref, e_ref, one_ref, two_ref, v_ref, i_ref, r_ref, k_ref,
                 cap_ref, shunt_ref, tap_ref, pad_ref, wave_ref, sems, *, s):
    sources = (wave_hbm, tap_hbm, pad_hbm, cap_hbm, shunt_hbm, v_hbm, i_hbm, r_hbm, k_hbm)
    targets = (wave_ref, tap_ref, pad_ref, cap_ref, shunt_ref, v_ref, i_ref, r_ref, k_ref)
    copies = [pltpu.make_async_copy(x, y, sems.at[n]) for n, (x, y) in enumerate(zip(sources, targets))]
    for copy in copies:
        copy.start()
    for copy in copies:
        copy.wait()
    even = lax.rem(lax.axis_index("col"), 2) == 0
    volt = v_ref[...]
    cap, shunt, tap = cap_ref[...], shunt_ref[...], tap_ref[...]
    keep = pad_ref[...] != 1
    loads = []
    for step in range(2):
        total = jnp.zeros(volt.shape, F32)
        for n in range(s.waves):
            total = jnp.where(tap == n, wave_ref[step, n], total)
        loads.append(total)
    b = jnp.where(keep, cap, 0.0)
    c = jnp.where(keep, 1.0, 0.0) - b * shunt
    a = c * volt + b * loads[0]
    a_ref[...], b_ref[...], c_ref[...], e_ref[...] = a, b, c, b * loads[1]
    rows, cols = volt.shape
    below = jnp.where(row_of(volt.shape) == rows - 1, 0.0, pltpu.roll(volt, rows - 1, 0))
    beside = jnp.where(lane_of(volt.shape) == cols - 1, 0.0, pltpu.roll(volt, cols - 1, 1))
    d0 = ((volt - below) - r_ref[0] * i_ref[0]).astype(BF16)
    d1 = ((volt - beside) - r_ref[1] * i_ref[1]).astype(BF16)
    d_ref[0], d_ref[1] = d0, d1
    groups = ((d0.astype(F32), d1.astype(F32), i_ref[0], i_ref[1]), (r_ref[0], r_ref[1], a, b, volt))
    lane = lane_of((rows, LANES))
    for tile, (slots, fields) in enumerate(zip(s.slots, groups)):
        left = jnp.zeros((rows, LANES), F32)
        right = jnp.zeros((rows, LANES), F32)
        for (n, off), field in zip(slots, fields):
            x = jnp.where(lane < n, field[:, :LANES], 0.0)
            y = jnp.where(lane >= LANES - n, field[:, cols - LANES :], 0.0)
            left = left + (pltpu.roll(x, off, 1) if off else x)
            right = right + (pltpu.roll(y, LANES - off, 1) if off else y)
        at = slice(tile * LANES, (tile + 1) * LANES)
        one_ref[:, at] = jnp.where(even, right, left).astype(BF16)
        two_ref[:, at] = jnp.where(even, left, right).astype(BF16)


def second_kernel(d_ref, v_ref, i_ref, r_ref, a_ref, b_ref, one_ref, two_ref, tab_ref,
                  df_ref, t_ref, up_ref, down_ref, *, s):
    even = lax.rem(lax.axis_index("col"), 2) == 0
    rows, cols = v_ref.shape
    lane = lane_of((rows, LANES))
    sides = []
    for tile, slots in enumerate(s.slots):
        at = slice(tile * LANES, (tile + 1) * LANES)
        one, two = one_ref[:, at].astype(F32), two_ref[:, at].astype(F32)
        from_right = jnp.where(even, one, two)
        from_left = jnp.where(even, two, one)
        for n, off in slots:
            x = pltpu.roll(from_right, LANES - off, 1) if off else from_right
            y = pltpu.roll(from_left, off, 1) if off else from_left
            sides.append(jnp.where(lane < n, x, jnp.where(lane >= LANES - n, y, 0.0)))
    d0s, d1s, i0s, i1s, r0s, r1s, as_, bs, vs = sides
    edge = lane == LANES - 1
    next_side = pltpu.roll(vs, LANES - 1, 1)
    next_own = pltpu.roll(v_ref[:, :LANES], LANES - 1, 1)
    d1 = d_ref[1]
    tail = d1[:, cols - LANES :].astype(F32)
    tail = jnp.where(edge, tail - next_side, tail).astype(BF16)
    d1s = jnp.where(edge, jnp.where(r1s > 0, d1s - next_own, 0.0), d1s).astype(BF16)
    df_ref[0, :, :cols] = d_ref[0]
    df_ref[0, :, cols:] = d0s.astype(BF16)
    df_ref[1, :, : cols - LANES] = d1[:, : cols - LANES]
    df_ref[1, :, cols - LANES : cols] = tail
    df_ref[1, :, cols:] = d1s
    for n, x in enumerate((i0s, i1s, r0s, r1s, as_, bs, vs)):
        t_ref[n] = x.astype(BF16)
    above = lax.rem(lax.axis_index("row"), 2) == 0

    own = (i_ref.at[0], i_ref.at[1], r_ref.at[0], r_ref.at[1], a_ref, b_ref)

    def rows_of(n, start, size):
        if n < 2:
            at = start // TILE * TILE
            x = df_ref[n, at : at + TILE, :].astype(F32)
            return x[start - at : start - at + size]
        source = v_ref if n == 8 else own[n - 2]
        at = start // TILE * TILE
        x = t_ref[n - 2, at : at + TILE, :].astype(F32)
        return jnp.concatenate([source[start : start + size, :], x[start - at : start - at + size]], 1)

    def pack(ref, down):
        at = 0
        dstart = rows - s.up_d if down else 0
        fstart = rows - s.up_f if down else 0
        for c in range(2):
            ref[at : at + s.up_d, :] = df_ref[c, dstart : dstart + s.up_d, :]
            at += s.up_d
        for n, field in enumerate(own):
            ref[at : at + s.up_f, :cols] = field[fstart : fstart + s.up_f, :].astype(BF16)
            ref[at : at + s.up_f, cols:] = t_ref[n, fstart : fstart + s.up_f, :]
            at += s.up_f
        eight = row_of((8, s.lanes))
        halves = [jnp.zeros((8, s.lanes), F32), jnp.zeros((8, s.lanes), F32)]
        for n in range(8):
            width = s.up_d if n < 2 else s.up_f
            slot = 2 * n % 8
            if down:
                x = pltpu.roll(rows_of(n, rows - width - 8, 8), (slot + 2) % 8, 0)
            else:
                x = pltpu.roll(rows_of(n, width, 8), slot, 0)
            keep = (eight == slot) | (eight == slot + 1)
            halves[n // 4] = jnp.where(keep, x, halves[n // 4])
        if not down:
            x = pltpu.roll(rows_of(8, 0, 8), 1, 0)
            halves[0] = jnp.where(eight == 1, x, halves[0])
        ref[at : at + TILE, :] = jnp.concatenate(halves, 0).astype(BF16)

    @pl.when(above)
    def _():
        pack(up_ref, True)
        pack(down_ref, False)

    @pl.when(jnp.logical_not(above))
    def _():
        pack(up_ref, False)
        pack(down_ref, True)


def convolve(d_ref, t_ref, c, s):
    tiles = s.frame // TILE
    lanes = s.lanes
    first = [t % tiles for t in range(-3, 5)]
    second = list(range(3, 11))
    acc = [jnp.zeros((288, 2 * LANES), F32) for _ in range(3)]
    for p in range(s.pairs):
        rhs1, rhs2, rhs3 = [], [], []
        for r in (2 * p, 2 * p + 1):
            shift = (s.half - s.group - r) % lanes if r < s.group else 0
            x = d_ref[c]
            x = pltpu.roll(x, shift, 1) if shift else x
            rhs1 += [x[t * TILE : (t + 1) * TILE, : s.cols] for t in first]
            rhs2 += [x[t * TILE : (t + 1) * TILE, : s.cols] for t in second]
            rhs3 += [jnp.concatenate([x[t * TILE : (t + 1) * TILE, s.cols :], x[u * TILE : (u + 1) * TILE, s.cols :]], 1)
                     for t, u in zip(first, second)]
        lhs = t_ref[c, p]
        for n, rhs in enumerate((rhs1, rhs2, rhs3)):
            acc[n] = acc[n] + jnp.dot(lhs, jnp.concatenate(rhs, 0), preferred_element_type=F32)

    def total(n, start, stop):
        parts = []
        for q in range(3):
            at = slice(96 * q + start, 96 * q + stop)
            x = jnp.concatenate([acc[n][at], acc[2][at, n * LANES : (n + 1) * LANES]], 1)
            shift = (s.group - s.group * q) % lanes
            parts.append(pltpu.roll(x, shift, 1) if shift else x)
        return parts[0] + parts[1] + parts[2]

    return total


def last_kernel(df_ref, v_ref, i_ref, r_ref, a_ref, b_ref, c_ref, e_ref, side_ref, tab_ref, one_ref, two_ref,
                vo_ref, io_ref, d_ref, if_ref, rf_ref, af_ref, bf_ref, vf_ref, *, s):
    even = lax.rem(lax.axis_index("row"), 2) == 0
    rows, cols, frame, lanes = s.rows, s.cols, s.frame, s.lanes
    low = jnp.where(even, one_ref[...], two_ref[...])
    high = jnp.where(even, two_ref[...], one_ref[...])
    ud, uf, full = s.up_d, s.up_f, s.fields
    tail = 2 * ud + 6 * uf
    low_rest, high_rest = low[tail:, :].astype(F32), high[tail:, :].astype(F32)
    eight = row_of((8, lanes))
    own = (i_ref.at[0], i_ref.at[1], r_ref.at[0], r_ref.at[1], a_ref, b_ref)
    frames = (if_ref.at[0], if_ref.at[1], rf_ref.at[0], rf_ref.at[1], af_ref, bf_ref)
    for n, (src, dst) in enumerate(zip(own, frames)):
        at = 2 * ud + n * uf
        half, slot = divmod(4 + 2 * n, 8)
        extra_low = pltpu.roll(low_rest[8 * half : 8 * half + 8], (8 - slot) % 8, 0)
        extra_high = pltpu.roll(high_rest[8 * half : 8 * half + 8], 6 - slot, 0)
        dst[0:rows, :cols] = src[...]
        dst[0:rows, cols:] = side_ref[n].astype(F32)
        dst[rows : rows + uf, :] = low[at : at + uf, :].astype(F32)
        dst[rows + uf : rows + uf + 8, :] = jnp.where(eight == 0, extra_low, 0.0)
        dst[full - uf - 8 : full - uf, :] = jnp.where(eight >= 6, extra_high, 0.0)
        dst[full - uf : full, :] = high[at : at + uf, :].astype(F32)
    v_next = low_rest[1:2, :]
    v_first = jnp.concatenate([v_ref[0:8, :][0:1, :], side_ref[6, 0:TILE, :].astype(F32)[0:1, :]], 1)
    gap = rows + ud
    shape = (TILE, lanes)
    for c in range(2):
        d_ref[c, 0:rows, :] = df_ref[c]
        d_ref[c, rows:gap, :] = low[c * ud : (c + 1) * ud, :]
        d_ref[c, gap + TILE :, :] = high[c * ud : (c + 1) * ud, :]
        extra_low = pltpu.roll(low_rest[0:8], (8 - 2 * c) % 8, 0)
        extra_high = pltpu.roll(high_rest[0:8], 6 - 2 * c, 0)
        d_ref[c, gap : gap + TILE, :] = jnp.concatenate(
            [jnp.where(eight == 0, extra_low, 0.0), jnp.where(eight >= 6, extra_high, 0.0)], 0).astype(BF16)
    last = row_of(shape) == TILE - 1
    x = d_ref[0, rows - TILE : rows, :].astype(F32)
    d_ref[0, rows - TILE : rows, :] = jnp.where(last, x - v_next, x).astype(BF16)
    x = d_ref[0, frame - TILE :, :].astype(F32)
    inside = rf_ref[0, full - TILE :, :] > 0
    d_ref[0, frame - TILE :, :] = jnp.where(last, jnp.where(inside, x - v_first, 0.0), x).astype(BF16)

    for c in range(2):
        total = convolve(d_ref, tab_ref, c, s)
        for dst, n, start, stop in ((0, 0, 32, 96), (full - 24, 0, 8, 32), (64, 1, 0, 88)):
            at = slice(dst, dst + stop - start)
            if_ref[c, at, :] = jnp.where(rf_ref[c, at, :] > 0, if_ref[c, at, :] + total(n, start, stop), 0.0)
    i0, i1 = if_ref[0], if_ref[1]
    div = i0 - pltpu.roll(i0, 1, 0) + i1 - pltpu.roll(i1, 1, 1)
    volt = af_ref[...] - bf_ref[...] * div
    vf_ref[...] = volt
    drop0 = volt - pltpu.roll(volt, full - 1, 0)
    drop1 = volt - pltpu.roll(volt, lanes - 1, 1)
    r0, r1 = rf_ref[0], rf_ref[1]
    for c, (drop, r, i) in enumerate(((drop0, r0, i0), (drop1, r1, i1))):
        x = jnp.where(r > 0, drop - r * i, 0.0).astype(BF16)
        d_ref[c, 0 : rows + TILE, :] = x[0 : rows + TILE]
        d_ref[c, frame - 2 * TILE :, :] = x[full - 2 * TILE :]

    total = convolve(d_ref, tab_ref, 0, s)
    above = jnp.where(rf_ref[0, full - 8 :, :] > 0, if_ref[0, full - 8 :, :] + total(0, 24, 32), 0.0)[7:8, :cols]
    io_ref[0, 0:64, :] = (if_ref[0, 0:64, :] + total(0, 32, 96))[:, :cols]
    io_ref[0, 64:128, :] = (if_ref[0, 64:128, :] + total(1, 0, 64))[:, :cols]
    total = convolve(d_ref, tab_ref, 1, s)
    ends = jnp.concatenate([total(0, 32, 96), total(1, 0, 64)], 0)
    ends = jnp.where(rf_ref[1, 0:rows, :] > 0, if_ref[1, 0:rows, :] + ends, 0.0)
    io_ref[1] = ends[:, :cols]
    side = ends[:, cols:]
    i0, i1 = io_ref[0], io_ref[1]
    up = jnp.where(row_of((rows, cols)) == 0, above, pltpu.roll(i0, 1, 0))
    left = pltpu.roll(jnp.concatenate([i1, side], 1), 1, 1)[:, :cols]
    div = i0 - up + i1 - left
    vo_ref[...] = c_ref[...] * vf_ref[0:rows, :cols] + e_ref[...] - b_ref[...] * div


def swapped(x, axis, odd):
    n = lax.axis_size(axis)
    pairs = []
    for i in range(odd, n - 1, 2):
        pairs += [(i, i + 1), (i + 1, i)]
    return lax.ppermute(x, axis, pairs)


def near(x):
    return pltpu.with_memory_space_constraint(x, pltpu.VMEM)


def call(kernel, outs, ins, scratch=(), specs=None, limit=16):
    return pl.pallas_call(
        kernel,
        compiler_params=pltpu.CompilerParams(vmem_limit_bytes=limit << 20),
        out_shape=outs,
        in_specs=specs or [VMEM] * len(ins),
        out_specs=jax.tree.map(lambda _: VMEM, outs),
        scratch_shapes=scratch,
    )(*ins)


def local(voltage, currents, resistance, inverse_cap, shunt, tap, pad, waveforms, k_window):
    rows, cols = voltage.shape
    s = Sizes(rows, cols, k_window.shape[1], waveforms.shape[1])
    sds = pltpu.VMEM
    k_window = k_window.transpose(1, 0, 2)
    block = sds((rows, cols), F32)
    half = sds((rows, 2 * LANES), BF16)
    d, a, b, c, e, one, two, v_near, i_near, r_near, k_near = call(
        functools.partial(first_kernel, s=s),
        (sds((2, rows, cols), BF16), block, block, block, block, half, half,
         block, sds((2, rows, cols), F32), sds((2, rows, cols), F32), sds(k_window.shape, BF16)),
        [pltpu.with_memory_space_constraint(x, pltpu.HBM)
         for x in (voltage, currents, resistance, inverse_cap, shunt, tap, pad, waveforms, k_window)],
        specs=[FAR] * 9,
        scratch=[pltpu.VMEM((rows, cols), F32)] * 2 + [pltpu.VMEM((rows, cols), jnp.int32)] * 2
        + [pltpu.SMEM(waveforms.shape, F32), pltpu.SemaphoreType.DMA((9,))])
    tables = call(
        functools.partial(tables_kernel, s=s),
        sds((2, s.pairs, 288, 2 * LANES), BF16), (k_near,),
        scratch=[pltpu.VMEM((LANES, LANES), F32)])
    one, two = near(swapped(one, "col", 0)), near(swapped(two, "col", 1))
    pay = sds((s.payload, s.lanes), BF16)
    df, side, one, two = call(
        functools.partial(second_kernel, s=s),
        (sds((2, rows, s.lanes), BF16), sds((7, rows, LANES), BF16), pay, pay),
        (d, v_near, i_near, r_near, a, b, one, two, tables))
    one, two = near(swapped(one, "row", 0)), near(swapped(two, "row", 1))
    f = pltpu.VMEM((s.fields, s.lanes), F32)
    f2 = pltpu.VMEM((2, s.fields, s.lanes), F32)
    return call(
        functools.partial(last_kernel, s=s),
        (jax.ShapeDtypeStruct((rows, cols), F32), jax.ShapeDtypeStruct((2, rows, cols), F32)),
        (df, v_near, i_near, r_near, a, b, c, e, side, tables, one, two),
        scratch=[pltpu.VMEM((2, s.frame, s.lanes), BF16), f2, f2, f, f, f])


def solution(mesh):
    grid = P("row", "col")
    pair = P(None, "row", "col")

    return jax.shard_map(
        local,
        mesh=mesh,
        in_specs=(grid, pair, pair, grid, grid, grid, grid, P(), P()),
        out_specs=(grid, pair),
        check_vma=False,
    )
```

```python
import functools
import itertools

import jax
import jax.numpy as jnp
from jax import lax
from jax.experimental import pallas as pl
from jax.experimental.pallas import tpu as pltpu
from jax.sharding import PartitionSpec as P


F32 = jnp.float32
BF16 = jnp.bfloat16
LANES = 128
TILE = 16
VMEM = pl.BlockSpec(memory_space=pltpu.VMEM)
FAR = pl.BlockSpec(memory_space=pltpu.HBM)


class Sizes:
    def __init__(self, rows, cols, span, waves):
        self.rows, self.cols, self.span, self.waves = rows, cols, span, waves
        self.half = (span - 1) // 2
        self.far = 2 * self.half + 2
        self.near = self.half + 2
        self.lanes = cols + LANES
        self.frame = rows + 5 * TILE
        self.group = -(-span // 3)
        self.pairs = (self.group + 1) // 2
        self.span3 = -(-self.group // 3)
        self.fields = rows + 3 * TILE
        self.up_d = 2 * self.half
        self.up_f = self.half
        self.payload = 2 * self.up_d + 6 * self.up_f + TILE
        far, near = self.far, self.near
        self.slots = (
            ((far, 0, 0), (far, far, far), (near, 2 * far, far + near),
             (near, 2 * far + near, far + 2 * near), (near, 2 * far + 2 * near, far + 3 * near)),
            ((near, 0, 0), (near, near, near), (near, 2 * near, 2 * near), (1, 3 * near, 3 * near)),
        )
        self.edge = rows + rows // 2 + TILE


def lane_of(shape):
    return lax.broadcasted_iota(jnp.int32, shape, len(shape) - 1)


def row_of(shape):
    return lax.broadcasted_iota(jnp.int32, shape, 0)


def border_rows(c):
    return 64 if c == 0 else 48


def turn(k_ref, pad_ref, c, s):
    pad_ref[...] = jnp.zeros((LANES, LANES), F32)
    pad_ref[0 : s.span, 0 : s.span] = k_ref[:, c, :].astype(F32)
    return pad_ref[...].T


def main_tables(k_ref, t_ref, pad_ref, s):
    for c in range(2):
        turned = turn(k_ref, pad_ref, c, s)
        for r in range(2 * s.pairs):
            p, at = divmod(r, 2)
            for q in range(3):
                if r < s.group:
                    b = s.group * q + r
                    row = jnp.broadcast_to(turned[b : b + 1, :], (96, LANES))
                    band = pltpu.roll(row, 0, 1, stride=1, stride_axis=0).astype(BF16)
                else:
                    band = jnp.zeros((96, LANES), BF16)
                t_ref[c, p, q * 96 : (q + 1) * 96, at * LANES : (at + 1) * LANES] = band


def border_tables(k_ref, e_ref, pad_ref, s):
    window = 5 * TILE
    blank = jnp.zeros((1, LANES), F32)
    for c in range(2):
        turned = turn(k_ref, pad_ref, c, s)
        n = border_rows(c)
        late = 1 - c
        for g in range(s.span3):
            for q in range(3):
                row = jnp.zeros((1, 2 * LANES), F32)
                for at in range(3):
                    r = 3 * g + at
                    if r < s.group:
                        b = s.group * q + r
                        wide = jnp.concatenate([turned[b : b + 1, :], blank], 1)
                        shift = (window * at - late) % (2 * LANES)
                        row = row + (pltpu.roll(wide, shift, 1) if shift else wide)
                row = jnp.broadcast_to(row, (n, 2 * LANES))
                band = pltpu.roll(row, 0, 1, stride=1, stride_axis=0)
                if late:
                    lane = lane_of(band.shape)
                    kept = lane == s.span - 2
                    for at in range(1, 3):
                        kept = kept | (lane == window * at + s.span - 2)
                    band = jnp.where((row_of(band.shape) > 0) | kept, band, 0.0)
                e_ref[c, g, q * n : (q + 1) * n, :] = band.astype(BF16)


def load_of(tap, wave_ref, step, s):
    total = jnp.zeros(tap.shape, F32)
    for n in range(s.waves):
        total = jnp.where(tap == n, wave_ref[step, n], total)
    return total


def border_rows(c):
    return 64 if c == 0 else 48


def first_kernel(v_hbm, i_hbm, r_hbm, cap_hbm, shunt_hbm, tap_hbm, pad_hbm, wave_hbm, k_hbm,
                 one_ref, two_ref, v_ref, i_ref, r_ref, cap_ref, shunt_ref, tap_ref, pad_ref, k_ref,
                 wave_ref, sems, *, s):
    sources = (wave_hbm, tap_hbm, pad_hbm, cap_hbm, shunt_hbm, v_hbm, i_hbm, r_hbm, k_hbm)
    targets = (wave_ref, tap_ref, pad_ref, cap_ref, shunt_ref, v_ref, i_ref, r_ref, k_ref)
    copies = [pltpu.make_async_copy(x, y, sems.at[n]) for n, (x, y) in enumerate(zip(sources, targets))]
    for copy in copies:
        copy.start()
    even = lax.rem(lax.axis_index("col"), 2) == 0
    rows, cols = s.rows, s.cols
    shape = (rows, LANES)
    lane, row = lane_of(shape), row_of(shape)

    def ends(ref):
        return jnp.where(lane < LANES // 2, ref[:, :LANES], ref[:, cols - LANES :])

    for copy in copies[:2]:
        copy.wait()
    load = load_of(ends(tap_ref), wave_ref, 0, s)
    for copy in copies[2:5]:
        copy.wait()
    keep = ends(pad_ref) != 1
    b = jnp.where(keep, ends(cap_ref), 0.0)
    c = jnp.where(keep, 1.0, 0.0) - b * ends(shunt_ref)
    a = b * load
    for copy in copies[5:]:
        copy.wait()
    volt = ends(v_ref)
    a = a + c * volt
    i0, i1, r0, r1 = ends(i_ref.at[0]), ends(i_ref.at[1]), ends(r_ref.at[0]), ends(r_ref.at[1])
    below = jnp.where(row == rows - 1, 0.0, pltpu.roll(volt, rows - 1, 0))
    beside = jnp.where(lane == LANES - 1, 0.0, pltpu.roll(volt, LANES - 1, 1))
    d0 = (volt - below) - r0 * i0
    d1 = (volt - beside) - r1 * i1
    half = rows // 2

    def put(start, left, right):
        at = slice(start, start + left.shape[0])
        one_ref[at, :] = jnp.where(even, right, left).astype(BF16)
        two_ref[at, :] = jnp.where(even, left, right).astype(BF16)

    for tile, (slots, fields) in enumerate(zip(s.slots, ((d0, d1, i0, i1, r0), (r1, a, b, volt)))):
        left = jnp.zeros(shape, F32)
        right = jnp.zeros(shape, F32)
        for (n, off, back), field in zip(slots, fields):
            x = rolled(field, off)
            left = jnp.where((lane >= off) & (lane < off + n), x, left)
            if n > 1:
                x = x if back == off else rolled(field, back)
                right = jnp.where(before(lane, n, back), x, right)
        if tile == 1:
            left = left[:half] + pltpu.roll(left[half:], LANES // 2, 1)
            right = right[:half] + pltpu.roll(right[half:], LANES // 2, 1)
        put(tile * rows, left, right)
    put(rows + half, v_ref[:TILE, :LANES], v_ref[:TILE, cols - LANES :])


def before(lane, n, off):
    if off >= n:
        return (lane >= off - n) & (lane < off)
    return (lane < off) | (lane >= LANES + off - n)


def own_kernel(v_ref, i_ref, r_ref, cap_ref, shunt_ref, tap_ref, pad_ref, k_ref, wave_hbm,
               d_ref, a_ref, b_ref, c_ref, e_ref, t_ref, wave_ref, square_ref, sem, *, s):
    copy = pltpu.make_async_copy(wave_hbm, wave_ref, sem.at[0])
    copy.start()
    main_tables(k_ref, t_ref, square_ref, s)
    volt = v_ref[...]
    rows, cols = volt.shape
    below = jnp.where(row_of(volt.shape) == rows - 1, 0.0, pltpu.roll(volt, rows - 1, 0))
    beside = jnp.where(lane_of(volt.shape) == cols - 1, 0.0, pltpu.roll(volt, cols - 1, 1))
    d_ref[0] = ((volt - below) - r_ref[0] * i_ref[0]).astype(BF16)
    d_ref[1] = ((volt - beside) - r_ref[1] * i_ref[1]).astype(BF16)
    keep = pad_ref[...] != 1
    b = jnp.where(keep, cap_ref[...], 0.0)
    c = jnp.where(keep, 1.0, 0.0) - b * shunt_ref[...]
    b_ref[...], c_ref[...] = b, c
    copy.wait()
    a_ref[...] = c * volt + b * load_of(tap_ref[...], wave_ref, 0, s)
    e_ref[...] = b * load_of(tap_ref[...], wave_ref, 1, s)


def second_kernel(d_ref, v_ref, i_ref, r_ref, a_ref, b_ref, one_ref, two_ref,
                  df_ref, t_ref, up_ref, down_ref, *, s):
    even = lax.rem(lax.axis_index("col"), 2) == 0
    rows, cols = v_ref.shape
    lane = lane_of((rows, LANES))
    half = rows // 2
    index, count = lax.axis_index("col"), lax.axis_size("col")

    def get(start, size):
        at = slice(start, start + size)
        one, two = one_ref[at, :].astype(F32), two_ref[at, :].astype(F32)
        right, left = jnp.where(even, one, two), jnp.where(even, two, one)
        return jnp.where(index < count - 1, right, 0.0), jnp.where(index > 0, left, 0.0)

    sides = []
    for tile, slots in enumerate(s.slots):
        if tile == 0:
            pair = get(0, rows)
        else:
            pair = [jnp.concatenate([x, pltpu.roll(x, LANES // 2, 1)], 0) for x in get(rows, half)]
        for n, off, back in slots:
            if back == off:
                x = jnp.where((lane >= off) & (lane < off + n), pair[0], pair[1])
                x = rolled(x, (LANES - off) % LANES)
                sides.append(jnp.where((lane < n) | (lane >= LANES - n), x, 0.0))
            else:
                x, y = rolled(pair[0], LANES - off), rolled(pair[1], LANES - back)
                sides.append(jnp.where(lane < n, x, jnp.where(lane >= LANES - n, y, 0.0)))
    d0s, d1s, i0s, i1s, r0s, r1s, as_, bs, vs = sides
    x, y = get(rows + half, TILE)
    first = lane_of((TILE, LANES))
    corner = jnp.where(first < s.far, x, jnp.where(first >= LANES - s.far, y, 0.0))
    edge = lane == LANES - 1
    next_side = pltpu.roll(vs, LANES - 1, 1)
    next_own = pltpu.roll(v_ref[:, :LANES], LANES - 1, 1)
    d1 = d_ref[1]
    tail = d1[:, cols - LANES :].astype(F32)
    tail = jnp.where(edge, tail - next_side, tail).astype(BF16)
    d1s = jnp.where(edge, jnp.where(r1s > 0, d1s - next_own, 0.0), d1s).astype(BF16)
    df_ref[0, :, :cols] = d_ref[0]
    df_ref[0, :, cols:] = d0s.astype(BF16)
    df_ref[1, :, : cols - LANES] = d1[:, : cols - LANES]
    df_ref[1, :, cols - LANES : cols] = tail
    df_ref[1, :, cols:] = d1s
    for n, x in enumerate((i0s, i1s, r0s, r1s, as_, bs)):
        t_ref[n] = x.astype(BF16)
    t_ref[6, :TILE, :] = corner.astype(BF16)
    above = lax.rem(lax.axis_index("row"), 2) == 0

    own = (i_ref.at[0], i_ref.at[1], r_ref.at[0], r_ref.at[1], a_ref, b_ref)

    def rows_of(n, start, size):
        if n < 2:
            at = start // TILE * TILE
            x = df_ref[n, at : at + TILE, :].astype(F32)
            return x[start - at : start - at + size]
        source = v_ref if n == 8 else own[n - 2]
        at = start // TILE * TILE
        x = t_ref[n - 2, at : at + TILE, :].astype(F32)
        return jnp.concatenate([source[start : start + size, :], x[start - at : start - at + size]], 1)

    def pack(ref, down):
        at = 0
        dstart = rows - s.up_d if down else 0
        fstart = rows - s.up_f if down else 0
        for c in range(2):
            ref[at : at + s.up_d, :] = df_ref[c, dstart : dstart + s.up_d, :]
            at += s.up_d
        for n, field in enumerate(own):
            ref[at : at + s.up_f, :cols] = field[fstart : fstart + s.up_f, :].astype(BF16)
            ref[at : at + s.up_f, cols:] = t_ref[n, fstart : fstart + s.up_f, :]
            at += s.up_f
        eight = row_of((8, s.lanes))
        halves = [jnp.zeros((8, s.lanes), F32), jnp.zeros((8, s.lanes), F32)]
        for n in range(8):
            width = s.up_d if n < 2 else s.up_f
            slot = 2 * n % 8
            if down:
                x = pltpu.roll(rows_of(n, rows - width - 8, 8), (slot + 2) % 8, 0)
            else:
                x = pltpu.roll(rows_of(n, width, 8), slot, 0)
            keep = (eight == slot) | (eight == slot + 1)
            halves[n // 4] = jnp.where(keep, x, halves[n // 4])
        if not down:
            x = pltpu.roll(rows_of(8, 0, 8), 1, 0)
            halves[0] = jnp.where(eight == 1, x, halves[0])
        ref[at : at + TILE, :] = jnp.concatenate(halves, 0).astype(BF16)

    @pl.when(above)
    def _():
        pack(up_ref, True)
        pack(down_ref, False)

    @pl.when(jnp.logical_not(above))
    def _():
        pack(up_ref, False)
        pack(down_ref, True)


def convolve(d_ref, t_ref, c, s, second=range(3, 11), low=0):
    tiles = s.frame // TILE
    lanes = s.lanes
    first = [t % tiles for t in range(-3, 5)]
    high = 96 - low
    acc = [jnp.zeros((3 * high, 2 * LANES), F32) for _ in range(3)]
    for p in range(s.pairs):
        rhs1, rhs2, rhs3 = [], [], []
        for r in (2 * p, 2 * p + 1):
            shift = (s.half - s.group - r) % lanes if r < s.group else 0
            x = d_ref[c]
            x = pltpu.roll(x, shift, 1) if shift else x
            rhs1 += [x[t * TILE : (t + 1) * TILE, : s.cols] for t in first]
            rhs2 += [x[t * TILE : (t + 1) * TILE, : s.cols] for t in second]
            rhs3 += [jnp.concatenate([x[t * TILE : (t + 1) * TILE, s.cols :], x[u * TILE : (u + 1) * TILE, s.cols :]], 1)
                     for t, u in zip(first, second)]
        lhs = jnp.concatenate([t_ref[c, p, 96 * q + low : 96 * q + 96, :] for q in range(3)], 0)
        for n, rhs in enumerate((rhs1, rhs2, rhs3)):
            acc[n] = acc[n] + jnp.dot(lhs, jnp.concatenate(rhs, 0), preferred_element_type=F32)

    def total(n, start, stop):
        parts = []
        for q in range(3):
            at = slice(high * q + start - low, high * q + stop - low)
            x = jnp.concatenate([acc[n][at], acc[2][at, n * LANES : (n + 1) * LANES]], 1)
            shift = (s.group - s.group * q) % lanes
            parts.append(pltpu.roll(x, shift, 1) if shift else x)
        return parts[0] + parts[1] + parts[2]

    return total


def rolled(x, shift):
    return pltpu.roll(x, shift, 1) if shift else x


def gather(acc, n, high, start, stop, s):
    parts = []
    for q in range(3):
        at = slice(high * q + start, high * q + stop)
        side = acc[2][at, n * LANES : (n + 1) * LANES]
        parts.append(rolled(jnp.concatenate([acc[n][at], side], 1), (s.group - s.group * q) % s.lanes))
    return parts[0] + parts[1] + parts[2]


def middle_kernel(df_ref, i_ref, r_ref, a_ref, b_ref, side_ref, tab_ref, k_ref,
                  if_ref, rf_ref, af_ref, bf_ref, x_ref, bor_ref, z_ref, square_ref, *, s):
    border_tables(k_ref, bor_ref, square_ref, s)
    rows, cols, lanes = s.rows, s.cols, s.lanes
    own = (i_ref.at[0], i_ref.at[1], r_ref.at[0], r_ref.at[1], a_ref, b_ref)
    frames = (if_ref.at[0], if_ref.at[1], rf_ref.at[0], rf_ref.at[1], af_ref, bf_ref)
    for n, (src, dst) in enumerate(zip(own, frames)):
        dst[0:rows, :cols] = src[...]
        dst[0:rows, cols:] = side_ref[n].astype(F32)
    z_ref[...] = df_ref[...]
    end = z_ref[0, rows - TILE :, :]
    z_ref[0, rows - TILE :, :] = jnp.where(row_of(end.shape) == TILE - 1, 0.0, end.astype(F32)).astype(BF16)
    for c in range(2):
        acc = [jnp.zeros((288, cols), F32), None, jnp.zeros((288, LANES), F32)]
        for p in range(s.pairs):
            pieces = []
            for r in (2 * p, 2 * p + 1):
                if r < s.group:
                    x = rolled(z_ref[c], (s.half - s.group - r) % lanes)
                    x_ref[c, r, 0 : 2 * TILE, :] = x[0 : 2 * TILE]
                    x_ref[c, r, 2 * TILE :, :] = x[rows - 2 * TILE :]
                pieces.append(x)
            rhs = jnp.concatenate(pieces, 0)
            acc[0] = acc[0] + jnp.dot(tab_ref[c, p], rhs[:, :cols], preferred_element_type=F32)
            acc[2] = acc[2] + jnp.dot(tab_ref[c, p], rhs[:, cols:], preferred_element_type=F32)
        at = slice(s.half, rows - s.half)
        total = gather(acc, 0, 96, 0, 96, s)
        if_ref[c, at, :] = jnp.where(rf_ref[c, at, :] > 0, if_ref[c, at, :] + total, 0.0)


def border(d_ref, x_ref, e_ref, c, s):
    n = border_rows(c)
    acc = [jnp.zeros((3 * n, 2 * LANES), F32) for _ in range(3)]
    rows, lanes, cols = s.rows, s.lanes, s.cols
    for g in range(s.span3):
        tops, bottoms = [], []
        for at in range(3):
            r = 3 * g + at
            r = r if r < s.group else 0
            shift = (s.half - s.group - r) % lanes
            outer = rolled(d_ref[c, rows : s.frame, :], shift)
            start, stop = x_ref[c, r, 0 : 2 * TILE, :], x_ref[c, r, 2 * TILE :, :]
            if c == 0:
                stop = jnp.concatenate([stop[:TILE], rolled(d_ref[c, rows - TILE : rows, :], shift)], 0)
            top = jnp.concatenate([outer[2 * TILE :], start], 0)
            bottom = jnp.concatenate([stop, outer[: 3 * TILE]], 0)
            tops.append(top)
            bottoms.append(bottom)
        tops.append(tops[0][:TILE])
        bottoms.append(bottoms[0][:TILE])
        top, bottom = jnp.concatenate(tops, 0), jnp.concatenate(bottoms, 0)
        strip = jnp.concatenate([top[:, cols:], bottom[:, cols:]], 1)
        lhs = e_ref[c, g, 0 : 3 * n, :]
        for k, rhs in enumerate((top[:, :cols], bottom[:, :cols], strip)):
            acc[k] = acc[k] + jnp.dot(lhs, rhs, preferred_element_type=F32)
    return [gather(acc, k, n, 0, n, s) for k in range(2)]


def last_kernel(df_ref, v_ref, b_ref, c_ref, e_ref, side_ref, tab_ref, bor_ref, x_ref, one_ref, two_ref,
                if_in, rf_in, af_in, bf_in, vo_hbm, io_hbm, if_ref, rf_ref, af_ref, bf_ref,
                d_ref, vf_ref, vo_ref, io_ref, sems, *, s):
    even = lax.rem(lax.axis_index("row"), 2) == 0
    rows, cols, frame, lanes = s.rows, s.cols, s.frame, s.lanes
    index = lax.axis_index("row")
    low = jnp.where(even, one_ref[...], two_ref[...])
    high = jnp.where(even, two_ref[...], one_ref[...])
    low = jnp.where(index < lax.axis_size("row") - 1, low, jnp.zeros_like(low))
    high = jnp.where(index > 0, high, jnp.zeros_like(high))
    ud, uf, full = s.up_d, s.up_f, s.fields
    tail = 2 * ud + 6 * uf
    low_rest, high_rest = low[tail:, :].astype(F32), high[tail:, :].astype(F32)
    eight = row_of((8, lanes))
    frames = (if_ref.at[0], if_ref.at[1], rf_ref.at[0], rf_ref.at[1], af_ref, bf_ref)
    for n, dst in enumerate(frames):
        at = 2 * ud + n * uf
        half, slot = divmod(4 + 2 * n, 8)
        extra_low = pltpu.roll(low_rest[8 * half : 8 * half + 8], (8 - slot) % 8, 0)
        extra_high = pltpu.roll(high_rest[8 * half : 8 * half + 8], 6 - slot, 0)
        dst[rows : rows + uf, :] = low[at : at + uf, :].astype(F32)
        dst[rows + uf : rows + uf + 8, :] = jnp.where(eight == 0, extra_low, 0.0)
        dst[full - uf - 8 : full - uf, :] = jnp.where(eight >= 6, extra_high, 0.0)
        dst[full - uf : full, :] = high[at : at + uf, :].astype(F32)
    v_next = low_rest[1:2, :]
    v_first = jnp.concatenate([v_ref[0:8, :][0:1, :], side_ref[6, 0:TILE, :].astype(F32)[0:1, :]], 1)
    gap = rows + ud
    shape = (TILE, lanes)
    for c in range(2):
        d_ref[c, 0:rows, :] = df_ref[c]
        d_ref[c, rows:gap, :] = low[c * ud : (c + 1) * ud, :]
        d_ref[c, gap + TILE :, :] = high[c * ud : (c + 1) * ud, :]
        extra_low = pltpu.roll(low_rest[0:8], (8 - 2 * c) % 8, 0)
        extra_high = pltpu.roll(high_rest[0:8], 6 - 2 * c, 0)
        d_ref[c, gap : gap + TILE, :] = jnp.concatenate(
            [jnp.where(eight == 0, extra_low, 0.0), jnp.where(eight >= 6, extra_high, 0.0)], 0).astype(BF16)
    last = row_of(shape) == TILE - 1
    x = d_ref[0, rows - TILE : rows, :].astype(F32)
    d_ref[0, rows - TILE : rows, :] = jnp.where(last, x - v_next, x).astype(BF16)
    x = d_ref[0, frame - TILE :, :].astype(F32)
    inside = rf_ref[0, full - TILE :, :] > 0
    d_ref[0, frame - TILE :, :] = jnp.where(last, jnp.where(inside, x - v_first, 0.0), x).astype(BF16)

    for c in range(2):
        top, bottom = border(d_ref, x_ref, bor_ref, c, s)
        n = border_rows(c)
        pieces = []
        if c == 0:
            pieces.append((rows - 24, jnp.where(eight == 7, jnp.broadcast_to(bottom[0:1], (8, lanes)), 0.0)))
            top, bottom = pltpu.roll(top, n - 1, 0), pltpu.roll(bottom, n - 1, 0)
        pieces += [(full - 24, top[8:32]), (0, top[32:48]), (rows - TILE, bottom[0:40])]
        for dst, add in pieces:
            at = slice(dst, dst + add.shape[0])
            if_ref[c, at, :] = jnp.where(rf_ref[c, at, :] > 0, if_ref[c, at, :] + add, 0.0)
    i0, i1 = if_ref[0], if_ref[1]
    div = i0 - pltpu.roll(i0, 1, 0) + i1 - pltpu.roll(i1, 1, 1)
    volt = af_ref[...] - bf_ref[...] * div
    vf_ref[...] = volt
    drop0 = volt - pltpu.roll(volt, full - 1, 0)
    drop1 = volt - pltpu.roll(volt, lanes - 1, 1)
    r0, r1 = rf_ref[0], rf_ref[1]
    for c, (drop, r, i) in enumerate(((drop0, r0, i0), (drop1, r1, i1))):
        x = jnp.where(r > 0, drop - r * i, 0.0).astype(BF16)
        d_ref[c, 0 : rows + TILE, :] = x[0 : rows + TILE]
        d_ref[c, frame - 2 * TILE :, :] = x[full - 2 * TILE :]

    total = convolve(d_ref, tab_ref, 0, s, range(1, 9), 16)
    above = jnp.where(rf_ref[0, full - 8 :, :] > 0, if_ref[0, full - 8 :, :] + total(0, 24, 32), 0.0)[7:8, :cols]
    for n in range(2):
        at = slice(64 * n, 64 * n + 64)
        io_ref[0, at, :] = (if_ref[0, at, :] + total(n, 32, 96))[:, :cols]
    out0 = pltpu.make_async_copy(io_ref.at[0], io_hbm.at[0], sems.at[0])
    out0.start()
    total = convolve(d_ref, tab_ref, 1, s, range(1, 9), 32)
    ends = jnp.concatenate([total(0, 32, 96), total(1, 32, 96)], 0)
    ends = jnp.where(rf_ref[1, 0:rows, :] > 0, if_ref[1, 0:rows, :] + ends, 0.0)
    io_ref[1] = ends[:, :cols]
    out1 = pltpu.make_async_copy(io_ref.at[1], io_hbm.at[1], sems.at[1])
    out1.start()
    side = ends[:, cols:]
    i0, i1 = io_ref[0], io_ref[1]
    up = jnp.where(row_of((rows, cols)) == 0, above, pltpu.roll(i0, 1, 0))
    left = pltpu.roll(jnp.concatenate([i1, side], 1), 1, 1)[:, :cols]
    div = i0 - up + i1 - left
    vo_ref[...] = c_ref[...] * vf_ref[0:rows, :cols] + e_ref[...] - b_ref[...] * div
    out2 = pltpu.make_async_copy(vo_ref, vo_hbm, sems.at[2])
    out2.start()
    for copy in (out0, out1, out2):
        copy.wait()


def swapped(x, axis, odd):
    sizes = lax.axis_size("row"), lax.axis_size("col")
    main = ("row", "col").index(axis)
    to = {}
    for at in itertools.product(range(sizes[0]), range(sizes[1])):
        along, other = at[main], at[1 - main]
        if along >= odd and (along ^ 1 if not odd else ((along - 1) ^ 1) + 1) < sizes[main]:
            along = along ^ 1 if not odd else ((along - 1) ^ 1) + 1
        elif other ^ 1 < sizes[1 - main]:
            other = other ^ 1
        else:
            continue
        there = (along, other) if main == 0 else (other, along)
        to[at[0] * sizes[1] + at[1]] = there[0] * sizes[1] + there[1]
    return lax.ppermute(x, ("row", "col"), list(to.items()))


def near(x):
    return pltpu.with_memory_space_constraint(x, pltpu.VMEM)


def call(kernel, outs, ins, scratch=(), specs=None, limit=16, out_specs=None, aliases=None):
    return pl.pallas_call(
        kernel,
        compiler_params=pltpu.CompilerParams(vmem_limit_bytes=limit << 20),
        out_shape=outs,
        in_specs=specs or [VMEM] * len(ins),
        out_specs=out_specs or jax.tree.map(lambda _: VMEM, outs),
        scratch_shapes=scratch,
        input_output_aliases=aliases or {},
    )(*ins)


def local(voltage, currents, resistance, inverse_cap, shunt, tap, pad, waveforms, k_window):
    rows, cols = voltage.shape
    s = Sizes(rows, cols, k_window.shape[1], waveforms.shape[1])
    sds = pltpu.VMEM
    k_window = k_window.transpose(1, 0, 2)
    block = sds((rows, cols), F32)
    half = sds((s.edge, LANES), BF16)
    pair = sds((2, rows, cols), F32)
    whole = sds((rows, cols), jnp.int32)
    waveforms = pltpu.with_memory_space_constraint(waveforms, pltpu.HBM)
    one, two, v_near, i_near, r_near, cap_near, shunt_near, tap_near, pad_near, k_near = call(
        functools.partial(first_kernel, s=s),
        (half, half, block, pair, pair, block, block, whole, whole, sds(k_window.shape, BF16)),
        [pltpu.with_memory_space_constraint(x, pltpu.HBM)
         for x in (voltage, currents, resistance, inverse_cap, shunt, tap, pad)]
        + [waveforms, pltpu.with_memory_space_constraint(k_window, pltpu.HBM)],
        specs=[FAR] * 9,
        scratch=[pltpu.SMEM(waveforms.shape, F32), pltpu.SemaphoreType.DMA((9,))])
    square = pltpu.VMEM((LANES, LANES), F32)
    d, a, b, c, e, tables = call(
        functools.partial(own_kernel, s=s),
        (sds((2, rows, cols), BF16), block, block, block, block, sds((2, s.pairs, 288, 2 * LANES), BF16)),
        (v_near, i_near, r_near, cap_near, shunt_near, tap_near, pad_near, k_near, waveforms),
        specs=[VMEM] * 8 + [FAR],
        scratch=[pltpu.SMEM(waveforms.shape, F32), square, pltpu.SemaphoreType.DMA((1,))])
    one, two = near(swapped(one, "col", 0)), near(swapped(two, "col", 1))
    pay = sds((s.payload, s.lanes), BF16)
    df, side, one, two = call(
        functools.partial(second_kernel, s=s),
        (sds((2, rows, s.lanes), BF16), sds((7, rows, LANES), BF16), pay, pay),
        (d, v_near, i_near, r_near, a, b, one, two))
    one, two = swapped(one, "row", 0), swapped(two, "row", 1)
    f = sds((s.fields, s.lanes), F32)
    f2 = sds((2, s.fields, s.lanes), F32)
    i_frame, r_frame, a_frame, b_frame, shifted, borders = call(
        functools.partial(middle_kernel, s=s),
        (f2, f2, f, f, sds((2, s.group, 4 * TILE, s.lanes), BF16),
         sds((2, s.span3, 192, 2 * LANES), BF16)),
        (df, i_near, r_near, a, b, side, tables, k_near),
        scratch=[pltpu.VMEM((2, rows, s.lanes), BF16), square])
    outs = call(
        functools.partial(last_kernel, s=s),
        (jax.ShapeDtypeStruct((rows, cols), F32), jax.ShapeDtypeStruct((2, rows, cols), F32), f2, f2, f, f),
        (df, v_near, b, c, e, side, tables, borders, shifted, near(one), near(two), i_frame, r_frame, a_frame, b_frame),
        scratch=[pltpu.VMEM((2, s.frame, s.lanes), BF16), pltpu.VMEM((s.fields, s.lanes), F32),
                 pltpu.VMEM((rows, cols), F32), pltpu.VMEM((2, rows, cols), F32), pltpu.SemaphoreType.DMA((3,))],
        out_specs=(FAR, FAR, VMEM, VMEM, VMEM, VMEM), aliases={11: 2, 12: 3, 13: 4, 14: 5})
    return outs[0], outs[1]


def solution(mesh):
    grid = P("row", "col")
    pair = P(None, "row", "col")

    return jax.shard_map(
        local,
        mesh=mesh,
        in_specs=(grid, pair, pair, grid, grid, grid, grid, P(), P()),
        out_specs=(grid, pair),
        check_vma=False,
    )
```

```python
import functools
import itertools

import jax
import jax.numpy as jnp
from jax import lax
from jax.experimental import pallas as pl
from jax.experimental.pallas import tpu as pltpu
from jax.sharding import PartitionSpec as P


F32 = jnp.float32
BF16 = jnp.bfloat16
LANES = 128
TILE = 16
VMEM = pl.BlockSpec(memory_space=pltpu.VMEM)
FAR = pl.BlockSpec(memory_space=pltpu.HBM)


class Sizes:
    def __init__(self, rows, cols, span, waves):
        self.rows, self.cols, self.span, self.waves = rows, cols, span, waves
        self.half = (span - 1) // 2
        self.far = 2 * self.half + 2
        self.near = self.half + 2
        self.lanes = cols + LANES
        self.frame = rows + 5 * TILE
        self.group = -(-span // 3)
        self.pairs = (self.group + 1) // 2
        self.span3 = -(-self.group // 3)
        self.fields = rows + 3 * TILE
        self.up_d = 2 * self.half
        self.up_f = self.half
        self.tail = 2 * self.up_d + 6 * self.up_f
        self.main = self.tail + TILE
        self.payload = self.main + 3 * TILE
        self.slide = self.far + self.near
        far, near = self.far, self.near
        self.slots = (
            ((far, 0, 0), (far, far, far), (near, 2 * far, far + near),
             (near, 2 * far + near, far + 2 * near), (near, 2 * far + 2 * near, far + 3 * near)),
            ((near, 0, 0), (near, near, near), (near, 2 * near, 2 * near), (1, 3 * near, 3 * near)),
        )
        self.edge = rows + rows // 2 + TILE


def lane_of(shape):
    return lax.broadcasted_iota(jnp.int32, shape, len(shape) - 1)


def row_of(shape):
    return lax.broadcasted_iota(jnp.int32, shape, 0)


def border_rows(c):
    return 64 if c == 0 else 48


def turn(k_ref, pad_ref, c, s):
    pad_ref[...] = jnp.zeros((LANES, LANES), F32)
    pad_ref[0 : s.span, 0 : s.span] = k_ref[:, c, :].astype(F32)
    return pad_ref[...].T


def main_tables(k_ref, t_ref, pad_ref, s):
    for c in range(2):
        turned = turn(k_ref, pad_ref, c, s)
        for r in range(2 * s.pairs):
            p, at = divmod(r, 2)
            for q in range(3):
                if r < s.group:
                    b = s.group * q + r
                    row = jnp.broadcast_to(turned[b : b + 1, :], (96, LANES))
                    band = pltpu.roll(row, 0, 1, stride=1, stride_axis=0).astype(BF16)
                else:
                    band = jnp.zeros((96, LANES), BF16)
                t_ref[c, p, q * 96 : (q + 1) * 96, at * LANES : (at + 1) * LANES] = band


def border_tables(t_ref, e_ref, s):
    window = 5 * TILE
    over = 2 * window - LANES
    for c in range(2):
        n = border_rows(c)
        late = 1 - c
        lane = lane_of((n, LANES))
        for g in range(s.span3):
            for q in range(3):
                def piece(at):
                    p, half = divmod(3 * g + at, 2)
                    return t_ref[c, p, 96 * q : 96 * q + n, half * LANES : (half + 1) * LANES]

                first = rolled(piece(0), (-late) % LANES).astype(F32)
                second = rolled(piece(1), window - late).astype(F32)
                third = rolled(piece(2), over - late).astype(F32)
                low = jnp.where(lane < window, first, second)
                high = jnp.where(lane < over, second, third)
                if late:
                    later = row_of(lane.shape) > 0
                    last = s.span - 2
                    low = jnp.where(later | (lane == last) | (lane == last + window), low, 0.0)
                    high = jnp.where(later | (lane == last + over), high, 0.0)
                e_ref[c, g, q * n : (q + 1) * n, :LANES] = low.astype(BF16)
                e_ref[c, g, q * n : (q + 1) * n, LANES:] = high.astype(BF16)


def load_of(tap, wave, s):
    total = jnp.zeros(tap.shape, F32)
    for n in range(s.waves):
        total = jnp.where(tap == n, wave(n), total)
    return total


def first_kernel(v_hbm, i_hbm, r_hbm, cap_hbm, shunt_hbm, tap_hbm, pad_hbm, wave_hbm, k_hbm,
                 one_ref, two_ref, v_ref, i_ref, r_ref, cap_ref, shunt_ref, tap_ref, pad_ref, k_ref, w_ref,
                 wave_ref, sems, *, s):
    sources = (wave_hbm, tap_hbm, pad_hbm, cap_hbm, shunt_hbm, v_hbm, i_hbm, r_hbm, k_hbm)
    targets = (wave_ref, tap_ref, pad_ref, cap_ref, shunt_ref, v_ref, i_ref, r_ref, k_ref)
    copies = [pltpu.make_async_copy(x, y, sems.at[n]) for n, (x, y) in enumerate(zip(sources, targets))]
    for copy in copies:
        copy.start()
    even = lax.rem(lax.axis_index("col"), 2) == 0
    rows, cols = s.rows, s.cols
    shape = (rows, LANES)
    lane, row = lane_of(shape), row_of(shape)

    def ends(ref):
        return jnp.where(lane < LANES // 2, ref[:, :LANES], ref[:, cols - LANES :])

    for copy in copies[:2]:
        copy.wait()
    load = load_of(ends(tap_ref), lambda n: wave_ref[0, n], s)
    for step in range(2):
        for n in range(s.waves):
            w_ref[step, n : n + 1, :] = jnp.full((1, LANES), wave_ref[step, n], F32)
    for copy in copies[2:5]:
        copy.wait()
    keep = ends(pad_ref) != 1
    b = jnp.where(keep, ends(cap_ref), 0.0)
    c = jnp.where(keep, 1.0, 0.0) - b * ends(shunt_ref)
    a = b * load
    for copy in copies[5:]:
        copy.wait()
    volt = ends(v_ref)
    a = a + c * volt
    i0, i1, r0, r1 = ends(i_ref.at[0]), ends(i_ref.at[1]), ends(r_ref.at[0]), ends(r_ref.at[1])
    below = jnp.where(row == rows - 1, 0.0, pltpu.roll(volt, rows - 1, 0))
    beside = jnp.where(lane == LANES - 1, 0.0, pltpu.roll(volt, LANES - 1, 1))
    d0 = (volt - below) - r0 * i0
    d1 = (volt - beside) - r1 * i1
    half = rows // 2

    def put(start, left, right):
        at = slice(start, start + left.shape[0])
        one_ref[at, :] = jnp.where(even, right, left).astype(BF16)
        two_ref[at, :] = jnp.where(even, left, right).astype(BF16)

    for tile, (slots, fields) in enumerate(zip(s.slots, ((d0, d1, i0, i1, r0), (r1, a, b, volt)))):
        left = jnp.zeros(shape, F32)
        right = jnp.zeros(shape, F32)
        for (n, off, back), field in zip(slots, fields):
            x = rolled(field, off)
            left = jnp.where((lane >= off) & (lane < off + n), x, left)
            if n > 1:
                x = x if back == off else rolled(field, back)
                right = jnp.where(before(lane, n, back), x, right)
        if tile == 1:
            left = left[:half] + pltpu.roll(left[half:], LANES // 2, 1)
            right = right[:half] + pltpu.roll(right[half:], LANES // 2, 1)
        put(tile * rows, left, right)
    put(rows + half, v_ref[:TILE, :LANES], v_ref[:TILE, cols - LANES :])


def before(lane, n, off):
    if off >= n:
        return (lane >= off - n) & (lane < off)
    return (lane < off) | (lane >= LANES + off - n)


def own_kernel(v_ref, i_ref, r_ref, cap_ref, shunt_ref, tap_ref, pad_ref, k_ref, w_ref,
               d_ref, a_ref, b_ref, c_ref, e_ref, t_ref, bor_ref, square_ref, *, s):
    main_tables(k_ref, t_ref, square_ref, s)
    border_tables(t_ref, bor_ref, s)
    volt = v_ref[...]
    rows, cols = volt.shape
    below = jnp.where(row_of(volt.shape) == rows - 1, 0.0, pltpu.roll(volt, rows - 1, 0))
    beside = jnp.where(lane_of(volt.shape) == cols - 1, 0.0, pltpu.roll(volt, cols - 1, 1))
    d_ref[0] = ((volt - below) - r_ref[0] * i_ref[0]).astype(BF16)
    d_ref[1] = ((volt - beside) - r_ref[1] * i_ref[1]).astype(BF16)
    keep = pad_ref[...] != 1
    b = jnp.where(keep, cap_ref[...], 0.0)
    c = jnp.where(keep, 1.0, 0.0) - b * shunt_ref[...]
    b_ref[...], c_ref[...] = b, c
    for at in range(0, cols, LANES):
        at = slice(at, at + LANES)
        first, second = [load_of(tap_ref[:, at], lambda n: w_ref[step, n : n + 1, :], s) for step in range(2)]
        a_ref[:, at] = c[:, at] * volt[:, at] + b[:, at] * first
        e_ref[:, at] = b[:, at] * second


def second_kernel(d_ref, v_ref, i_ref, r_ref, a_ref, b_ref, one_ref, two_ref,
                  df_ref, t_ref, up_ref, down_ref, *, s):
    even = lax.rem(lax.axis_index("col"), 2) == 0
    rows, cols = v_ref.shape
    lane = lane_of((rows, LANES))
    half = rows // 2
    index, count = lax.axis_index("col"), lax.axis_size("col")

    def get(start, size):
        at = slice(start, start + size)
        one, two = one_ref[at, :].astype(F32), two_ref[at, :].astype(F32)
        right, left = jnp.where(even, one, two), jnp.where(even, two, one)
        return jnp.where(index < count - 1, right, 0.0), jnp.where(index > 0, left, 0.0)

    sides = []
    for tile, slots in enumerate(s.slots):
        if tile == 0:
            pair = get(0, rows)
        else:
            pair = [jnp.concatenate([x, pltpu.roll(x, LANES // 2, 1)], 0) for x in get(rows, half)]
        for n, off, back in slots:
            if back == off:
                x = jnp.where((lane >= off) & (lane < off + n), pair[0], pair[1])
                x = rolled(x, (LANES - off) % LANES)
                sides.append(jnp.where((lane < n) | (lane >= LANES - n), x, 0.0))
            else:
                x, y = rolled(pair[0], LANES - off), rolled(pair[1], LANES - back)
                sides.append(jnp.where(lane < n, x, jnp.where(lane >= LANES - n, y, 0.0)))
    d0s, d1s, i0s, i1s, r0s, r1s, as_, bs, vs = sides
    x, y = get(rows + half, TILE)
    first = lane_of((TILE, LANES))
    corner = jnp.where(first < s.far, x, jnp.where(first >= LANES - s.far, y, 0.0))
    edge = lane == LANES - 1
    next_side = pltpu.roll(vs, LANES - 1, 1)
    next_own = pltpu.roll(v_ref[:, :LANES], LANES - 1, 1)
    d1 = d_ref[1]
    tail = d1[:, cols - LANES :].astype(F32)
    tail = jnp.where(edge, tail - next_side, tail).astype(BF16)
    d1s = jnp.where(edge, jnp.where(r1s > 0, d1s - next_own, 0.0), d1s).astype(BF16)
    df_ref[0, :, :cols] = d_ref[0]
    df_ref[0, :, cols:] = d0s.astype(BF16)
    df_ref[1, :, : cols - LANES] = d1[:, : cols - LANES]
    df_ref[1, :, cols - LANES : cols] = tail
    df_ref[1, :, cols:] = d1s
    for n, x in enumerate((i0s, i1s, r0s, r1s, as_, bs)):
        t_ref[n] = x.astype(BF16)
    t_ref[6, :TILE, :] = corner.astype(BF16)
    above = lax.rem(lax.axis_index("row"), 2) == 0

    own = (i_ref.at[0], i_ref.at[1], r_ref.at[0], r_ref.at[1], a_ref, b_ref)

    def rows_of(n, start, size):
        if n < 2:
            at = start // TILE * TILE
            x = df_ref[n, at : at + TILE, :].astype(F32)
            return x[start - at : start - at + size]
        source = v_ref if n == 8 else own[n - 2]
        at = start // TILE * TILE
        x = t_ref[n - 2, at : at + TILE, :].astype(F32)
        return jnp.concatenate([source[start : start + size, :], x[start - at : start - at + size]], 1)

    lane16 = lane_of((TILE, LANES))
    wide = (lane16 < s.far) | (lane16 >= LANES - s.far)

    def pack(ref, down):
        at = 0
        dstart = rows - s.up_d if down else 0
        fstart = rows - s.up_f if down else 0

        def corner(k, x):
            ref[s.main + k // 2 * TILE : s.main + (k // 2 + 1) * TILE, k % 2 * LANES : (k % 2 + 1) * LANES] = x.astype(BF16)

        def field_side(n):
            return t_ref[n, fstart : fstart + s.up_f, :].astype(F32)

        for c in range(2):
            ref[at : at + s.up_d, :] = df_ref[c, dstart : dstart + s.up_d, :cols]
            at += s.up_d
            for h in range(2):
                x = df_ref[c, dstart + h * TILE : dstart + (h + 1) * TILE, cols:].astype(F32)
                corner(2 * c + h, jnp.where(wide, x, pltpu.roll(field_side(2 * c + h), s.slide, 1)))
        for field in own:
            ref[at : at + s.up_f, :] = field[fstart : fstart + s.up_f, :].astype(BF16)
            at += s.up_f
        corner(4, jnp.where(wide, field_side(4), pltpu.roll(field_side(5), s.slide, 1)))
        eight = row_of((8, s.lanes))
        halves = [jnp.zeros((8, s.lanes), F32), jnp.zeros((8, s.lanes), F32)]
        for n in range(8):
            width = s.up_d if n < 2 else s.up_f
            slot = 2 * n % 8
            if down:
                x = pltpu.roll(rows_of(n, rows - width - 8, 8), (slot + 2) % 8, 0)
            else:
                x = pltpu.roll(rows_of(n, width, 8), slot, 0)
            keep = (eight == slot) | (eight == slot + 1)
            halves[n // 4] = jnp.where(keep, x, halves[n // 4])
        if not down:
            x = pltpu.roll(rows_of(8, 0, 8), 1, 0)
            halves[0] = jnp.where(eight == 1, x, halves[0])
        extra = jnp.concatenate(halves, 0)
        ref[at : at + TILE, :] = extra[:, :cols].astype(BF16)
        corner(5, extra[:, cols:])

    @pl.when(above)
    def _():
        pack(up_ref, True)
        pack(down_ref, False)

    @pl.when(jnp.logical_not(above))
    def _():
        pack(up_ref, False)
        pack(down_ref, True)


def convolve(d_ref, t_ref, c, s, second=range(3, 11), low=0):
    tiles = s.frame // TILE
    lanes = s.lanes
    first = [t % tiles for t in range(-3, 5)]
    high = 96 - low
    acc = [jnp.zeros((3 * high, 2 * LANES), F32) for _ in range(3)]
    for p in range(s.pairs):
        rhs1, rhs2, rhs3 = [], [], []
        for r in (2 * p, 2 * p + 1):
            shift = (s.half - s.group - r) % lanes if r < s.group else 0
            x = d_ref[c]
            x = pltpu.roll(x, shift, 1) if shift else x
            rhs1 += [x[t * TILE : (t + 1) * TILE, : s.cols] for t in first]
            rhs2 += [x[t * TILE : (t + 1) * TILE, : s.cols] for t in second]
            rhs3 += [jnp.concatenate([x[t * TILE : (t + 1) * TILE, s.cols :], x[u * TILE : (u + 1) * TILE, s.cols :]], 1)
                     for t, u in zip(first, second)]
        lhs = jnp.concatenate([t_ref[c, p, 96 * q + low : 96 * q + 96, :] for q in range(3)], 0)
        for n, rhs in enumerate((rhs1, rhs2, rhs3)):
            acc[n] = acc[n] + jnp.dot(lhs, jnp.concatenate(rhs, 0), preferred_element_type=F32)

    def total(n, start, stop):
        parts = []
        for q in range(3):
            at = slice(high * q + start - low, high * q + stop - low)
            x = jnp.concatenate([acc[n][at], acc[2][at, n * LANES : (n + 1) * LANES]], 1)
            shift = (s.group - s.group * q) % lanes
            parts.append(pltpu.roll(x, shift, 1) if shift else x)
        return parts[0] + parts[1] + parts[2]

    return total


def rolled(x, shift):
    return pltpu.roll(x, shift, 1) if shift else x


def gather(acc, n, high, start, stop, s):
    parts = []
    for q in range(3):
        at = slice(high * q + start, high * q + stop)
        side = acc[2][at, n * LANES : (n + 1) * LANES]
        parts.append(rolled(jnp.concatenate([acc[n][at], side], 1), (s.group - s.group * q) % s.lanes))
    return parts[0] + parts[1] + parts[2]


def middle_kernel(df_ref, i_ref, r_ref, a_ref, b_ref, side_ref, tab_ref,
                  if_ref, rf_ref, af_ref, bf_ref, x_ref, z_ref, *, s):
    rows, cols, lanes = s.rows, s.cols, s.lanes
    own = (i_ref.at[0], i_ref.at[1], r_ref.at[0], r_ref.at[1], a_ref, b_ref)
    frames = (if_ref.at[0], if_ref.at[1], rf_ref.at[0], rf_ref.at[1], af_ref, bf_ref)
    for n, (src, dst) in enumerate(zip(own, frames)):
        dst[0:rows, :cols] = src[...]
        dst[0:rows, cols:] = side_ref[n].astype(F32)
    z_ref[...] = df_ref[...]
    end = z_ref[0, rows - TILE :, :]
    z_ref[0, rows - TILE :, :] = jnp.where(row_of(end.shape) == TILE - 1, 0.0, end.astype(F32)).astype(BF16)
    for c in range(2):
        acc = [jnp.zeros((288, cols), F32), None, jnp.zeros((288, LANES), F32)]
        for p in range(s.pairs):
            pieces = []
            for r in (2 * p, 2 * p + 1):
                if r < s.group:
                    x = rolled(z_ref[c], (s.half - s.group - r) % lanes)
                    x_ref[c, r, 0 : 2 * TILE, :] = x[0 : 2 * TILE]
                    x_ref[c, r, 2 * TILE :, :] = x[rows - 2 * TILE :]
                pieces.append(x)
            rhs = jnp.concatenate(pieces, 0)
            acc[0] = acc[0] + jnp.dot(tab_ref[c, p], rhs[:, :cols], preferred_element_type=F32)
            acc[2] = acc[2] + jnp.dot(tab_ref[c, p], rhs[:, cols:], preferred_element_type=F32)
        at = slice(s.half, rows - s.half)
        total = gather(acc, 0, 96, 0, 96, s)
        if_ref[c, at, :] = jnp.where(rf_ref[c, at, :] > 0, if_ref[c, at, :] + total, 0.0)


def border(d_ref, x_ref, e_ref, c, s):
    n = border_rows(c)
    acc = [jnp.zeros((3 * n, 2 * LANES), F32) for _ in range(3)]
    rows, lanes, cols = s.rows, s.lanes, s.cols
    for g in range(s.span3):
        tops, bottoms = [], []
        for at in range(3):
            r = 3 * g + at
            r = r if r < s.group else 0
            shift = (s.half - s.group - r) % lanes
            outer = rolled(d_ref[c, rows : s.frame, :], shift)
            start, stop = x_ref[c, r, 0 : 2 * TILE, :], x_ref[c, r, 2 * TILE :, :]
            if c == 0:
                stop = jnp.concatenate([stop[:TILE], rolled(d_ref[c, rows - TILE : rows, :], shift)], 0)
            top = jnp.concatenate([outer[2 * TILE :], start], 0)
            bottom = jnp.concatenate([stop, outer[: 3 * TILE]], 0)
            tops.append(top)
            bottoms.append(bottom)
        tops.append(tops[0][:TILE])
        bottoms.append(bottoms[0][:TILE])
        top, bottom = jnp.concatenate(tops, 0), jnp.concatenate(bottoms, 0)
        strip = jnp.concatenate([top[:, cols:], bottom[:, cols:]], 1)
        lhs = e_ref[c, g, 0 : 3 * n, :]
        for k, rhs in enumerate((top[:, :cols], bottom[:, :cols], strip)):
            acc[k] = acc[k] + jnp.dot(lhs, rhs, preferred_element_type=F32)
    return [gather(acc, k, n, 0, n, s) for k in range(2)]


def last_kernel(df_ref, v_ref, b_ref, c_ref, e_ref, side_ref, tab_ref, bor_ref, x_ref, one_ref, two_ref,
                if_in, rf_in, af_in, bf_in, vo_hbm, io_hbm, if_ref, rf_ref, af_ref, bf_ref,
                d_ref, vf_ref, vo_ref, io_ref, sems, *, s):
    even = lax.rem(lax.axis_index("row"), 2) == 0
    rows, cols, frame, lanes = s.rows, s.cols, s.frame, s.lanes
    index = lax.axis_index("row")
    low = jnp.where(even, one_ref[...], two_ref[...])
    high = jnp.where(even, two_ref[...], one_ref[...])
    low = jnp.where(index < lax.axis_size("row") - 1, low, jnp.zeros_like(low))
    high = jnp.where(index > 0, high, jnp.zeros_like(high))
    ud, uf, full = s.up_d, s.up_f, s.fields
    lane = lane_of((TILE, LANES))

    def corner(x, k):
        return x[s.main + k // 2 * TILE : s.main + (k // 2 + 1) * TILE, k % 2 * LANES : (k % 2 + 1) * LANES].astype(F32)

    def rest(x):
        return jnp.concatenate([x[s.tail : s.main, :].astype(F32), corner(x, 5)], 1)

    def field(x, n):
        at = 2 * ud + n * uf
        side = corner(x, min(n, 4))
        if n != 4:
            side = pltpu.roll(side, LANES - s.slide, 1)
        side = jnp.where((lane < s.near) | (lane >= LANES - s.near), side, 0.0)
        return jnp.concatenate([x[at : at + uf, :].astype(F32), side], 1)

    def driving(x, c):
        sides = [jnp.where((lane < s.far) | (lane >= LANES - s.far), corner(x, 2 * c + h), 0.0) for h in range(2)]
        return jnp.concatenate([x[c * ud : (c + 1) * ud, :], jnp.concatenate(sides, 0).astype(BF16)], 1)

    low_rest, high_rest = rest(low), rest(high)
    eight = row_of((8, lanes))
    frames = (if_ref.at[0], if_ref.at[1], rf_ref.at[0], rf_ref.at[1], af_ref, bf_ref)
    for n, dst in enumerate(frames):
        half, slot = divmod(4 + 2 * n, 8)
        extra_low = pltpu.roll(low_rest[8 * half : 8 * half + 8], (8 - slot) % 8, 0)
        extra_high = pltpu.roll(high_rest[8 * half : 8 * half + 8], 6 - slot, 0)
        dst[rows : rows + uf, :] = field(low, n)
        dst[rows + uf : rows + uf + 8, :] = jnp.where(eight == 0, extra_low, 0.0)
        dst[full - uf - 8 : full - uf, :] = jnp.where(eight >= 6, extra_high, 0.0)
        dst[full - uf : full, :] = field(high, n)
    v_next = low_rest[1:2, :]
    v_first = jnp.concatenate([v_ref[0:8, :][0:1, :], side_ref[6, 0:TILE, :].astype(F32)[0:1, :]], 1)
    gap = rows + ud
    shape = (TILE, lanes)
    for c in range(2):
        d_ref[c, 0:rows, :] = df_ref[c]
        d_ref[c, rows:gap, :] = driving(low, c)
        d_ref[c, gap + TILE :, :] = driving(high, c)
        extra_low = pltpu.roll(low_rest[0:8], (8 - 2 * c) % 8, 0)
        extra_high = pltpu.roll(high_rest[0:8], 6 - 2 * c, 0)
        d_ref[c, gap : gap + TILE, :] = jnp.concatenate(
            [jnp.where(eight == 0, extra_low, 0.0), jnp.where(eight >= 6, extra_high, 0.0)], 0).astype(BF16)
    last = row_of(shape) == TILE - 1
    x = d_ref[0, rows - TILE : rows, :].astype(F32)
    d_ref[0, rows - TILE : rows, :] = jnp.where(last, x - v_next, x).astype(BF16)
    x = d_ref[0, frame - TILE :, :].astype(F32)
    inside = rf_ref[0, full - TILE :, :] > 0
    d_ref[0, frame - TILE :, :] = jnp.where(last, jnp.where(inside, x - v_first, 0.0), x).astype(BF16)

    for c in range(2):
        top, bottom = border(d_ref, x_ref, bor_ref, c, s)
        n = border_rows(c)
        pieces = []
        if c == 0:
            pieces.append((rows - 24, jnp.where(eight == 7, jnp.broadcast_to(bottom[0:1], (8, lanes)), 0.0)))
            top, bottom = pltpu.roll(top, n - 1, 0), pltpu.roll(bottom, n - 1, 0)
        pieces += [(full - 24, top[8:32]), (0, top[32:48]), (rows - TILE, bottom[0:40])]
        for dst, add in pieces:
            at = slice(dst, dst + add.shape[0])
            if_ref[c, at, :] = jnp.where(rf_ref[c, at, :] > 0, if_ref[c, at, :] + add, 0.0)
    i0, i1 = if_ref[0], if_ref[1]
    div = i0 - pltpu.roll(i0, 1, 0) + i1 - pltpu.roll(i1, 1, 1)
    volt = af_ref[...] - bf_ref[...] * div
    vf_ref[...] = volt
    drop0 = volt - pltpu.roll(volt, full - 1, 0)
    drop1 = volt - pltpu.roll(volt, lanes - 1, 1)
    r0, r1 = rf_ref[0], rf_ref[1]
    for c, (drop, r, i) in enumerate(((drop0, r0, i0), (drop1, r1, i1))):
        x = jnp.where(r > 0, drop - r * i, 0.0).astype(BF16)
        d_ref[c, 0 : rows + TILE, :] = x[0 : rows + TILE]
        d_ref[c, frame - 2 * TILE :, :] = x[full - 2 * TILE :]

    total = convolve(d_ref, tab_ref, 0, s, range(1, 9), 16)
    above = jnp.where(rf_ref[0, full - 8 :, :] > 0, if_ref[0, full - 8 :, :] + total(0, 24, 32), 0.0)[7:8, :cols]
    for n in range(2):
        at = slice(64 * n, 64 * n + 64)
        io_ref[0, at, :] = (if_ref[0, at, :] + total(n, 32, 96))[:, :cols]
    out0 = pltpu.make_async_copy(io_ref.at[0], io_hbm.at[0], sems.at[0])
    out0.start()
    total = convolve(d_ref, tab_ref, 1, s, range(1, 9), 32)
    ends = jnp.concatenate([total(0, 32, 96), total(1, 32, 96)], 0)
    ends = jnp.where(rf_ref[1, 0:rows, :] > 0, if_ref[1, 0:rows, :] + ends, 0.0)
    io_ref[1] = ends[:, :cols]
    out1 = pltpu.make_async_copy(io_ref.at[1], io_hbm.at[1], sems.at[1])
    out1.start()
    side = ends[:, cols:]
    i0, i1 = io_ref[0], io_ref[1]
    up = jnp.where(row_of((rows, cols)) == 0, above, pltpu.roll(i0, 1, 0))
    left = pltpu.roll(jnp.concatenate([i1, side], 1), 1, 1)[:, :cols]
    div = i0 - up + i1 - left
    vo_ref[...] = c_ref[...] * vf_ref[0:rows, :cols] + e_ref[...] - b_ref[...] * div
    out2 = pltpu.make_async_copy(vo_ref, vo_hbm, sems.at[2])
    out2.start()
    for copy in (out0, out1, out2):
        copy.wait()


def swapped(x, axis, odd):
    sizes = lax.axis_size("row"), lax.axis_size("col")
    main = ("row", "col").index(axis)
    to = {}
    for at in itertools.product(range(sizes[0]), range(sizes[1])):
        along, other = at[main], at[1 - main]
        if along >= odd and (along ^ 1 if not odd else ((along - 1) ^ 1) + 1) < sizes[main]:
            along = along ^ 1 if not odd else ((along - 1) ^ 1) + 1
        elif other ^ 1 < sizes[1 - main]:
            other = other ^ 1
        else:
            continue
        there = (along, other) if main == 0 else (other, along)
        to[at[0] * sizes[1] + at[1]] = there[0] * sizes[1] + there[1]
    return lax.ppermute(x, ("row", "col"), list(to.items()))


def near(x):
    return pltpu.with_memory_space_constraint(x, pltpu.VMEM)


def call(kernel, outs, ins, scratch=(), specs=None, limit=16, out_specs=None, aliases=None):
    return pl.pallas_call(
        kernel,
        compiler_params=pltpu.CompilerParams(vmem_limit_bytes=limit << 20),
        out_shape=outs,
        in_specs=specs or [VMEM] * len(ins),
        out_specs=out_specs or jax.tree.map(lambda _: VMEM, outs),
        scratch_shapes=scratch,
        input_output_aliases=aliases or {},
    )(*ins)


def local(voltage, currents, resistance, inverse_cap, shunt, tap, pad, waveforms, k_window):
    rows, cols = voltage.shape
    s = Sizes(rows, cols, k_window.shape[1], waveforms.shape[1])
    sds = pltpu.VMEM
    k_window = k_window.transpose(1, 0, 2)
    block = sds((rows, cols), F32)
    half = sds((s.edge, LANES), BF16)
    pair = sds((2, rows, cols), F32)
    whole = sds((rows, cols), jnp.int32)
    one, two, v_near, i_near, r_near, cap_near, shunt_near, tap_near, pad_near, k_near, w_near = call(
        functools.partial(first_kernel, s=s),
        (half, half, block, pair, pair, block, block, whole, whole, sds(k_window.shape, BF16),
         sds((2, s.waves, LANES), F32)),
        [pltpu.with_memory_space_constraint(x, pltpu.HBM)
         for x in (voltage, currents, resistance, inverse_cap, shunt, tap, pad, waveforms, k_window)],
        specs=[FAR] * 9,
        scratch=[pltpu.SMEM(waveforms.shape, F32), pltpu.SemaphoreType.DMA((9,))])
    square = pltpu.VMEM((LANES, LANES), F32)
    d, a, b, c, e, tables, borders = call(
        functools.partial(own_kernel, s=s),
        (sds((2, rows, cols), BF16), block, block, block, block, sds((2, s.pairs, 288, 2 * LANES), BF16),
         sds((2, s.span3, 192, 2 * LANES), BF16)),
        (v_near, i_near, r_near, cap_near, shunt_near, tap_near, pad_near, k_near, w_near),
        scratch=[square])
    one, two = near(swapped(one, "col", 0)), near(swapped(two, "col", 1))
    pay = sds((s.payload, cols), BF16)
    df, side, one, two = call(
        functools.partial(second_kernel, s=s),
        (sds((2, rows, s.lanes), BF16), sds((7, rows, LANES), BF16), pay, pay),
        (d, v_near, i_near, r_near, a, b, one, two))
    one, two = swapped(one, "row", 0), swapped(two, "row", 1)
    f = sds((s.fields, s.lanes), F32)
    f2 = sds((2, s.fields, s.lanes), F32)
    i_frame, r_frame, a_frame, b_frame, shifted = call(
        functools.partial(middle_kernel, s=s),
        (f2, f2, f, f, sds((2, s.group, 4 * TILE, s.lanes), BF16)),
        (df, i_near, r_near, a, b, side, tables),
        scratch=[pltpu.VMEM((2, rows, s.lanes), BF16)])
    outs = call(
        functools.partial(last_kernel, s=s),
        (jax.ShapeDtypeStruct((rows, cols), F32), jax.ShapeDtypeStruct((2, rows, cols), F32), f2, f2, f, f),
        (df, v_near, b, c, e, side, tables, borders, shifted, near(one), near(two), i_frame, r_frame, a_frame, b_frame),
        scratch=[pltpu.VMEM((2, s.frame, s.lanes), BF16), pltpu.VMEM((s.fields, s.lanes), F32),
                 pltpu.VMEM((rows, cols), F32), pltpu.VMEM((2, rows, cols), F32), pltpu.SemaphoreType.DMA((3,))],
        out_specs=(FAR, FAR, VMEM, VMEM, VMEM, VMEM), aliases={11: 2, 12: 3, 13: 4, 14: 5})
    return outs[0], outs[1]


def solution(mesh):
    grid = P("row", "col")
    pair = P(None, "row", "col")

    return jax.shard_map(
        local,
        mesh=mesh,
        in_specs=(grid, pair, pair, grid, grid, grid, grid, P(), P()),
        out_specs=(grid, pair),
        check_vma=False,
    )
```

```python
import functools
import itertools

import jax
import jax.numpy as jnp
from jax import lax
from jax.experimental import pallas as pl
from jax.experimental.pallas import tpu as pltpu
from jax.sharding import PartitionSpec as P


F32 = jnp.float32
BF16 = jnp.bfloat16
LANES = 128
TILE = 16
VMEM = pl.BlockSpec(memory_space=pltpu.VMEM)
FAR = pl.BlockSpec(memory_space=pltpu.HBM)


class Sizes:
    def __init__(self, rows, cols, span, waves):
        self.rows, self.cols, self.span, self.waves = rows, cols, span, waves
        self.half = (span - 1) // 2
        self.far = 2 * self.half + 2
        self.near = self.half + 2
        self.lanes = cols + LANES
        self.frame = rows + 5 * TILE
        self.group = -(-span // 3)
        self.pairs = (self.group + 1) // 2
        self.span3 = -(-self.group // 3)
        self.fields = rows + 3 * TILE
        self.up_d = 2 * self.half
        self.up_f = self.half
        self.tail = 2 * self.up_d + 6 * self.up_f
        self.main = self.tail + TILE
        self.payload = self.main + 3 * TILE
        self.slide = self.far + self.near
        far, near = self.far, self.near
        self.slots = (
            ((far, 0, 0), (far, far, far), (near, 2 * far, far + near),
             (near, 2 * far + near, far + 2 * near), (near, 2 * far + 2 * near, far + 3 * near)),
            ((near, 0, 0), (near, near, near), (near, 2 * near, 2 * near), (1, 3 * near, 3 * near)),
        )
        self.edge = rows + rows // 2 + TILE


def lane_of(shape):
    return lax.broadcasted_iota(jnp.int32, shape, len(shape) - 1)


def row_of(shape):
    return lax.broadcasted_iota(jnp.int32, shape, 0)


def border_rows(c):
    return 64 if c == 0 else 48


def turn(k_ref, pad_ref, c, s):
    pad_ref[...] = jnp.zeros((LANES, LANES), F32)
    pad_ref[0 : s.span, 0 : s.span] = k_ref[:, c, :].astype(F32)
    return pad_ref[...].T


def main_tables(k_ref, t_ref, pad_ref, s):
    for c in range(2):
        turned = turn(k_ref, pad_ref, c, s)
        for r in range(2 * s.pairs):
            p, at = divmod(r, 2)
            for q in range(3):
                if r < s.group:
                    b = s.group * q + r
                    row = jnp.broadcast_to(turned[b : b + 1, :], (96, LANES))
                    band = pltpu.roll(row, 0, 1, stride=1, stride_axis=0).astype(BF16)
                else:
                    band = jnp.zeros((96, LANES), BF16)
                t_ref[c, p, q * 96 : (q + 1) * 96, at * LANES : (at + 1) * LANES] = band


def border_tables(t_ref, e_ref, s):
    window = 5 * TILE
    over = 2 * window - LANES
    for c in range(2):
        n = border_rows(c)
        late = 1 - c
        lane = lane_of((n, LANES))
        for g in range(s.span3):
            for q in range(3):
                def piece(at):
                    p, half = divmod(3 * g + at, 2)
                    return t_ref[c, p, 96 * q : 96 * q + n, half * LANES : (half + 1) * LANES]

                first = rolled(piece(0), (-late) % LANES).astype(F32)
                second = rolled(piece(1), window - late).astype(F32)
                third = rolled(piece(2), over - late).astype(F32)
                low = jnp.where(lane < window, first, second)
                high = jnp.where(lane < over, second, third)
                if late:
                    later = row_of(lane.shape) > 0
                    last = s.span - 2
                    low = jnp.where(later | (lane == last) | (lane == last + window), low, 0.0)
                    high = jnp.where(later | (lane == last + over), high, 0.0)
                e_ref[c, g, q * n : (q + 1) * n, :LANES] = low.astype(BF16)
                e_ref[c, g, q * n : (q + 1) * n, LANES:] = high.astype(BF16)


def load_of(tap, wave, s):
    total = jnp.zeros(tap.shape, F32)
    for n in range(s.waves):
        total = jnp.where(tap == n, wave(n), total)
    return total


def first_kernel(v_hbm, i_hbm, r_hbm, cap_hbm, shunt_hbm, tap_hbm, pad_hbm, wave_hbm, k_hbm,
                 one_ref, two_ref, v_ref, i_ref, r_ref, cap_ref, shunt_ref, tap_ref, pad_ref, k_ref, w_ref,
                 wave_ref, sems, *, s):
    sources = (v_hbm, r_hbm, i_hbm, wave_hbm, tap_hbm, pad_hbm, cap_hbm, shunt_hbm, k_hbm)
    targets = (v_ref, r_ref, i_ref, wave_ref, tap_ref, pad_ref, cap_ref, shunt_ref, k_ref)
    copies = [pltpu.make_async_copy(x, y, sems.at[n]) for n, (x, y) in enumerate(zip(sources, targets))]
    for copy in copies:
        copy.start()
    even = lax.rem(lax.axis_index("col"), 2) == 0
    rows, cols = s.rows, s.cols
    shape = (rows, LANES)
    lane, row = lane_of(shape), row_of(shape)

    def ends(ref):
        return jnp.where(lane < LANES // 2, ref[:, :LANES], ref[:, cols - LANES :])

    for copy in copies[:3]:
        copy.wait()
    volt = ends(v_ref)
    i0, i1, r0, r1 = ends(i_ref.at[0]), ends(i_ref.at[1]), ends(r_ref.at[0]), ends(r_ref.at[1])
    below = jnp.where(row == rows - 1, 0.0, pltpu.roll(volt, rows - 1, 0))
    beside = jnp.where(lane == LANES - 1, 0.0, pltpu.roll(volt, LANES - 1, 1))
    d0 = (volt - below) - r0 * i0
    d1 = (volt - beside) - r1 * i1
    half = rows // 2

    def put(start, left, right):
        at = slice(start, start + left.shape[0])
        one_ref[at, :] = jnp.where(even, right, left).astype(BF16)
        two_ref[at, :] = jnp.where(even, left, right).astype(BF16)

    def slotted(slots, fields):
        left = jnp.zeros(shape, F32)
        right = jnp.zeros(shape, F32)
        for (n, off, back), field in zip(slots, fields):
            x = rolled(field, off)
            left = jnp.where((lane >= off) & (lane < off + n), x, left)
            if n > 1:
                x = x if back == off else rolled(field, back)
                right = jnp.where(before(lane, n, back), x, right)
        return left, right

    put(0, *slotted(s.slots[0], (d0, d1, i0, i1, r0)))
    put(rows + half, v_ref[:TILE, :LANES], v_ref[:TILE, cols - LANES :])
    for copy in copies[3:]:
        copy.wait()
    for step in range(2):
        for n in range(s.waves):
            w_ref[step, n : n + 1, :] = jnp.full((1, LANES), wave_ref[step, n], F32)
    load = load_of(ends(tap_ref), lambda n: wave_ref[0, n], s)
    keep = ends(pad_ref) != 1
    b = jnp.where(keep, ends(cap_ref), 0.0)
    c = jnp.where(keep, 1.0, 0.0) - b * ends(shunt_ref)
    volt = ends(v_ref)
    a = b * load + c * volt
    folded = [x[:half] + pltpu.roll(x[half:], LANES // 2, 1)
              for x in slotted(s.slots[1], (ends(r_ref.at[1]), a, b, volt))]
    put(rows, *folded)


def before(lane, n, off):
    if off >= n:
        return (lane >= off - n) & (lane < off)
    return (lane < off) | (lane >= LANES + off - n)


def own_kernel(v_ref, i_ref, r_ref, cap_ref, shunt_ref, tap_ref, pad_ref, k_ref, w_ref,
               d_ref, a_ref, b_ref, c_ref, e_ref, t_ref, bor_ref, square_ref, *, s):
    main_tables(k_ref, t_ref, square_ref, s)
    border_tables(t_ref, bor_ref, s)
    volt = v_ref[...]
    rows, cols = volt.shape
    below = jnp.where(row_of(volt.shape) == rows - 1, 0.0, pltpu.roll(volt, rows - 1, 0))
    beside = jnp.where(lane_of(volt.shape) == cols - 1, 0.0, pltpu.roll(volt, cols - 1, 1))
    d_ref[0] = ((volt - below) - r_ref[0] * i_ref[0]).astype(BF16)
    d_ref[1] = ((volt - beside) - r_ref[1] * i_ref[1]).astype(BF16)
    keep = pad_ref[...] != 1
    b = jnp.where(keep, cap_ref[...], 0.0)
    c = jnp.where(keep, 1.0, 0.0) - b * shunt_ref[...]
    b_ref[...], c_ref[...] = b, c
    for at in range(0, cols, LANES):
        at = slice(at, at + LANES)
        first, second = [load_of(tap_ref[:, at], lambda n: w_ref[step, n : n + 1, :], s) for step in range(2)]
        a_ref[:, at] = c[:, at] * volt[:, at] + b[:, at] * first
        e_ref[:, at] = b[:, at] * second


def second_kernel(d_ref, v_ref, i_ref, r_ref, a_ref, b_ref, one_ref, two_ref,
                  df_ref, t_ref, up_ref, down_ref, *, s):
    even = lax.rem(lax.axis_index("col"), 2) == 0
    rows, cols = v_ref.shape
    lane = lane_of((rows, LANES))
    half = rows // 2
    index, count = lax.axis_index("col"), lax.axis_size("col")

    def get(start, size):
        at = slice(start, start + size)
        one, two = one_ref[at, :].astype(F32), two_ref[at, :].astype(F32)
        right, left = jnp.where(even, one, two), jnp.where(even, two, one)
        return jnp.where(index < count - 1, right, 0.0), jnp.where(index > 0, left, 0.0)

    sides = []
    for tile, slots in enumerate(s.slots):
        if tile == 0:
            pair = get(0, rows)
        else:
            pair = [jnp.concatenate([x, pltpu.roll(x, LANES // 2, 1)], 0) for x in get(rows, half)]
        for n, off, back in slots:
            if back == off:
                x = jnp.where((lane >= off) & (lane < off + n), pair[0], pair[1])
                x = rolled(x, (LANES - off) % LANES)
                sides.append(jnp.where((lane < n) | (lane >= LANES - n), x, 0.0))
            else:
                x, y = rolled(pair[0], LANES - off), rolled(pair[1], LANES - back)
                sides.append(jnp.where(lane < n, x, jnp.where(lane >= LANES - n, y, 0.0)))
    d0s, d1s, i0s, i1s, r0s, r1s, as_, bs, vs = sides
    x, y = get(rows + half, TILE)
    first = lane_of((TILE, LANES))
    corner = jnp.where(first < s.far, x, jnp.where(first >= LANES - s.far, y, 0.0))
    edge = lane == LANES - 1
    next_side = pltpu.roll(vs, LANES - 1, 1)
    next_own = pltpu.roll(v_ref[:, :LANES], LANES - 1, 1)
    d1 = d_ref[1]
    tail = d1[:, cols - LANES :].astype(F32)
    tail = jnp.where(edge, tail - next_side, tail).astype(BF16)
    d1s = jnp.where(edge, jnp.where(r1s > 0, d1s - next_own, 0.0), d1s).astype(BF16)
    df_ref[0, :, :cols] = d_ref[0]
    df_ref[0, :, cols:] = d0s.astype(BF16)
    df_ref[1, :, : cols - LANES] = d1[:, : cols - LANES]
    df_ref[1, :, cols - LANES : cols] = tail
    df_ref[1, :, cols:] = d1s
    for n, x in enumerate((i0s, i1s, r0s, r1s, as_, bs)):
        t_ref[n] = x.astype(BF16)
    t_ref[6, :TILE, :] = corner.astype(BF16)
    above = lax.rem(lax.axis_index("row"), 2) == 0

    own = (i_ref.at[0], i_ref.at[1], r_ref.at[0], r_ref.at[1], a_ref, b_ref)

    def rows_of(n, start, size):
        if n < 2:
            at = start // TILE * TILE
            x = df_ref[n, at : at + TILE, :].astype(F32)
            return x[start - at : start - at + size]
        source = v_ref if n == 8 else own[n - 2]
        at = start // TILE * TILE
        x = t_ref[n - 2, at : at + TILE, :].astype(F32)
        return jnp.concatenate([source[start : start + size, :], x[start - at : start - at + size]], 1)

    lane16 = lane_of((TILE, LANES))
    wide = (lane16 < s.far) | (lane16 >= LANES - s.far)

    def pack(ref, down):
        at = 0
        dstart = rows - s.up_d if down else 0
        fstart = rows - s.up_f if down else 0

        def corner(k, x):
            ref[s.main + k // 2 * TILE : s.main + (k // 2 + 1) * TILE, k % 2 * LANES : (k % 2 + 1) * LANES] = x.astype(BF16)

        def field_side(n):
            return t_ref[n, fstart : fstart + s.up_f, :].astype(F32)

        for c in range(2):
            ref[at : at + s.up_d, :] = df_ref[c, dstart : dstart + s.up_d, :cols]
            at += s.up_d
            for h in range(2):
                x = df_ref[c, dstart + h * TILE : dstart + (h + 1) * TILE, cols:].astype(F32)
                corner(2 * c + h, jnp.where(wide, x, pltpu.roll(field_side(2 * c + h), s.slide, 1)))
        for field in own:
            ref[at : at + s.up_f, :] = field[fstart : fstart + s.up_f, :].astype(BF16)
            at += s.up_f
        corner(4, jnp.where(wide, field_side(4), pltpu.roll(field_side(5), s.slide, 1)))
        eight = row_of((8, s.lanes))
        halves = [jnp.zeros((8, s.lanes), F32), jnp.zeros((8, s.lanes), F32)]
        for n in range(8):
            width = s.up_d if n < 2 else s.up_f
            slot = 2 * n % 8
            if down:
                x = pltpu.roll(rows_of(n, rows - width - 8, 8), (slot + 2) % 8, 0)
            else:
                x = pltpu.roll(rows_of(n, width, 8), slot, 0)
            keep = (eight == slot) | (eight == slot + 1)
            halves[n // 4] = jnp.where(keep, x, halves[n // 4])
        if not down:
            x = pltpu.roll(rows_of(8, 0, 8), 1, 0)
            halves[0] = jnp.where(eight == 1, x, halves[0])
        extra = jnp.concatenate(halves, 0)
        ref[at : at + TILE, :] = extra[:, :cols].astype(BF16)
        corner(5, extra[:, cols:])

    @pl.when(above)
    def _():
        pack(up_ref, True)
        pack(down_ref, False)

    @pl.when(jnp.logical_not(above))
    def _():
        pack(up_ref, False)
        pack(down_ref, True)


class Convolution:
    def __init__(self, d_ref, t_ref, c, s, low):
        self.s, self.high, self.low = s, 96 - low, low
        self.acc = [jnp.zeros((3 * self.high, 2 * LANES), F32) for _ in range(3)]
        self.late = []
        tiles = s.frame // TILE
        first = [t % tiles for t in range(-3, 5)]
        second = range(1, 9)
        for p in range(s.pairs):
            rhs1, rhs2, rhs3 = [], [], []
            for r in (2 * p, 2 * p + 1):
                x = d_ref[c]
                rhs1.append(d_ref[c, first[0] * TILE : (first[0] + 1) * TILE, : s.cols])
                x = rolled(x, (s.half - s.group - r) % s.lanes) if r < s.group else x
                rhs1 += [x[t * TILE : (t + 1) * TILE, : s.cols] for t in first[1:]]
                rhs2 += [x[t * TILE : (t + 1) * TILE, : s.cols] for t in second]
                rhs3 += [jnp.concatenate([x[t * TILE : (t + 1) * TILE, s.cols :], x[u * TILE : (u + 1) * TILE, s.cols :]], 1)
                         for t, u in zip(first, second)]
            lhs = jnp.concatenate([t_ref[c, p, 96 * q + low : 96 * q + 96, :] for q in range(3)], 0)
            self.late.append((lhs, rhs2))
            self.add(2, lhs, rhs3)
            self.add(0, lhs, rhs1)

    def add(self, n, lhs, rhs):
        self.acc[n] = self.acc[n] + jnp.dot(lhs, jnp.concatenate(rhs, 0), preferred_element_type=F32)

    def finish(self):
        for lhs, rhs in self.late:
            self.add(1, lhs, rhs)

    def total(self, n, start, stop):
        return gather(self.acc, n, self.high, start - self.low, stop - self.low, self.s)


def rolled(x, shift):
    return pltpu.roll(x, shift, 1) if shift else x


def gather(acc, n, high, start, stop, s):
    parts = []
    for q in range(3):
        at = slice(high * q + start, high * q + stop)
        side = acc[2][at, n * LANES : (n + 1) * LANES]
        parts.append(rolled(jnp.concatenate([acc[n][at], side], 1), (s.group - s.group * q) % s.lanes))
    return parts[0] + parts[1] + parts[2]


def middle_kernel(df_ref, i_ref, r_ref, a_ref, b_ref, side_ref, tab_ref,
                  if_ref, rf_ref, af_ref, bf_ref, x_ref, z_ref, *, s):
    rows, cols, lanes = s.rows, s.cols, s.lanes
    own = (i_ref.at[0], i_ref.at[1], r_ref.at[0], r_ref.at[1], a_ref, b_ref)
    frames = (if_ref.at[0], if_ref.at[1], rf_ref.at[0], rf_ref.at[1], af_ref, bf_ref)
    for n, (src, dst) in enumerate(zip(own, frames)):
        dst[0:rows, :cols] = src[...]
        dst[0:rows, cols:] = side_ref[n].astype(F32)
    z_ref[...] = df_ref[...]
    end = z_ref[0, rows - TILE :, :]
    z_ref[0, rows - TILE :, :] = jnp.where(row_of(end.shape) == TILE - 1, 0.0, end.astype(F32)).astype(BF16)
    for c in range(2):
        acc = [jnp.zeros((288, cols), F32), None, jnp.zeros((288, LANES), F32)]
        for p in range(s.pairs):
            pieces = []
            for r in (2 * p, 2 * p + 1):
                if r < s.group:
                    x = rolled(z_ref[c], (s.half - s.group - r) % lanes)
                    x_ref[c, r, 0 : 2 * TILE, :] = x[0 : 2 * TILE]
                    x_ref[c, r, 2 * TILE :, :] = x[rows - 2 * TILE :]
                pieces.append(x)
            rhs = jnp.concatenate(pieces, 0)
            acc[0] = acc[0] + jnp.dot(tab_ref[c, p], rhs[:, :cols], preferred_element_type=F32)
            acc[2] = acc[2] + jnp.dot(tab_ref[c, p], rhs[:, cols:], preferred_element_type=F32)
        at = slice(s.half, rows - s.half)
        total = gather(acc, 0, 96, 0, 96, s)
        if_ref[c, at, :] = jnp.where(rf_ref[c, at, :] > 0, if_ref[c, at, :] + total, 0.0)


def border(d_ref, x_ref, e_ref, c, s):
    n = border_rows(c)
    acc = [jnp.zeros((3 * n, 2 * LANES), F32) for _ in range(3)]
    rows, lanes, cols = s.rows, s.lanes, s.cols
    for g in range(s.span3):
        tops, bottoms = [], []
        for at in range(3):
            r = 3 * g + at
            r = r if r < s.group else 0
            shift = (s.half - s.group - r) % lanes
            outer = rolled(d_ref[c, rows : s.frame, :], shift)
            start, stop = x_ref[c, r, 0 : 2 * TILE, :], x_ref[c, r, 2 * TILE :, :]
            if c == 0:
                stop = jnp.concatenate([stop[:TILE], rolled(d_ref[c, rows - TILE : rows, :], shift)], 0)
            top = jnp.concatenate([outer[2 * TILE :], start], 0)
            bottom = jnp.concatenate([stop, outer[: 3 * TILE]], 0)
            tops.append(top)
            bottoms.append(bottom)
        tops.append(tops[0][:TILE])
        bottoms.append(bottoms[0][:TILE])
        top, bottom = jnp.concatenate(tops, 0), jnp.concatenate(bottoms, 0)
        strip = jnp.concatenate([top[:, cols:], bottom[:, cols:]], 1)
        lhs = e_ref[c, g, 0 : 3 * n, :]
        for k, rhs in enumerate((top[:, :cols], bottom[:, :cols], strip)):
            acc[k] = acc[k] + jnp.dot(lhs, rhs, preferred_element_type=F32)
    return [gather(acc, k, n, 0, n, s) for k in range(2)]


def last_kernel(df_ref, v_ref, b_ref, c_ref, e_ref, side_ref, tab_ref, bor_ref, x_ref, one_ref, two_ref,
                if_in, rf_in, af_in, bf_in, vo_hbm, io_hbm, if_ref, rf_ref, af_ref, bf_ref,
                d_ref, vf_ref, vo_ref, io_ref, sems, *, s):
    even = lax.rem(lax.axis_index("row"), 2) == 0
    rows, cols, frame, lanes = s.rows, s.cols, s.frame, s.lanes
    index = lax.axis_index("row")
    low = jnp.where(even, one_ref[...], two_ref[...])
    high = jnp.where(even, two_ref[...], one_ref[...])
    low = jnp.where(index < lax.axis_size("row") - 1, low, jnp.zeros_like(low))
    high = jnp.where(index > 0, high, jnp.zeros_like(high))
    ud, uf, full = s.up_d, s.up_f, s.fields
    lane = lane_of((TILE, LANES))

    def corner(x, k):
        return x[s.main + k // 2 * TILE : s.main + (k // 2 + 1) * TILE, k % 2 * LANES : (k % 2 + 1) * LANES].astype(F32)

    def rest(x):
        return jnp.concatenate([x[s.tail : s.main, :].astype(F32), corner(x, 5)], 1)

    def field(x, n):
        at = 2 * ud + n * uf
        side = corner(x, min(n, 4))
        if n != 4:
            side = pltpu.roll(side, LANES - s.slide, 1)
        side = jnp.where((lane < s.near) | (lane >= LANES - s.near), side, 0.0)
        return jnp.concatenate([x[at : at + uf, :].astype(F32), side], 1)

    def driving(x, c):
        sides = [jnp.where((lane < s.far) | (lane >= LANES - s.far), corner(x, 2 * c + h), 0.0) for h in range(2)]
        return jnp.concatenate([x[c * ud : (c + 1) * ud, :], jnp.concatenate(sides, 0).astype(BF16)], 1)

    low_rest, high_rest = rest(low), rest(high)
    eight = row_of((8, lanes))
    frames = (if_ref.at[0], if_ref.at[1], rf_ref.at[0], rf_ref.at[1], af_ref, bf_ref)
    for n, dst in enumerate(frames):
        half, slot = divmod(4 + 2 * n, 8)
        extra_low = pltpu.roll(low_rest[8 * half : 8 * half + 8], (8 - slot) % 8, 0)
        extra_high = pltpu.roll(high_rest[8 * half : 8 * half + 8], 6 - slot, 0)
        dst[rows : rows + uf, :] = field(low, n)
        dst[rows + uf : rows + uf + 8, :] = jnp.where(eight == 0, extra_low, 0.0)
        dst[full - uf - 8 : full - uf, :] = jnp.where(eight >= 6, extra_high, 0.0)
        dst[full - uf : full, :] = field(high, n)
    v_next = low_rest[1:2, :]
    v_first = jnp.concatenate([v_ref[0:8, :][0:1, :], side_ref[6, 0:TILE, :].astype(F32)[0:1, :]], 1)
    gap = rows + ud
    shape = (TILE, lanes)
    for c in range(2):
        d_ref[c, 0:rows, :] = df_ref[c]
        d_ref[c, rows:gap, :] = driving(low, c)
        d_ref[c, gap + TILE :, :] = driving(high, c)
        extra_low = pltpu.roll(low_rest[0:8], (8 - 2 * c) % 8, 0)
        extra_high = pltpu.roll(high_rest[0:8], 6 - 2 * c, 0)
        d_ref[c, gap : gap + TILE, :] = jnp.concatenate(
            [jnp.where(eight == 0, extra_low, 0.0), jnp.where(eight >= 6, extra_high, 0.0)], 0).astype(BF16)
    last = row_of(shape) == TILE - 1
    x = d_ref[0, rows - TILE : rows, :].astype(F32)
    d_ref[0, rows - TILE : rows, :] = jnp.where(last, x - v_next, x).astype(BF16)
    x = d_ref[0, frame - TILE :, :].astype(F32)
    inside = rf_ref[0, full - TILE :, :] > 0
    d_ref[0, frame - TILE :, :] = jnp.where(last, jnp.where(inside, x - v_first, 0.0), x).astype(BF16)

    for c in range(2):
        top, bottom = border(d_ref, x_ref, bor_ref, c, s)
        n = border_rows(c)
        pieces = []
        if c == 0:
            pieces.append((rows - 24, jnp.where(eight == 7, jnp.broadcast_to(bottom[0:1], (8, lanes)), 0.0)))
            top, bottom = pltpu.roll(top, n - 1, 0), pltpu.roll(bottom, n - 1, 0)
        pieces += [(full - 24, top[8:32]), (0, top[32:48]), (rows - TILE, bottom[0:40])]
        for dst, add in pieces:
            at = slice(dst, dst + add.shape[0])
            if_ref[c, at, :] = jnp.where(rf_ref[c, at, :] > 0, if_ref[c, at, :] + add, 0.0)
    i0, i1 = if_ref[0], if_ref[1]
    div = i0 - pltpu.roll(i0, 1, 0) + i1 - pltpu.roll(i1, 1, 1)
    volt = af_ref[...] - bf_ref[...] * div
    vf_ref[...] = volt
    drop0 = volt - pltpu.roll(volt, full - 1, 0)
    drop1 = volt - pltpu.roll(volt, lanes - 1, 1)
    r0, r1 = rf_ref[0], rf_ref[1]
    for c, (drop, r, i) in enumerate(((drop0, r0, i0), (drop1, r1, i1))):
        x = jnp.where(r > 0, drop - r * i, 0.0).astype(BF16)
        d_ref[c, 0 : rows + TILE, :] = x[0 : rows + TILE]
        d_ref[c, frame - 2 * TILE :, :] = x[full - 2 * TILE :]

    copies = []

    def send(src, dst):
        copies.append(pltpu.make_async_copy(src, dst, sems.at[len(copies)]))
        copies[-1].start()

    def emit(n, above):
        size = rows // 2
        at = slice(size * n, size * n + size)
        i0 = (if_ref[0, at, :] + parts[0].total(n, 32, 96))[:, :cols]
        io_ref[0, at, :] = i0
        send(io_ref.at[0, at], io_hbm.at[0, at])
        ends = jnp.where(rf_ref[1, at, :] > 0, if_ref[1, at, :] + parts[1].total(n, 32, 96), 0.0)
        i1 = ends[:, :cols]
        io_ref[1, at, :] = i1
        send(io_ref.at[1, at], io_hbm.at[1, at])
        left = pltpu.roll(ends, 1, 1)[:, :cols]
        up = jnp.where(row_of(i0.shape) == 0, above, pltpu.roll(i0, 1, 0))
        div = i0 - up + i1 - left
        vo_ref[at, :] = c_ref[at, :] * vf_ref[at, :cols] + e_ref[at, :] - b_ref[at, :] * div
        send(vo_ref.at[at], vo_hbm.at[at])

    parts = [Convolution(d_ref, tab_ref, 0, s, 16), Convolution(d_ref, tab_ref, 1, s, 32)]
    above = if_ref[0, full - 8 :, :] + parts[0].total(0, 24, 32)
    above = jnp.where(rf_ref[0, full - 8 :, :] > 0, above, 0.0)[7:8, :cols]
    parts[0].finish()
    emit(0, above)
    parts[1].finish()
    emit(1, io_ref[0, rows // 2 - 8 : rows // 2, :][7:8])
    for copy in copies:
        copy.wait()


def swapped(x, axis, odd):
    sizes = lax.axis_size("row"), lax.axis_size("col")
    main = ("row", "col").index(axis)
    to = {}
    for at in itertools.product(range(sizes[0]), range(sizes[1])):
        along, other = at[main], at[1 - main]
        if along >= odd and (along ^ 1 if not odd else ((along - 1) ^ 1) + 1) < sizes[main]:
            along = along ^ 1 if not odd else ((along - 1) ^ 1) + 1
        elif other ^ 1 < sizes[1 - main]:
            other = other ^ 1
        else:
            continue
        there = (along, other) if main == 0 else (other, along)
        to[at[0] * sizes[1] + at[1]] = there[0] * sizes[1] + there[1]
    return lax.ppermute(x, ("row", "col"), list(to.items()))


def near(x):
    return pltpu.with_memory_space_constraint(x, pltpu.VMEM)


def call(kernel, outs, ins, scratch=(), specs=None, limit=16, out_specs=None, aliases=None):
    return pl.pallas_call(
        kernel,
        compiler_params=pltpu.CompilerParams(vmem_limit_bytes=limit << 20),
        out_shape=outs,
        in_specs=specs or [VMEM] * len(ins),
        out_specs=out_specs or jax.tree.map(lambda _: VMEM, outs),
        scratch_shapes=scratch,
        input_output_aliases=aliases or {},
    )(*ins)


def local(voltage, currents, resistance, inverse_cap, shunt, tap, pad, waveforms, k_window):
    rows, cols = voltage.shape
    s = Sizes(rows, cols, k_window.shape[1], waveforms.shape[1])
    sds = pltpu.VMEM
    k_window = k_window.transpose(1, 0, 2)
    block = sds((rows, cols), F32)
    half = sds((s.edge, LANES), BF16)
    pair = sds((2, rows, cols), F32)
    whole = sds((rows, cols), jnp.int32)
    one, two, v_near, i_near, r_near, cap_near, shunt_near, tap_near, pad_near, k_near, w_near = call(
        functools.partial(first_kernel, s=s),
        (half, half, block, pair, pair, block, block, whole, whole, sds(k_window.shape, BF16),
         sds((2, s.waves, LANES), F32)),
        [pltpu.with_memory_space_constraint(x, pltpu.HBM)
         for x in (voltage, currents, resistance, inverse_cap, shunt, tap, pad, waveforms, k_window)],
        specs=[FAR] * 9,
        scratch=[pltpu.SMEM(waveforms.shape, F32), pltpu.SemaphoreType.DMA((9,))])
    square = pltpu.VMEM((LANES, LANES), F32)
    d, a, b, c, e, tables, borders = call(
        functools.partial(own_kernel, s=s),
        (sds((2, rows, cols), BF16), block, block, block, block, sds((2, s.pairs, 288, 2 * LANES), BF16),
         sds((2, s.span3, 192, 2 * LANES), BF16)),
        (v_near, i_near, r_near, cap_near, shunt_near, tap_near, pad_near, k_near, w_near),
        scratch=[square])
    one, two = near(swapped(one, "col", 0)), near(swapped(two, "col", 1))
    pay = sds((s.payload, cols), BF16)
    df, side, one, two = call(
        functools.partial(second_kernel, s=s),
        (sds((2, rows, s.lanes), BF16), sds((7, rows, LANES), BF16), pay, pay),
        (d, v_near, i_near, r_near, a, b, one, two))
    one, two = swapped(one, "row", 0), swapped(two, "row", 1)
    f = sds((s.fields, s.lanes), F32)
    f2 = sds((2, s.fields, s.lanes), F32)
    i_frame, r_frame, a_frame, b_frame, shifted = call(
        functools.partial(middle_kernel, s=s),
        (f2, f2, f, f, sds((2, s.group, 4 * TILE, s.lanes), BF16)),
        (df, i_near, r_near, a, b, side, tables),
        scratch=[pltpu.VMEM((2, rows, s.lanes), BF16)])
    outs = call(
        functools.partial(last_kernel, s=s),
        (jax.ShapeDtypeStruct((rows, cols), F32), jax.ShapeDtypeStruct((2, rows, cols), F32), f2, f2, f, f),
        (df, v_near, b, c, e, side, tables, borders, shifted, near(one), near(two), i_frame, r_frame, a_frame, b_frame),
        scratch=[pltpu.VMEM((2, s.frame, s.lanes), BF16), pltpu.VMEM((s.fields, s.lanes), F32),
                 pltpu.VMEM((rows, cols), F32), pltpu.VMEM((2, rows, cols), F32), pltpu.SemaphoreType.DMA((6,))],
        out_specs=(FAR, FAR, VMEM, VMEM, VMEM, VMEM), aliases={11: 2, 12: 3, 13: 4, 14: 5})
    return outs[0], outs[1]


def solution(mesh):
    grid = P("row", "col")
    pair = P(None, "row", "col")

    return jax.shard_map(
        local,
        mesh=mesh,
        in_specs=(grid, pair, pair, grid, grid, grid, grid, P(), P()),
        out_specs=(grid, pair),
        check_vma=False,
    )
```

```python
import functools
import itertools

import jax
import jax.numpy as jnp
from jax import lax
from jax.experimental import pallas as pl
from jax.experimental.pallas import tpu as pltpu
from jax.sharding import PartitionSpec as P


F32 = jnp.float32
BF16 = jnp.bfloat16
LANES = 128
TILE = 16
VMEM = pl.BlockSpec(memory_space=pltpu.VMEM)
FAR = pl.BlockSpec(memory_space=pltpu.HBM)


class Sizes:
    def __init__(self, rows, cols, span, waves):
        self.rows, self.cols, self.span, self.waves = rows, cols, span, waves
        self.half = (span - 1) // 2
        self.far = 2 * self.half + 2
        self.near = self.half + 2
        self.lanes = cols + LANES
        self.frame = rows + 5 * TILE
        self.group = -(-span // 3)
        self.pairs = (self.group + 1) // 2
        self.span3 = -(-self.group // 3)
        self.fields = rows + 3 * TILE
        self.up_d = 2 * self.half
        self.up_f = self.half
        self.tail = 2 * self.up_d + 6 * self.up_f
        self.main = self.tail + TILE
        self.payload = self.main + 3 * TILE
        self.slide = self.far + self.near
        far, near = self.far, self.near
        self.slots = (
            ((far, 0, 0), (far, far, far), (near, 2 * far, far + near),
             (near, 2 * far + near, far + 2 * near), (near, 2 * far + 2 * near, far + 3 * near)),
            ((near, 0, 0), (near, near, near), (near, 2 * near, 2 * near), (1, 3 * near, 3 * near)),
        )
        self.edge = rows + rows // 2 + TILE


def lane_of(shape):
    return lax.broadcasted_iota(jnp.int32, shape, len(shape) - 1)


def row_of(shape):
    return lax.broadcasted_iota(jnp.int32, shape, 0)


def border_rows(c):
    return 64 if c == 0 else 48


def turn(k_ref, pad_ref, c, s):
    pad_ref[...] = jnp.zeros((LANES, LANES), F32)
    pad_ref[0 : s.span, 0 : s.span] = k_ref[:, c, :].astype(F32)
    return pad_ref[...].T


def main_tables(k_ref, t_ref, pad_ref, s):
    for c in range(2):
        turned = turn(k_ref, pad_ref, c, s)
        for r in range(2 * s.pairs):
            p, at = divmod(r, 2)
            for q in range(3):
                if r < s.group:
                    b = s.group * q + r
                    row = jnp.broadcast_to(turned[b : b + 1, :], (96, LANES))
                    band = pltpu.roll(row, 0, 1, stride=1, stride_axis=0).astype(BF16)
                else:
                    band = jnp.zeros((96, LANES), BF16)
                t_ref[c, p, q * 96 : (q + 1) * 96, at * LANES : (at + 1) * LANES] = band


def border_tables(t_ref, e_ref, s):
    window = 5 * TILE
    over = 2 * window - LANES
    for c in range(2):
        n = border_rows(c)
        late = 1 - c
        lane = lane_of((n, LANES))
        for g in range(s.span3):
            for q in range(3):
                def piece(at):
                    p, half = divmod(3 * g + at, 2)
                    return t_ref[c, p, 96 * q : 96 * q + n, half * LANES : (half + 1) * LANES]

                first = rolled(piece(0), (-late) % LANES).astype(F32)
                second = rolled(piece(1), window - late).astype(F32)
                third = rolled(piece(2), over - late).astype(F32)
                low = jnp.where(lane < window, first, second)
                high = jnp.where(lane < over, second, third)
                if late:
                    later = row_of(lane.shape) > 0
                    last = s.span - 2
                    low = jnp.where(later | (lane == last) | (lane == last + window), low, 0.0)
                    high = jnp.where(later | (lane == last + over), high, 0.0)
                e_ref[c, g, q * n : (q + 1) * n, :LANES] = low.astype(BF16)
                e_ref[c, g, q * n : (q + 1) * n, LANES:] = high.astype(BF16)


def load_of(tap, wave, s):
    total = jnp.zeros(tap.shape, F32)
    for n in range(s.waves):
        total = jnp.where(tap == n, wave(n), total)
    return total


def first_kernel(v_hbm, i_hbm, r_hbm, cap_hbm, shunt_hbm, tap_hbm, pad_hbm, wave_hbm, k_hbm,
                 one_ref, two_ref, v_ref, i_ref, r_ref, cap_ref, shunt_ref, tap_ref, pad_ref, k_ref, w_ref,
                 wave_ref, sems, *, s):
    sources = (v_hbm, r_hbm, i_hbm, wave_hbm, tap_hbm, pad_hbm, cap_hbm, shunt_hbm, k_hbm)
    targets = (v_ref, r_ref, i_ref, wave_ref, tap_ref, pad_ref, cap_ref, shunt_ref, k_ref)
    copies = [pltpu.make_async_copy(x, y, sems.at[n]) for n, (x, y) in enumerate(zip(sources, targets))]
    for copy in copies:
        copy.start()
    even = lax.rem(lax.axis_index("col"), 2) == 0
    rows, cols = s.rows, s.cols
    shape = (rows, LANES)
    lane, row = lane_of(shape), row_of(shape)

    def ends(ref):
        return jnp.where(lane < LANES // 2, ref[:, :LANES], ref[:, cols - LANES :])

    for copy in copies[:3]:
        copy.wait()
    volt = ends(v_ref)
    i0, i1, r0, r1 = ends(i_ref.at[0]), ends(i_ref.at[1]), ends(r_ref.at[0]), ends(r_ref.at[1])
    below = jnp.where(row == rows - 1, 0.0, pltpu.roll(volt, rows - 1, 0))
    beside = jnp.where(lane == LANES - 1, 0.0, pltpu.roll(volt, LANES - 1, 1))
    d0 = (volt - below) - r0 * i0
    d1 = (volt - beside) - r1 * i1
    half = rows // 2

    def put(start, left, right):
        at = slice(start, start + left.shape[0])
        one_ref[at, :] = jnp.where(even, right, left).astype(BF16)
        two_ref[at, :] = jnp.where(even, left, right).astype(BF16)

    def slotted(slots, fields):
        left = jnp.zeros(shape, F32)
        right = jnp.zeros(shape, F32)
        for (n, off, back), field in zip(slots, fields):
            x = rolled(field, off)
            left = jnp.where((lane >= off) & (lane < off + n), x, left)
            if n > 1:
                x = x if back == off else rolled(field, back)
                right = jnp.where(before(lane, n, back), x, right)
        return left, right

    put(0, *slotted(s.slots[0], (d0, d1, i0, i1, r0)))
    put(rows + half, v_ref[:TILE, :LANES], v_ref[:TILE, cols - LANES :])
    for copy in copies[3:]:
        copy.wait()
    for step in range(2):
        for n in range(s.waves):
            w_ref[step, n : n + 1, :] = jnp.full((1, LANES), wave_ref[step, n], F32)
    load = load_of(ends(tap_ref), lambda n: wave_ref[0, n], s)
    keep = ends(pad_ref) != 1
    b = jnp.where(keep, ends(cap_ref), 0.0)
    c = jnp.where(keep, 1.0, 0.0) - b * ends(shunt_ref)
    volt = ends(v_ref)
    a = b * load + c * volt
    folded = [x[:half] + pltpu.roll(x[half:], LANES // 2, 1)
              for x in slotted(s.slots[1], (ends(r_ref.at[1]), a, b, volt))]
    put(rows, *folded)


def before(lane, n, off):
    if off >= n:
        return (lane >= off - n) & (lane < off)
    return (lane < off) | (lane >= LANES + off - n)


def own_kernel(v_ref, i_ref, r_ref, cap_ref, shunt_ref, tap_ref, pad_ref, k_ref, w_ref,
               d_ref, a_ref, b_ref, c_ref, e_ref, t_ref, bor_ref, square_ref, *, s):
    main_tables(k_ref, t_ref, square_ref, s)
    border_tables(t_ref, bor_ref, s)
    volt = v_ref[...]
    rows, cols = volt.shape
    below = jnp.where(row_of(volt.shape) == rows - 1, 0.0, pltpu.roll(volt, rows - 1, 0))
    beside = jnp.where(lane_of(volt.shape) == cols - 1, 0.0, pltpu.roll(volt, cols - 1, 1))
    d_ref[0] = ((volt - below) - r_ref[0] * i_ref[0]).astype(BF16)
    d_ref[1] = ((volt - beside) - r_ref[1] * i_ref[1]).astype(BF16)
    keep = pad_ref[...] != 1
    b = jnp.where(keep, cap_ref[...], 0.0)
    c = jnp.where(keep, 1.0, 0.0) - b * shunt_ref[...]
    b_ref[...], c_ref[...] = b, c
    for at in range(0, cols, LANES):
        at = slice(at, at + LANES)
        first, second = [load_of(tap_ref[:, at], lambda n: w_ref[step, n : n + 1, :], s) for step in range(2)]
        a_ref[:, at] = c[:, at] * volt[:, at] + b[:, at] * first
        e_ref[:, at] = b[:, at] * second


def second_kernel(d_ref, v_ref, i_ref, r_ref, a_ref, b_ref, one_ref, two_ref,
                  df_ref, t_ref, up_ref, down_ref, *, s):
    even = lax.rem(lax.axis_index("col"), 2) == 0
    rows, cols = v_ref.shape
    lane = lane_of((rows, LANES))
    half = rows // 2
    index, count = lax.axis_index("col"), lax.axis_size("col")

    def get(start, size):
        at = slice(start, start + size)
        one, two = one_ref[at, :].astype(F32), two_ref[at, :].astype(F32)
        right, left = jnp.where(even, one, two), jnp.where(even, two, one)
        return jnp.where(index < count - 1, right, 0.0), jnp.where(index > 0, left, 0.0)

    sides = []
    for tile, slots in enumerate(s.slots):
        if tile == 0:
            pair = get(0, rows)
        else:
            pair = [jnp.concatenate([x, pltpu.roll(x, LANES // 2, 1)], 0) for x in get(rows, half)]
        for n, off, back in slots:
            if back == off:
                x = jnp.where((lane >= off) & (lane < off + n), pair[0], pair[1])
                x = rolled(x, (LANES - off) % LANES)
                sides.append(jnp.where((lane < n) | (lane >= LANES - n), x, 0.0))
            else:
                x, y = rolled(pair[0], LANES - off), rolled(pair[1], LANES - back)
                sides.append(jnp.where(lane < n, x, jnp.where(lane >= LANES - n, y, 0.0)))
    d0s, d1s, i0s, i1s, r0s, r1s, as_, bs, vs = sides
    x, y = get(rows + half, TILE)
    first = lane_of((TILE, LANES))
    corner = jnp.where(first < s.far, x, jnp.where(first >= LANES - s.far, y, 0.0))
    edge = lane == LANES - 1
    next_side = pltpu.roll(vs, LANES - 1, 1)
    next_own = pltpu.roll(v_ref[:, :LANES], LANES - 1, 1)
    d1 = d_ref[1]
    tail = d1[:, cols - LANES :].astype(F32)
    tail = jnp.where(edge, tail - next_side, tail).astype(BF16)
    d1s = jnp.where(edge, jnp.where(r1s > 0, d1s - next_own, 0.0), d1s).astype(BF16)
    df_ref[0, :, :cols] = d_ref[0]
    df_ref[0, :, cols:] = d0s.astype(BF16)
    df_ref[1, :, : cols - LANES] = d1[:, : cols - LANES]
    df_ref[1, :, cols - LANES : cols] = tail
    df_ref[1, :, cols:] = d1s
    for n, x in enumerate((i0s, i1s, r0s, r1s, as_, bs)):
        t_ref[n] = x.astype(BF16)
    t_ref[6, :TILE, :] = corner.astype(BF16)
    above = lax.rem(lax.axis_index("row"), 2) == 0

    own = (i_ref.at[0], i_ref.at[1], r_ref.at[0], r_ref.at[1], a_ref, b_ref)

    def rows_of(n, start, size):
        if n < 2:
            at = start // TILE * TILE
            x = df_ref[n, at : at + TILE, :].astype(F32)
            return x[start - at : start - at + size]
        source = v_ref if n == 8 else own[n - 2]
        at = start // TILE * TILE
        x = t_ref[n - 2, at : at + TILE, :].astype(F32)
        return jnp.concatenate([source[start : start + size, :], x[start - at : start - at + size]], 1)

    lane16 = lane_of((TILE, LANES))
    wide = (lane16 < s.far) | (lane16 >= LANES - s.far)

    def pack(ref, down):
        at = 0
        dstart = rows - s.up_d if down else 0
        fstart = rows - s.up_f if down else 0

        def corner(k, x):
            ref[s.main + k // 2 * TILE : s.main + (k // 2 + 1) * TILE, k % 2 * LANES : (k % 2 + 1) * LANES] = x.astype(BF16)

        def field_side(n):
            return t_ref[n, fstart : fstart + s.up_f, :].astype(F32)

        for c in range(2):
            ref[at : at + s.up_d, :] = df_ref[c, dstart : dstart + s.up_d, :cols]
            at += s.up_d
            for h in range(2):
                x = df_ref[c, dstart + h * TILE : dstart + (h + 1) * TILE, cols:].astype(F32)
                corner(2 * c + h, jnp.where(wide, x, pltpu.roll(field_side(2 * c + h), s.slide, 1)))
        for field in own:
            ref[at : at + s.up_f, :] = field[fstart : fstart + s.up_f, :].astype(BF16)
            at += s.up_f
        corner(4, jnp.where(wide, field_side(4), pltpu.roll(field_side(5), s.slide, 1)))
        eight = row_of((8, s.lanes))
        halves = [jnp.zeros((8, s.lanes), F32), jnp.zeros((8, s.lanes), F32)]
        for n in range(8):
            width = s.up_d if n < 2 else s.up_f
            slot = 2 * n % 8
            if down:
                x = pltpu.roll(rows_of(n, rows - width - 8, 8), (slot + 2) % 8, 0)
            else:
                x = pltpu.roll(rows_of(n, width, 8), slot, 0)
            keep = (eight == slot) | (eight == slot + 1)
            halves[n // 4] = jnp.where(keep, x, halves[n // 4])
        if not down:
            x = pltpu.roll(rows_of(8, 0, 8), 1, 0)
            halves[0] = jnp.where(eight == 1, x, halves[0])
        extra = jnp.concatenate(halves, 0)
        ref[at : at + TILE, :] = extra[:, :cols].astype(BF16)
        corner(5, extra[:, cols:])

    @pl.when(above)
    def _():
        pack(up_ref, True)
        pack(down_ref, False)

    @pl.when(jnp.logical_not(above))
    def _():
        pack(up_ref, False)
        pack(down_ref, True)


class Convolution:
    def __init__(self, d_ref, inner_ref, t_ref, c, s, low):
        self.s, self.high, self.low = s, 96 - low, low
        self.acc = [jnp.zeros((3 * self.high, 2 * LANES), F32) for _ in range(3)]
        self.late = []
        tiles = s.frame // TILE
        first = [t % tiles for t in range(-3, 5)]
        second = range(1, 9)
        for p in range(s.pairs):
            rhs1, rhs2, rhs3 = [], [], []
            for r in (2 * p, 2 * p + 1):
                shift = (s.half - s.group - r) % s.lanes if r < s.group else 0
                x = {}
                for t in sorted(set(first[1:]) | set(second)):
                    if 2 <= t < s.rows // TILE - 2:
                        at = (t - 2) * TILE
                        x[t] = inner_ref[c, r if r < s.group else 0, at : at + TILE, :]
                    else:
                        x[t] = rolled(d_ref[c, t * TILE : (t + 1) * TILE, :], shift)
                x[first[0]] = d_ref[c, first[0] * TILE : (first[0] + 1) * TILE, :]
                rhs1 += [x[t][:, : s.cols] for t in first]
                rhs2 += [x[t][:, : s.cols] for t in second]
                rhs3 += [jnp.concatenate([x[t][:, s.cols :], x[u][:, s.cols :]], 1) for t, u in zip(first, second)]
            lhs = jnp.concatenate([t_ref[c, p, 96 * q + low : 96 * q + 96, :] for q in range(3)], 0)
            self.late.append((lhs, rhs2))
            self.add(2, lhs, rhs3)
            self.add(0, lhs, rhs1)

    def add(self, n, lhs, rhs):
        self.acc[n] = self.acc[n] + jnp.dot(lhs, jnp.concatenate(rhs, 0), preferred_element_type=F32)

    def finish(self):
        for lhs, rhs in self.late:
            self.add(1, lhs, rhs)

    def total(self, n, start, stop):
        return gather(self.acc, n, self.high, start - self.low, stop - self.low, self.s)


def rolled(x, shift):
    return pltpu.roll(x, shift, 1) if shift else x


def gather(acc, n, high, start, stop, s):
    parts = []
    for q in range(3):
        at = slice(high * q + start, high * q + stop)
        side = acc[2][at, n * LANES : (n + 1) * LANES]
        parts.append(rolled(jnp.concatenate([acc[n][at], side], 1), (s.group - s.group * q) % s.lanes))
    return parts[0] + parts[1] + parts[2]


def middle_kernel(df_ref, i_ref, r_ref, a_ref, b_ref, side_ref, tab_ref,
                  if_ref, rf_ref, af_ref, bf_ref, x_ref, inner_ref, vm_ref, z_ref, *, s):
    rows, cols, lanes = s.rows, s.cols, s.lanes
    own = (i_ref.at[0], i_ref.at[1], r_ref.at[0], r_ref.at[1], a_ref, b_ref)
    frames = (if_ref.at[0], if_ref.at[1], rf_ref.at[0], rf_ref.at[1], af_ref, bf_ref)
    for n, (src, dst) in enumerate(zip(own, frames)):
        dst[0:rows, :cols] = src[...]
        dst[0:rows, cols:] = side_ref[n].astype(F32)
    z_ref[...] = df_ref[...]
    end = z_ref[0, rows - TILE :, :]
    z_ref[0, rows - TILE :, :] = jnp.where(row_of(end.shape) == TILE - 1, 0.0, end.astype(F32)).astype(BF16)
    for c in range(2):
        acc = [jnp.zeros((288, cols), F32), None, jnp.zeros((288, LANES), F32)]
        for p in range(s.pairs):
            pieces = []
            for r in (2 * p, 2 * p + 1):
                if r < s.group:
                    x = rolled(z_ref[c], (s.half - s.group - r) % lanes)
                    x_ref[c, r, 0 : 2 * TILE, :] = x[0 : 2 * TILE]
                    x_ref[c, r, 2 * TILE :, :] = x[rows - 2 * TILE :]
                pieces.append(x)
            rhs = jnp.concatenate(pieces, 0)
            acc[0] = acc[0] + jnp.dot(tab_ref[c, p], rhs[:, :cols], preferred_element_type=F32)
            acc[2] = acc[2] + jnp.dot(tab_ref[c, p], rhs[:, cols:], preferred_element_type=F32)
        at = slice(s.half, rows - s.half)
        total = gather(acc, 0, 96, 0, 96, s)
        if_ref[c, at, :] = jnp.where(rf_ref[c, at, :] > 0, if_ref[c, at, :] + total, 0.0)
    at = slice(2 * TILE - 8, rows - 2 * TILE + 8)
    size = rows - 4 * TILE
    i = [if_ref[c, at, :] for c in range(2)]
    r = [rf_ref[c, at, :] for c in range(2)]
    volt, drive = advance(i, r, af_ref[at, :], bf_ref[at, :])
    vm_ref[...] = volt[8 : 8 + size, :cols]
    for c in range(2):
        x = drive[c][8 : 8 + size].astype(BF16)
        for n in range(s.group):
            inner_ref[c, n] = rolled(x, (s.half - s.group - n) % lanes)


def advance(i, r, a, b):
    rows, lanes = a.shape
    volt = a - b * (i[0] - pltpu.roll(i[0], 1, 0) + i[1] - pltpu.roll(i[1], 1, 1))
    drops = volt - pltpu.roll(volt, rows - 1, 0), volt - pltpu.roll(volt, lanes - 1, 1)
    return volt, [jnp.where(r[c] > 0, drops[c] - r[c] * i[c], 0.0) for c in range(2)]


def border(d_ref, x_ref, e_ref, c, s):
    n = border_rows(c)
    acc = [jnp.zeros((3 * n, 2 * LANES), F32) for _ in range(3)]
    rows, lanes, cols = s.rows, s.lanes, s.cols
    for g in range(s.span3):
        tops, bottoms = [], []
        for at in range(3):
            r = 3 * g + at
            r = r if r < s.group else 0
            shift = (s.half - s.group - r) % lanes
            outer = rolled(d_ref[c, rows : s.frame, :], shift)
            start, stop = x_ref[c, r, 0 : 2 * TILE, :], x_ref[c, r, 2 * TILE :, :]
            if c == 0:
                stop = jnp.concatenate([stop[:TILE], rolled(d_ref[c, rows - TILE : rows, :], shift)], 0)
            top = jnp.concatenate([outer[2 * TILE :], start], 0)
            bottom = jnp.concatenate([stop, outer[: 3 * TILE]], 0)
            tops.append(top)
            bottoms.append(bottom)
        tops.append(tops[0][:TILE])
        bottoms.append(bottoms[0][:TILE])
        top, bottom = jnp.concatenate(tops, 0), jnp.concatenate(bottoms, 0)
        strip = jnp.concatenate([top[:, cols:], bottom[:, cols:]], 1)
        lhs = e_ref[c, g, 0 : 3 * n, :]
        for k, rhs in enumerate((top[:, :cols], bottom[:, :cols], strip)):
            acc[k] = acc[k] + jnp.dot(lhs, rhs, preferred_element_type=F32)
    return [gather(acc, k, n, 0, n, s) for k in range(2)]


def last_kernel(df_ref, v_ref, b_ref, c_ref, e_ref, side_ref, tab_ref, bor_ref, x_ref, inner_ref, vm_ref,
                one_ref, two_ref,
                if_in, rf_in, af_in, bf_in, vo_hbm, io_hbm, if_ref, rf_ref, af_ref, bf_ref,
                d_ref, vf_ref, vo_ref, io_ref, sems, *, s):
    even = lax.rem(lax.axis_index("row"), 2) == 0
    rows, cols, frame, lanes = s.rows, s.cols, s.frame, s.lanes
    index = lax.axis_index("row")
    low = jnp.where(even, one_ref[...], two_ref[...])
    high = jnp.where(even, two_ref[...], one_ref[...])
    low = jnp.where(index < lax.axis_size("row") - 1, low, jnp.zeros_like(low))
    high = jnp.where(index > 0, high, jnp.zeros_like(high))
    ud, uf, full = s.up_d, s.up_f, s.fields
    lane = lane_of((TILE, LANES))

    def corner(x, k):
        return x[s.main + k // 2 * TILE : s.main + (k // 2 + 1) * TILE, k % 2 * LANES : (k % 2 + 1) * LANES].astype(F32)

    def rest(x):
        return jnp.concatenate([x[s.tail : s.main, :].astype(F32), corner(x, 5)], 1)

    def field(x, n):
        at = 2 * ud + n * uf
        side = corner(x, min(n, 4))
        if n != 4:
            side = pltpu.roll(side, LANES - s.slide, 1)
        side = jnp.where((lane < s.near) | (lane >= LANES - s.near), side, 0.0)
        return jnp.concatenate([x[at : at + uf, :].astype(F32), side], 1)

    def driving(x, c):
        sides = [jnp.where((lane < s.far) | (lane >= LANES - s.far), corner(x, 2 * c + h), 0.0) for h in range(2)]
        return jnp.concatenate([x[c * ud : (c + 1) * ud, :], jnp.concatenate(sides, 0).astype(BF16)], 1)

    low_rest, high_rest = rest(low), rest(high)
    eight = row_of((8, lanes))
    frames = (if_ref.at[0], if_ref.at[1], rf_ref.at[0], rf_ref.at[1], af_ref, bf_ref)
    for n, dst in enumerate(frames):
        half, slot = divmod(4 + 2 * n, 8)
        extra_low = pltpu.roll(low_rest[8 * half : 8 * half + 8], (8 - slot) % 8, 0)
        extra_high = pltpu.roll(high_rest[8 * half : 8 * half + 8], 6 - slot, 0)
        dst[rows : rows + uf, :] = field(low, n)
        dst[rows + uf : rows + uf + 8, :] = jnp.where(eight == 0, extra_low, 0.0)
        dst[full - uf - 8 : full - uf, :] = jnp.where(eight >= 6, extra_high, 0.0)
        dst[full - uf : full, :] = field(high, n)
    v_next = low_rest[1:2, :]
    v_first = jnp.concatenate([v_ref[0:8, :][0:1, :], side_ref[6, 0:TILE, :].astype(F32)[0:1, :]], 1)
    gap = rows + ud
    shape = (TILE, lanes)
    for c in range(2):
        d_ref[c, rows - TILE : rows, :] = df_ref[c, rows - TILE : rows, :]
        d_ref[c, rows:gap, :] = driving(low, c)
        d_ref[c, gap + TILE :, :] = driving(high, c)
        extra_low = pltpu.roll(low_rest[0:8], (8 - 2 * c) % 8, 0)
        extra_high = pltpu.roll(high_rest[0:8], 6 - 2 * c, 0)
        d_ref[c, gap : gap + TILE, :] = jnp.concatenate(
            [jnp.where(eight == 0, extra_low, 0.0), jnp.where(eight >= 6, extra_high, 0.0)], 0).astype(BF16)
    last = row_of(shape) == TILE - 1
    x = d_ref[0, rows - TILE : rows, :].astype(F32)
    d_ref[0, rows - TILE : rows, :] = jnp.where(last, x - v_next, x).astype(BF16)
    x = d_ref[0, frame - TILE :, :].astype(F32)
    inside = rf_ref[0, full - TILE :, :] > 0
    d_ref[0, frame - TILE :, :] = jnp.where(last, jnp.where(inside, x - v_first, 0.0), x).astype(BF16)

    for c in range(2):
        top, bottom = border(d_ref, x_ref, bor_ref, c, s)
        n = border_rows(c)
        pieces = []
        if c == 0:
            pieces.append((rows - 24, jnp.where(eight == 7, jnp.broadcast_to(bottom[0:1], (8, lanes)), 0.0)))
            top, bottom = pltpu.roll(top, n - 1, 0), pltpu.roll(bottom, n - 1, 0)
        pieces += [(full - 24, top[8:32]), (0, top[32:48]), (rows - TILE, bottom[0:40])]
        for dst, add in pieces:
            at = slice(dst, dst + add.shape[0])
            if_ref[c, at, :] = jnp.where(rf_ref[c, at, :] > 0, if_ref[c, at, :] + add, 0.0)
    inset = 2 * TILE
    vf_ref[inset : rows - inset, :] = vm_ref[...]

    def upper(ref):
        return jnp.concatenate([ref[full - 24 : full, :], ref[0 : inset + 8, :]], 0)

    def lower(ref):
        return ref[rows - inset - 8 : rows + 24, :]

    for part in (upper, lower):
        volt, drive = advance([part(if_ref.at[c]) for c in range(2)], [part(rf_ref.at[c]) for c in range(2)],
                              part(af_ref), part(bf_ref))
        if part is upper:
            vf_ref[0:inset, :] = volt[24 : 24 + inset, :cols]
        else:
            vf_ref[rows - inset : rows, :] = volt[8 : 8 + inset, :cols]
        for c in range(2):
            if part is upper:
                x = jnp.concatenate([jnp.zeros((8, lanes), F32), drive[c][: 24 + inset]], 0).astype(BF16)
                d_ref[c, frame - 2 * TILE :, :] = x[: 2 * TILE]
                d_ref[c, 0:inset, :] = x[2 * TILE :]
            else:
                d_ref[c, rows - inset : rows + TILE, :] = drive[c][8 : 8 + inset + TILE].astype(BF16)

    copies = []

    def send(src, dst):
        copies.append(pltpu.make_async_copy(src, dst, sems.at[len(copies)]))
        copies[-1].start()

    def emit(n, above):
        size = rows // 2
        at = slice(size * n, size * n + size)
        i0 = (if_ref[0, at, :] + parts[0].total(n, 32, 96))[:, :cols]
        io_ref[0, at, :] = i0
        send(io_ref.at[0, at], io_hbm.at[0, at])
        ends = jnp.where(rf_ref[1, at, :] > 0, if_ref[1, at, :] + parts[1].total(n, 32, 96), 0.0)
        i1 = ends[:, :cols]
        io_ref[1, at, :] = i1
        send(io_ref.at[1, at], io_hbm.at[1, at])
        left = pltpu.roll(ends, 1, 1)[:, :cols]
        up = jnp.where(row_of(i0.shape) == 0, above, pltpu.roll(i0, 1, 0))
        div = i0 - up + i1 - left
        vo_ref[at, :] = c_ref[at, :] * vf_ref[at, :] + e_ref[at, :] - b_ref[at, :] * div
        send(vo_ref.at[at], vo_hbm.at[at])

    parts = [Convolution(d_ref, inner_ref, tab_ref, 0, s, 16), Convolution(d_ref, inner_ref, tab_ref, 1, s, 32)]
    above = if_ref[0, full - 8 :, :] + parts[0].total(0, 24, 32)
    above = jnp.where(rf_ref[0, full - 8 :, :] > 0, above, 0.0)[7:8, :cols]
    parts[0].finish()
    emit(0, above)
    parts[1].finish()
    emit(1, io_ref[0, rows // 2 - 8 : rows // 2, :][7:8])
    for copy in copies:
        copy.wait()


def swapped(x, axis, odd):
    sizes = lax.axis_size("row"), lax.axis_size("col")
    main = ("row", "col").index(axis)
    to = {}
    for at in itertools.product(range(sizes[0]), range(sizes[1])):
        along, other = at[main], at[1 - main]
        if along >= odd and (along ^ 1 if not odd else ((along - 1) ^ 1) + 1) < sizes[main]:
            along = along ^ 1 if not odd else ((along - 1) ^ 1) + 1
        elif other ^ 1 < sizes[1 - main]:
            other = other ^ 1
        else:
            continue
        there = (along, other) if main == 0 else (other, along)
        to[at[0] * sizes[1] + at[1]] = there[0] * sizes[1] + there[1]
    return lax.ppermute(x, ("row", "col"), list(to.items()))


def near(x):
    return pltpu.with_memory_space_constraint(x, pltpu.VMEM)


def call(kernel, outs, ins, scratch=(), specs=None, limit=16, out_specs=None, aliases=None):
    return pl.pallas_call(
        kernel,
        compiler_params=pltpu.CompilerParams(vmem_limit_bytes=limit << 20),
        out_shape=outs,
        in_specs=specs or [VMEM] * len(ins),
        out_specs=out_specs or jax.tree.map(lambda _: VMEM, outs),
        scratch_shapes=scratch,
        input_output_aliases=aliases or {},
    )(*ins)


def local(voltage, currents, resistance, inverse_cap, shunt, tap, pad, waveforms, k_window):
    rows, cols = voltage.shape
    s = Sizes(rows, cols, k_window.shape[1], waveforms.shape[1])
    sds = pltpu.VMEM
    k_window = k_window.transpose(1, 0, 2)
    block = sds((rows, cols), F32)
    half = sds((s.edge, LANES), BF16)
    pair = sds((2, rows, cols), F32)
    whole = sds((rows, cols), jnp.int32)
    one, two, v_near, i_near, r_near, cap_near, shunt_near, tap_near, pad_near, k_near, w_near = call(
        functools.partial(first_kernel, s=s),
        (half, half, block, pair, pair, block, block, whole, whole, sds(k_window.shape, BF16),
         sds((2, s.waves, LANES), F32)),
        [pltpu.with_memory_space_constraint(x, pltpu.HBM)
         for x in (voltage, currents, resistance, inverse_cap, shunt, tap, pad, waveforms, k_window)],
        specs=[FAR] * 9,
        scratch=[pltpu.SMEM(waveforms.shape, F32), pltpu.SemaphoreType.DMA((9,))])
    square = pltpu.VMEM((LANES, LANES), F32)
    d, a, b, c, e, tables, borders = call(
        functools.partial(own_kernel, s=s),
        (sds((2, rows, cols), BF16), block, block, block, block, sds((2, s.pairs, 288, 2 * LANES), BF16),
         sds((2, s.span3, 192, 2 * LANES), BF16)),
        (v_near, i_near, r_near, cap_near, shunt_near, tap_near, pad_near, k_near, w_near),
        scratch=[square])
    one, two = near(swapped(one, "col", 0)), near(swapped(two, "col", 1))
    pay = sds((s.payload, cols), BF16)
    df, side, one, two = call(
        functools.partial(second_kernel, s=s),
        (sds((2, rows, s.lanes), BF16), sds((7, rows, LANES), BF16), pay, pay),
        (d, v_near, i_near, r_near, a, b, one, two))
    one, two = swapped(one, "row", 0), swapped(two, "row", 1)
    f = sds((s.fields, s.lanes), F32)
    f2 = sds((2, s.fields, s.lanes), F32)
    i_frame, r_frame, a_frame, b_frame, shifted, inner, v_inner = call(
        functools.partial(middle_kernel, s=s),
        (f2, f2, f, f, sds((2, s.group, 4 * TILE, s.lanes), BF16),
         sds((2, s.group, rows - 4 * TILE, s.lanes), BF16), sds((rows - 4 * TILE, cols), F32)),
        (df, i_near, r_near, a, b, side, tables),
        scratch=[pltpu.VMEM((2, rows, s.lanes), BF16)])
    outs = call(
        functools.partial(last_kernel, s=s),
        (jax.ShapeDtypeStruct((rows, cols), F32), jax.ShapeDtypeStruct((2, rows, cols), F32), f2, f2, f, f),
        (df, v_near, b, c, e, side, tables, borders, shifted, inner, v_inner, near(one), near(two), i_frame, r_frame, a_frame, b_frame),
        scratch=[pltpu.VMEM((2, s.frame, s.lanes), BF16), pltpu.VMEM((rows, cols), F32),
                 pltpu.VMEM((rows, cols), F32), pltpu.VMEM((2, rows, cols), F32), pltpu.SemaphoreType.DMA((6,))],
        out_specs=(FAR, FAR, VMEM, VMEM, VMEM, VMEM), aliases={13: 2, 14: 3, 15: 4, 16: 5})
    return outs[0], outs[1]


def solution(mesh):
    grid = P("row", "col")
    pair = P(None, "row", "col")

    return jax.shard_map(
        local,
        mesh=mesh,
        in_specs=(grid, pair, pair, grid, grid, grid, grid, P(), P()),
        out_specs=(grid, pair),
        check_vma=False,
    )
```

```python
import functools
import itertools

import jax
import jax.numpy as jnp
from jax import lax
from jax.experimental import pallas as pl
from jax.experimental.pallas import tpu as pltpu
from jax.sharding import PartitionSpec as P


F32 = jnp.float32
BF16 = jnp.bfloat16
LANES = 128
TILE = 16
VMEM = pl.BlockSpec(memory_space=pltpu.VMEM)
FAR = pl.BlockSpec(memory_space=pltpu.HBM)


class Sizes:
    def __init__(self, rows, cols, span, waves):
        self.rows, self.cols, self.span, self.waves = rows, cols, span, waves
        self.half = (span - 1) // 2
        self.far = 2 * self.half + 2
        self.near = self.half + 2
        self.lanes = cols + LANES
        self.frame = rows + 5 * TILE
        self.group = -(-span // 3)
        self.pairs = (self.group + 1) // 2
        self.span3 = -(-self.group // 3)
        self.quads = -(-self.group // 4)
        self.fields = rows + 3 * TILE
        self.up_d = 2 * self.half
        self.up_f = self.half
        self.tail = 2 * self.up_d + 6 * self.up_f
        self.main = self.tail + TILE
        self.payload = self.main + 3 * TILE
        self.slide = self.far + self.near
        far, near = self.far, self.near
        self.slots = (
            ((far, 0, 0), (far, far, far), (near, 2 * far, far + near),
             (near, 2 * far + near, far + 2 * near), (near, 2 * far + 2 * near, far + 3 * near)),
            ((near, 0, 0), (near, near, near), (near, 2 * near, 2 * near), (1, 3 * near, 3 * near)),
        )
        self.edge = rows + rows // 2 + TILE

    def turn(self, r):
        return (self.half - self.group - r) % self.lanes if r < self.group else 0


def lane_of(shape):
    return lax.broadcasted_iota(jnp.int32, shape, len(shape) - 1)


def row_of(shape):
    return lax.broadcasted_iota(jnp.int32, shape, 0)


def border_rows(c):
    return 64 if c == 0 else 48


def turn(k_ref, pad_ref, c, s):
    pad_ref[...] = jnp.zeros((LANES, LANES), F32)
    pad_ref[0 : s.span, 0 : s.span] = k_ref[:, c, :].astype(F32)
    return pad_ref[...].T


def main_tables(k_ref, t_ref, pad_ref, s):
    for c in range(2):
        turned = turn(k_ref, pad_ref, c, s)
        for r in range(2 * s.pairs):
            p, at = divmod(r, 2)
            for q in range(3):
                if r < s.group:
                    b = s.group * q + r
                    row = jnp.broadcast_to(turned[b : b + 1, :], (96, LANES))
                    band = pltpu.roll(row, 0, 1, stride=1, stride_axis=0).astype(BF16)
                else:
                    band = jnp.zeros((96, LANES), BF16)
                t_ref[c, p, q * 96 : (q + 1) * 96, at * LANES : (at + 1) * LANES] = band


def border_tables(t_ref, e_ref, s):
    window = 5 * TILE
    over = 2 * window - LANES
    for c in range(2):
        n = border_rows(c)
        late = 1 - c
        lane = lane_of((n, LANES))
        for g in range(s.span3):
            for q in range(3):
                def piece(at):
                    p, half = divmod(3 * g + at, 2)
                    return t_ref[c, p, 96 * q : 96 * q + n, half * LANES : (half + 1) * LANES]

                first = rolled(piece(0), (-late) % LANES).astype(F32)
                second = rolled(piece(1), window - late).astype(F32)
                third = rolled(piece(2), over - late).astype(F32)
                low = jnp.where(lane < window, first, second)
                high = jnp.where(lane < over, second, third)
                if late:
                    later = row_of(lane.shape) > 0
                    last = s.span - 2
                    low = jnp.where(later | (lane == last) | (lane == last + window), low, 0.0)
                    high = jnp.where(later | (lane == last + over), high, 0.0)
                e_ref[c, g, q * n : (q + 1) * n, :LANES] = low.astype(BF16)
                e_ref[c, g, q * n : (q + 1) * n, LANES:] = high.astype(BF16)


def quarter_tables(t_ref, e_ref, start, stop, offset, kept, s):
    n = stop - start
    lane = lane_of((n, LANES))
    half = LANES // 2
    for c in range(2):
        for g in range(s.quads):
            for q in range(3):
                pieces = []
                for at in range(4):
                    p, side = divmod(4 * g + at, 2)
                    x = t_ref[c, p, 96 * q + start : 96 * q + stop, side * LANES : (side + 1) * LANES]
                    pieces.append(rolled(x, (half * side - offset) % LANES).astype(F32))
                for h in range(2):
                    x = jnp.where(lane < half, pieces[2 * h], pieces[2 * h + 1])
                    if kept < half:
                        x = jnp.where((lane < kept) | ((lane >= half) & (lane < half + kept)), x, 0.0)
                    e_ref[c, g, q * n : (q + 1) * n, h * LANES : (h + 1) * LANES] = x.astype(BF16)


def load_of(tap, wave, s):
    total = jnp.zeros(tap.shape, F32)
    for n in range(s.waves):
        total = jnp.where(tap == n, wave(n), total)
    return total


def first_kernel(v_hbm, i_hbm, r_hbm, cap_hbm, shunt_hbm, tap_hbm, pad_hbm, wave_hbm, k_hbm,
                 one_ref, two_ref, v_ref, i_ref, r_ref, cap_ref, shunt_ref, tap_ref, pad_ref, k_ref, w_ref,
                 wave_ref, sems, *, s):
    sources = (v_hbm, r_hbm, i_hbm, wave_hbm, tap_hbm, pad_hbm, cap_hbm, shunt_hbm, k_hbm)
    targets = (v_ref, r_ref, i_ref, wave_ref, tap_ref, pad_ref, cap_ref, shunt_ref, k_ref)
    copies = [pltpu.make_async_copy(x, y, sems.at[n]) for n, (x, y) in enumerate(zip(sources, targets))]
    for copy in copies:
        copy.start()
    even = lax.rem(lax.axis_index("col"), 2) == 0
    rows, cols = s.rows, s.cols
    shape = (rows, LANES)
    lane, row = lane_of(shape), row_of(shape)

    def ends(ref):
        return jnp.where(lane < LANES // 2, ref[:, :LANES], ref[:, cols - LANES :])

    for copy in copies[:3]:
        copy.wait()
    volt = ends(v_ref)
    i0, i1, r0, r1 = ends(i_ref.at[0]), ends(i_ref.at[1]), ends(r_ref.at[0]), ends(r_ref.at[1])
    below = jnp.where(row == rows - 1, 0.0, pltpu.roll(volt, rows - 1, 0))
    beside = jnp.where(lane == LANES - 1, 0.0, pltpu.roll(volt, LANES - 1, 1))
    d0 = (volt - below) - r0 * i0
    d1 = (volt - beside) - r1 * i1
    half = rows // 2

    def put(start, left, right):
        at = slice(start, start + left.shape[0])
        one_ref[at, :] = jnp.where(even, right, left).astype(BF16)
        two_ref[at, :] = jnp.where(even, left, right).astype(BF16)

    def slotted(slots, fields):
        left = jnp.zeros(shape, F32)
        right = jnp.zeros(shape, F32)
        for (n, off, back), field in zip(slots, fields):
            x = rolled(field, off)
            left = jnp.where((lane >= off) & (lane < off + n), x, left)
            if n > 1:
                x = x if back == off else rolled(field, back)
                right = jnp.where(before(lane, n, back), x, right)
        return left, right

    put(0, *slotted(s.slots[0], (d0, d1, i0, i1, r0)))
    put(rows + half, v_ref[:TILE, :LANES], v_ref[:TILE, cols - LANES :])
    for copy in copies[3:]:
        copy.wait()
    for step in range(2):
        for n in range(s.waves):
            w_ref[step, n : n + 1, :] = jnp.full((1, LANES), wave_ref[step, n], F32)
    load = load_of(ends(tap_ref), lambda n: wave_ref[0, n], s)
    keep = ends(pad_ref) != 1
    b = jnp.where(keep, ends(cap_ref), 0.0)
    c = jnp.where(keep, 1.0, 0.0) - b * ends(shunt_ref)
    volt = ends(v_ref)
    a = b * load + c * volt
    folded = [x[:half] + pltpu.roll(x[half:], LANES // 2, 1)
              for x in slotted(s.slots[1], (ends(r_ref.at[1]), a, b, volt))]
    put(rows, *folded)


def before(lane, n, off):
    if off >= n:
        return (lane >= off - n) & (lane < off)
    return (lane < off) | (lane >= LANES + off - n)


def own_kernel(v_ref, i_ref, r_ref, cap_ref, shunt_ref, tap_ref, pad_ref, k_ref, w_ref,
               d_ref, a_ref, b_ref, c_ref, e_ref, t_ref, bor_ref, mid_ref, up_ref, down_ref, square_ref, *, s):
    main_tables(k_ref, t_ref, square_ref, s)
    border_tables(t_ref, bor_ref, s)
    quarter_tables(t_ref, mid_ref, 0, 96, 32, 64, s)
    quarter_tables(t_ref, up_ref, 16, 80, 16, 64, s)
    quarter_tables(t_ref, down_ref, 48, 96, 80, 48, s)
    volt = v_ref[...]
    rows, cols = volt.shape
    below = jnp.where(row_of(volt.shape) == rows - 1, 0.0, pltpu.roll(volt, rows - 1, 0))
    beside = jnp.where(lane_of(volt.shape) == cols - 1, 0.0, pltpu.roll(volt, cols - 1, 1))
    d_ref[0] = ((volt - below) - r_ref[0] * i_ref[0]).astype(BF16)
    d_ref[1] = ((volt - beside) - r_ref[1] * i_ref[1]).astype(BF16)
    keep = pad_ref[...] != 1
    b = jnp.where(keep, cap_ref[...], 0.0)
    c = jnp.where(keep, 1.0, 0.0) - b * shunt_ref[...]
    b_ref[...], c_ref[...] = b, c
    for at in range(0, cols, LANES):
        at = slice(at, at + LANES)
        first, second = [load_of(tap_ref[:, at], lambda n: w_ref[step, n : n + 1, :], s) for step in range(2)]
        a_ref[:, at] = c[:, at] * volt[:, at] + b[:, at] * first
        e_ref[:, at] = b[:, at] * second


def second_kernel(d_ref, v_ref, i_ref, r_ref, a_ref, b_ref, one_ref, two_ref,
                  df_ref, t_ref, up_ref, down_ref, *, s):
    even = lax.rem(lax.axis_index("col"), 2) == 0
    rows, cols = v_ref.shape
    lane = lane_of((rows, LANES))
    half = rows // 2
    index, count = lax.axis_index("col"), lax.axis_size("col")

    def get(start, size):
        at = slice(start, start + size)
        one, two = one_ref[at, :].astype(F32), two_ref[at, :].astype(F32)
        right, left = jnp.where(even, one, two), jnp.where(even, two, one)
        return jnp.where(index < count - 1, right, 0.0), jnp.where(index > 0, left, 0.0)

    sides = []
    for tile, slots in enumerate(s.slots):
        if tile == 0:
            pair = get(0, rows)
        else:
            pair = [jnp.concatenate([x, pltpu.roll(x, LANES // 2, 1)], 0) for x in get(rows, half)]
        for n, off, back in slots:
            if back == off:
                x = jnp.where((lane >= off) & (lane < off + n), pair[0], pair[1])
                x = rolled(x, (LANES - off) % LANES)
                sides.append(jnp.where((lane < n) | (lane >= LANES - n), x, 0.0))
            else:
                x, y = rolled(pair[0], LANES - off), rolled(pair[1], LANES - back)
                sides.append(jnp.where(lane < n, x, jnp.where(lane >= LANES - n, y, 0.0)))
    d0s, d1s, i0s, i1s, r0s, r1s, as_, bs, vs = sides
    x, y = get(rows + half, TILE)
    first = lane_of((TILE, LANES))
    corner = jnp.where(first < s.far, x, jnp.where(first >= LANES - s.far, y, 0.0))
    edge = lane == LANES - 1
    next_side = pltpu.roll(vs, LANES - 1, 1)
    next_own = pltpu.roll(v_ref[:, :LANES], LANES - 1, 1)
    d1 = d_ref[1]
    tail = d1[:, cols - LANES :].astype(F32)
    tail = jnp.where(edge, tail - next_side, tail).astype(BF16)
    d1s = jnp.where(edge, jnp.where(r1s > 0, d1s - next_own, 0.0), d1s).astype(BF16)
    df_ref[0, :, :cols] = d_ref[0]
    df_ref[0, :, cols:] = d0s.astype(BF16)
    df_ref[1, :, : cols - LANES] = d1[:, : cols - LANES]
    df_ref[1, :, cols - LANES : cols] = tail
    df_ref[1, :, cols:] = d1s
    for n, x in enumerate((i0s, i1s, r0s, r1s, as_, bs)):
        t_ref[n] = x.astype(BF16)
    t_ref[6, :TILE, :] = corner.astype(BF16)
    above = lax.rem(lax.axis_index("row"), 2) == 0

    own = (i_ref.at[0], i_ref.at[1], r_ref.at[0], r_ref.at[1], a_ref, b_ref)

    def rows_of(n, start, size):
        if n < 2:
            at = start // TILE * TILE
            x = df_ref[n, at : at + TILE, :].astype(F32)
            return x[start - at : start - at + size]
        source = v_ref if n == 8 else own[n - 2]
        at = start // TILE * TILE
        x = t_ref[n - 2, at : at + TILE, :].astype(F32)
        return jnp.concatenate([source[start : start + size, :], x[start - at : start - at + size]], 1)

    lane16 = lane_of((TILE, LANES))
    wide = (lane16 < s.far) | (lane16 >= LANES - s.far)

    def pack(ref, down):
        at = 0
        dstart = rows - s.up_d if down else 0
        fstart = rows - s.up_f if down else 0

        def corner(k, x):
            ref[s.main + k // 2 * TILE : s.main + (k // 2 + 1) * TILE, k % 2 * LANES : (k % 2 + 1) * LANES] = x.astype(BF16)

        def field_side(n):
            return t_ref[n, fstart : fstart + s.up_f, :].astype(F32)

        for c in range(2):
            ref[at : at + s.up_d, :] = df_ref[c, dstart : dstart + s.up_d, :cols]
            at += s.up_d
            for h in range(2):
                x = df_ref[c, dstart + h * TILE : dstart + (h + 1) * TILE, cols:].astype(F32)
                corner(2 * c + h, jnp.where(wide, x, pltpu.roll(field_side(2 * c + h), s.slide, 1)))
        for field in own:
            ref[at : at + s.up_f, :] = field[fstart : fstart + s.up_f, :].astype(BF16)
            at += s.up_f
        corner(4, jnp.where(wide, field_side(4), pltpu.roll(field_side(5), s.slide, 1)))
        eight = row_of((8, s.lanes))
        halves = [jnp.zeros((8, s.lanes), F32), jnp.zeros((8, s.lanes), F32)]
        for n in range(8):
            width = s.up_d if n < 2 else s.up_f
            slot = 2 * n % 8
            if down:
                x = pltpu.roll(rows_of(n, rows - width - 8, 8), (slot + 2) % 8, 0)
            else:
                x = pltpu.roll(rows_of(n, width, 8), slot, 0)
            keep = (eight == slot) | (eight == slot + 1)
            halves[n // 4] = jnp.where(keep, x, halves[n // 4])
        if not down:
            x = pltpu.roll(rows_of(8, 0, 8), 1, 0)
            halves[0] = jnp.where(eight == 1, x, halves[0])
        extra = jnp.concatenate(halves, 0)
        ref[at : at + TILE, :] = extra[:, :cols].astype(BF16)
        corner(5, extra[:, cols:])

    @pl.when(above)
    def _():
        pack(up_ref, True)
        pack(down_ref, False)

    @pl.when(jnp.logical_not(above))
    def _():
        pack(up_ref, False)
        pack(down_ref, True)


class Convolution:
    def __init__(self, d_ref, up_ref, down_ref, c, s):
        self.s, self.c, self.down_ref = s, c, down_ref
        self.acc = [None] * 4
        tiles = s.frame // TILE
        above = [tiles - 2, tiles - 1, 0, 1]
        last = s.rows // TILE
        below = [last - 2, last - 1, last, last]
        self.late = []
        for g in range(s.quads):
            upper, lower = [], []
            for at in range(4):
                shift = s.turn(4 * g + at)
                upper += [rolled(d_ref[c, t * TILE : (t + 1) * TILE, :], shift) for t in above]
                x = [rolled(d_ref[c, t * TILE : (t + 1) * TILE, :], shift) for t in below[:3]]
                lower += x + x[2:]
            upper, lower = jnp.concatenate(upper, 0), jnp.concatenate(lower, 0)
            lhs = up_ref[c, g]
            self.add(0, lhs, upper[:, : s.cols])
            self.add(1, lhs, upper[:, s.cols :])
            self.late.append(lower)

    def add(self, n, lhs, rhs):
        x = jnp.dot(lhs, rhs, preferred_element_type=F32)
        self.acc[n] = x if self.acc[n] is None else self.acc[n] + x

    def finish(self):
        for g, lower in enumerate(self.late):
            lhs = self.down_ref[self.c, g]
            self.add(2, lhs, lower[:, : self.s.cols])
            self.add(3, lhs, lower[:, self.s.cols :])

    def total(self, n):
        acc = [self.acc[2 * n], None, self.acc[2 * n + 1]]
        size = acc[0].shape[0] // 3
        return gather(acc, 0, size, 0, size, self.s)


def rolled(x, shift):
    return pltpu.roll(x, shift, 1) if shift else x


def gather(acc, n, high, start, stop, s):
    parts = []
    for q in range(3):
        at = slice(high * q + start, high * q + stop)
        side = acc[2][at, n * LANES : (n + 1) * LANES]
        parts.append(rolled(jnp.concatenate([acc[n][at], side], 1), (s.group - s.group * q) % s.lanes))
    return parts[0] + parts[1] + parts[2]


def middle_kernel(df_ref, i_ref, r_ref, a_ref, b_ref, side_ref, tab_ref, mid_ref,
                  if_ref, rf_ref, af_ref, bf_ref, x_ref, vm_ref, part_ref, z_ref, *, s):
    rows, cols, lanes = s.rows, s.cols, s.lanes
    own = (i_ref.at[0], i_ref.at[1], r_ref.at[0], r_ref.at[1], a_ref, b_ref)
    frames = (if_ref.at[0], if_ref.at[1], rf_ref.at[0], rf_ref.at[1], af_ref, bf_ref)
    for n, (src, dst) in enumerate(zip(own, frames)):
        dst[0:rows, :cols] = src[...]
        dst[0:rows, cols:] = side_ref[n].astype(F32)
    z_ref[...] = df_ref[...]
    end = z_ref[0, rows - TILE :, :]
    z_ref[0, rows - TILE :, :] = jnp.where(row_of(end.shape) == TILE - 1, 0.0, end.astype(F32)).astype(BF16)
    for c in range(2):
        acc = [jnp.zeros((288, cols), F32), None, jnp.zeros((288, LANES), F32)]
        for p in range(s.pairs):
            pieces = []
            for r in (2 * p, 2 * p + 1):
                if r < s.group:
                    x = rolled(z_ref[c], (s.half - s.group - r) % lanes)
                    x_ref[c, r, 0 : 2 * TILE, :] = x[0 : 2 * TILE]
                    x_ref[c, r, 2 * TILE :, :] = x[rows - 2 * TILE :]
                pieces.append(x)
            rhs = jnp.concatenate(pieces, 0)
            acc[0] = acc[0] + jnp.dot(tab_ref[c, p], rhs[:, :cols], preferred_element_type=F32)
            acc[2] = acc[2] + jnp.dot(tab_ref[c, p], rhs[:, cols:], preferred_element_type=F32)
        at = slice(s.half, rows - s.half)
        total = gather(acc, 0, 96, 0, 96, s)
        if_ref[c, at, :] = jnp.where(rf_ref[c, at, :] > 0, if_ref[c, at, :] + total, 0.0)
    at = slice(2 * TILE - 8, rows - 2 * TILE + 8)
    size = rows - 4 * TILE
    i = [if_ref[c, at, :] for c in range(2)]
    r = [rf_ref[c, at, :] for c in range(2)]
    volt, drive = advance(i, r, af_ref[at, :], bf_ref[at, :])
    vm_ref[...] = volt[8 : 8 + size, :cols]
    for c in range(2):
        x = drive[c][8 : 8 + size].astype(BF16)
        acc = [jnp.zeros((288, cols), F32), None, jnp.zeros((288, LANES), F32)]
        for g in range(s.quads):
            pieces = [rolled(x, s.turn(4 * g + at)) for at in range(4)]
            rhs = jnp.concatenate(pieces, 0)
            acc[0] = acc[0] + jnp.dot(mid_ref[c, g], rhs[:, :cols], preferred_element_type=F32)
            acc[2] = acc[2] + jnp.dot(mid_ref[c, g], rhs[:, cols:], preferred_element_type=F32)
        part_ref[c] = gather(acc, 0, 96, 0, 96, s)


def advance(i, r, a, b):
    rows, lanes = a.shape
    volt = a - b * (i[0] - pltpu.roll(i[0], 1, 0) + i[1] - pltpu.roll(i[1], 1, 1))
    drops = volt - pltpu.roll(volt, rows - 1, 0), volt - pltpu.roll(volt, lanes - 1, 1)
    return volt, [jnp.where(r[c] > 0, drops[c] - r[c] * i[c], 0.0) for c in range(2)]


def border(d_ref, x_ref, e_ref, c, s):
    n = border_rows(c)
    acc = [jnp.zeros((3 * n, 2 * LANES), F32) for _ in range(3)]
    rows, lanes, cols = s.rows, s.lanes, s.cols
    for g in range(s.span3):
        tops, bottoms = [], []
        for at in range(3):
            r = 3 * g + at
            r = r if r < s.group else 0
            shift = (s.half - s.group - r) % lanes
            outer = rolled(d_ref[c, rows : s.frame, :], shift)
            start, stop = x_ref[c, r, 0 : 2 * TILE, :], x_ref[c, r, 2 * TILE :, :]
            if c == 0:
                stop = jnp.concatenate([stop[:TILE], rolled(d_ref[c, rows - TILE : rows, :], shift)], 0)
            top = jnp.concatenate([outer[2 * TILE :], start], 0)
            bottom = jnp.concatenate([stop, outer[: 3 * TILE]], 0)
            tops.append(top)
            bottoms.append(bottom)
        tops.append(tops[0][:TILE])
        bottoms.append(bottoms[0][:TILE])
        top, bottom = jnp.concatenate(tops, 0), jnp.concatenate(bottoms, 0)
        strip = jnp.concatenate([top[:, cols:], bottom[:, cols:]], 1)
        lhs = e_ref[c, g, 0 : 3 * n, :]
        for k, rhs in enumerate((top[:, :cols], bottom[:, :cols], strip)):
            acc[k] = acc[k] + jnp.dot(lhs, rhs, preferred_element_type=F32)
    return [gather(acc, k, n, 0, n, s) for k in range(2)]


def last_kernel(df_ref, v_ref, b_ref, c_ref, e_ref, side_ref, up_ref, down_ref, bor_ref, x_ref, vm_ref, part_ref,
                one_ref, two_ref,
                if_in, rf_in, af_in, bf_in, vo_hbm, io_hbm, if_ref, rf_ref, af_ref, bf_ref,
                d_ref, vf_ref, vo_ref, io_ref, sems, *, s):
    even = lax.rem(lax.axis_index("row"), 2) == 0
    rows, cols, frame, lanes = s.rows, s.cols, s.frame, s.lanes
    index = lax.axis_index("row")
    low = jnp.where(even, one_ref[...], two_ref[...])
    high = jnp.where(even, two_ref[...], one_ref[...])
    low = jnp.where(index < lax.axis_size("row") - 1, low, jnp.zeros_like(low))
    high = jnp.where(index > 0, high, jnp.zeros_like(high))
    ud, uf, full = s.up_d, s.up_f, s.fields
    lane = lane_of((TILE, LANES))

    def corner(x, k):
        return x[s.main + k // 2 * TILE : s.main + (k // 2 + 1) * TILE, k % 2 * LANES : (k % 2 + 1) * LANES].astype(F32)

    def rest(x):
        return jnp.concatenate([x[s.tail : s.main, :].astype(F32), corner(x, 5)], 1)

    def field(x, n):
        at = 2 * ud + n * uf
        side = corner(x, min(n, 4))
        if n != 4:
            side = pltpu.roll(side, LANES - s.slide, 1)
        side = jnp.where((lane < s.near) | (lane >= LANES - s.near), side, 0.0)
        return jnp.concatenate([x[at : at + uf, :].astype(F32), side], 1)

    def driving(x, c):
        sides = [jnp.where((lane < s.far) | (lane >= LANES - s.far), corner(x, 2 * c + h), 0.0) for h in range(2)]
        return jnp.concatenate([x[c * ud : (c + 1) * ud, :], jnp.concatenate(sides, 0).astype(BF16)], 1)

    low_rest, high_rest = rest(low), rest(high)
    eight = row_of((8, lanes))
    frames = (if_ref.at[0], if_ref.at[1], rf_ref.at[0], rf_ref.at[1], af_ref, bf_ref)
    for n, dst in enumerate(frames):
        half, slot = divmod(4 + 2 * n, 8)
        extra_low = pltpu.roll(low_rest[8 * half : 8 * half + 8], (8 - slot) % 8, 0)
        extra_high = pltpu.roll(high_rest[8 * half : 8 * half + 8], 6 - slot, 0)
        dst[rows : rows + uf, :] = field(low, n)
        dst[rows + uf : rows + uf + 8, :] = jnp.where(eight == 0, extra_low, 0.0)
        dst[full - uf - 8 : full - uf, :] = jnp.where(eight >= 6, extra_high, 0.0)
        dst[full - uf : full, :] = field(high, n)
    v_next = low_rest[1:2, :]
    v_first = jnp.concatenate([v_ref[0:8, :][0:1, :], side_ref[6, 0:TILE, :].astype(F32)[0:1, :]], 1)
    gap = rows + ud
    shape = (TILE, lanes)
    for c in range(2):
        d_ref[c, rows - TILE : rows, :] = df_ref[c, rows - TILE : rows, :]
        d_ref[c, rows:gap, :] = driving(low, c)
        d_ref[c, gap + TILE :, :] = driving(high, c)
        extra_low = pltpu.roll(low_rest[0:8], (8 - 2 * c) % 8, 0)
        extra_high = pltpu.roll(high_rest[0:8], 6 - 2 * c, 0)
        d_ref[c, gap : gap + TILE, :] = jnp.concatenate(
            [jnp.where(eight == 0, extra_low, 0.0), jnp.where(eight >= 6, extra_high, 0.0)], 0).astype(BF16)
    last = row_of(shape) == TILE - 1
    x = d_ref[0, rows - TILE : rows, :].astype(F32)
    d_ref[0, rows - TILE : rows, :] = jnp.where(last, x - v_next, x).astype(BF16)
    x = d_ref[0, frame - TILE :, :].astype(F32)
    inside = rf_ref[0, full - TILE :, :] > 0
    d_ref[0, frame - TILE :, :] = jnp.where(last, jnp.where(inside, x - v_first, 0.0), x).astype(BF16)

    for c in range(2):
        top, bottom = border(d_ref, x_ref, bor_ref, c, s)
        n = border_rows(c)
        pieces = []
        if c == 0:
            pieces.append((rows - 24, jnp.where(eight == 7, jnp.broadcast_to(bottom[0:1], (8, lanes)), 0.0)))
            top, bottom = pltpu.roll(top, n - 1, 0), pltpu.roll(bottom, n - 1, 0)
        pieces += [(full - 24, top[8:32]), (0, top[32:48]), (rows - TILE, bottom[0:40])]
        for dst, add in pieces:
            at = slice(dst, dst + add.shape[0])
            if_ref[c, at, :] = jnp.where(rf_ref[c, at, :] > 0, if_ref[c, at, :] + add, 0.0)
    inset = 2 * TILE
    vf_ref[inset : rows - inset, :] = vm_ref[...]

    def upper(ref):
        return jnp.concatenate([ref[full - 24 : full, :], ref[0 : inset + 8, :]], 0)

    def lower(ref):
        return ref[rows - inset - 8 : rows + 24, :]

    for part in (upper, lower):
        volt, drive = advance([part(if_ref.at[c]) for c in range(2)], [part(rf_ref.at[c]) for c in range(2)],
                              part(af_ref), part(bf_ref))
        if part is upper:
            vf_ref[0:inset, :] = volt[24 : 24 + inset, :cols]
        else:
            vf_ref[rows - inset : rows, :] = volt[8 : 8 + inset, :cols]
        for c in range(2):
            if part is upper:
                x = jnp.concatenate([jnp.zeros((8, lanes), F32), drive[c][: 24 + inset]], 0).astype(BF16)
                d_ref[c, frame - 2 * TILE :, :] = x[: 2 * TILE]
                d_ref[c, 0:inset, :] = x[2 * TILE :]
            else:
                d_ref[c, rows - inset : rows + TILE, :] = drive[c][8 : 8 + inset + TILE].astype(BF16)

    copies = []

    def send(src, dst):
        copies.append(pltpu.make_async_copy(src, dst, sems.at[len(copies)]))
        copies[-1].start()

    def emit(n, above, adds):
        size = rows // 2
        at = slice(size * n, size * n + size)
        i0 = (if_ref[0, at, :] + adds[0])[:, :cols]
        io_ref[0, at, :] = i0
        send(io_ref.at[0, at], io_hbm.at[0, at])
        ends = jnp.where(rf_ref[1, at, :] > 0, if_ref[1, at, :] + adds[1], 0.0)
        i1 = ends[:, :cols]
        io_ref[1, at, :] = i1
        send(io_ref.at[1, at], io_hbm.at[1, at])
        left = pltpu.roll(ends, 1, 1)[:, :cols]
        up = jnp.where(row_of(i0.shape) == 0, above, pltpu.roll(i0, 1, 0))
        div = i0 - up + i1 - left
        vo_ref[at, :] = c_ref[at, :] * vf_ref[at, :] + e_ref[at, :] - b_ref[at, :] * div
        send(vo_ref.at[at], vo_hbm.at[at])

    parts = [Convolution(d_ref, up_ref, down_ref, c, s) for c in range(2)]
    tops = [part.total(0) for part in parts]
    above = if_ref[0, full - 8 :, :] + tops[0][8:16]
    above = jnp.where(rf_ref[0, full - 8 :, :] > 0, above, 0.0)[7:8, :cols]
    parts[0].finish()
    emit(0, above, [jnp.concatenate([tops[c][16:32], tops[c][32:64] + part_ref[c, 0:32, :], part_ref[c, 32:48, :]], 0)
                    for c in range(2)])
    parts[1].finish()
    ends = [part.total(1) for part in parts]
    emit(1, io_ref[0, rows // 2 - 8 : rows // 2, :][7:8],
         [jnp.concatenate([part_ref[c, 48:64, :], part_ref[c, 64:96, :] + ends[c][0:32], ends[c][32:48]], 0)
          for c in range(2)])
    for copy in copies:
        copy.wait()


def swapped(x, axis, odd):
    sizes = lax.axis_size("row"), lax.axis_size("col")
    main = ("row", "col").index(axis)
    to = {}
    for at in itertools.product(range(sizes[0]), range(sizes[1])):
        along, other = at[main], at[1 - main]
        if along >= odd and (along ^ 1 if not odd else ((along - 1) ^ 1) + 1) < sizes[main]:
            along = along ^ 1 if not odd else ((along - 1) ^ 1) + 1
        elif other ^ 1 < sizes[1 - main]:
            other = other ^ 1
        else:
            continue
        there = (along, other) if main == 0 else (other, along)
        to[at[0] * sizes[1] + at[1]] = there[0] * sizes[1] + there[1]
    return lax.ppermute(x, ("row", "col"), list(to.items()))


def near(x):
    return pltpu.with_memory_space_constraint(x, pltpu.VMEM)


def call(kernel, outs, ins, scratch=(), specs=None, limit=16, out_specs=None, aliases=None):
    return pl.pallas_call(
        kernel,
        compiler_params=pltpu.CompilerParams(vmem_limit_bytes=limit << 20),
        out_shape=outs,
        in_specs=specs or [VMEM] * len(ins),
        out_specs=out_specs or jax.tree.map(lambda _: VMEM, outs),
        scratch_shapes=scratch,
        input_output_aliases=aliases or {},
    )(*ins)


def local(voltage, currents, resistance, inverse_cap, shunt, tap, pad, waveforms, k_window):
    rows, cols = voltage.shape
    s = Sizes(rows, cols, k_window.shape[1], waveforms.shape[1])
    sds = pltpu.VMEM
    k_window = k_window.transpose(1, 0, 2)
    block = sds((rows, cols), F32)
    half = sds((s.edge, LANES), BF16)
    pair = sds((2, rows, cols), F32)
    whole = sds((rows, cols), jnp.int32)
    one, two, v_near, i_near, r_near, cap_near, shunt_near, tap_near, pad_near, k_near, w_near = call(
        functools.partial(first_kernel, s=s),
        (half, half, block, pair, pair, block, block, whole, whole, sds(k_window.shape, BF16),
         sds((2, s.waves, LANES), F32)),
        [pltpu.with_memory_space_constraint(x, pltpu.HBM)
         for x in (voltage, currents, resistance, inverse_cap, shunt, tap, pad, waveforms, k_window)],
        specs=[FAR] * 9,
        scratch=[pltpu.SMEM(waveforms.shape, F32), pltpu.SemaphoreType.DMA((9,))])
    square = pltpu.VMEM((LANES, LANES), F32)
    d, a, b, c, e, tables, borders, mids, uppers, lowers = call(
        functools.partial(own_kernel, s=s),
        (sds((2, rows, cols), BF16), block, block, block, block, sds((2, s.pairs, 288, 2 * LANES), BF16),
         sds((2, s.span3, 192, 2 * LANES), BF16), *[sds((2, s.quads, 3 * n, 2 * LANES), BF16) for n in (96, 64, 48)]),
        (v_near, i_near, r_near, cap_near, shunt_near, tap_near, pad_near, k_near, w_near),
        scratch=[square])
    one, two = near(swapped(one, "col", 0)), near(swapped(two, "col", 1))
    pay = sds((s.payload, cols), BF16)
    df, side, one, two = call(
        functools.partial(second_kernel, s=s),
        (sds((2, rows, s.lanes), BF16), sds((7, rows, LANES), BF16), pay, pay),
        (d, v_near, i_near, r_near, a, b, one, two))
    one, two = swapped(one, "row", 0), swapped(two, "row", 1)
    f = sds((s.fields, s.lanes), F32)
    f2 = sds((2, s.fields, s.lanes), F32)
    i_frame, r_frame, a_frame, b_frame, shifted, v_inner, partial = call(
        functools.partial(middle_kernel, s=s),
        (f2, f2, f, f, sds((2, s.group, 4 * TILE, s.lanes), BF16),
         sds((rows - 4 * TILE, cols), F32), sds((2, 96, s.lanes), F32)),
        (df, i_near, r_near, a, b, side, tables, mids),
        scratch=[pltpu.VMEM((2, rows, s.lanes), BF16)])
    outs = call(
        functools.partial(last_kernel, s=s),
        (jax.ShapeDtypeStruct((rows, cols), F32), jax.ShapeDtypeStruct((2, rows, cols), F32), f2, f2, f, f),
        (df, v_near, b, c, e, side, uppers, lowers, borders, shifted, v_inner, partial, near(one), near(two), i_frame, r_frame, a_frame, b_frame),
        scratch=[pltpu.VMEM((2, s.frame, s.lanes), BF16), pltpu.VMEM((rows, cols), F32),
                 pltpu.VMEM((rows, cols), F32), pltpu.VMEM((2, rows, cols), F32), pltpu.SemaphoreType.DMA((6,))],
        out_specs=(FAR, FAR, VMEM, VMEM, VMEM, VMEM), aliases={14: 2, 15: 3, 16: 4, 17: 5})
    return outs[0], outs[1]


def solution(mesh):
    grid = P("row", "col")
    pair = P(None, "row", "col")

    return jax.shard_map(
        local,
        mesh=mesh,
        in_specs=(grid, pair, pair, grid, grid, grid, grid, P(), P()),
        out_specs=(grid, pair),
        check_vma=False,
    )
```

```python
import functools
import itertools

import jax
import jax.numpy as jnp
from jax import lax
from jax.experimental import pallas as pl
from jax.experimental.pallas import tpu as pltpu
from jax.sharding import PartitionSpec as P


F32 = jnp.float32
BF16 = jnp.bfloat16
LANES = 128
TILE = 16
VMEM = pl.BlockSpec(memory_space=pltpu.VMEM)
FAR = pl.BlockSpec(memory_space=pltpu.HBM)


class Sizes:
    def __init__(self, rows, cols, span, waves):
        self.rows, self.cols, self.span, self.waves = rows, cols, span, waves
        self.half = (span - 1) // 2
        assert rows == LANES and self.half == TILE and cols % LANES == 0
        self.far = 2 * self.half + 2
        self.near = self.half + 2
        self.lanes = cols + LANES
        self.frame = rows + 5 * TILE
        self.group = -(-span // 3)
        self.pairs = (self.group + 1) // 2
        self.span3 = -(-self.group // 3)
        self.quads = -(-self.group // 4)
        self.fields = rows + 3 * TILE
        self.up_d = 2 * self.half
        self.up_f = self.half
        self.tail = 2 * self.up_d + 6 * self.up_f
        self.main = self.tail + TILE
        self.payload = self.main + 3 * TILE
        self.slide = self.far + self.near
        far, near = self.far, self.near
        self.slots = (
            ((far, 0, 0), (far, far, far), (near, 2 * far, far + near),
             (near, 2 * far + near, far + 2 * near), (near, 2 * far + 2 * near, far + 3 * near)),
            ((near, 0, 0), (near, near, near), (near, 2 * near, 2 * near), (1, 3 * near, 3 * near)),
        )
        self.edge = rows + rows // 2 + TILE

    def turn(self, r):
        return (self.half - self.group - r) % self.lanes if r < self.group else 0


def lane_of(shape):
    return lax.broadcasted_iota(jnp.int32, shape, len(shape) - 1)


def row_of(shape):
    return lax.broadcasted_iota(jnp.int32, shape, 0)


def border_rows(c):
    return 64 if c == 0 else 48


def turn(k_ref, pad_ref, c, s):
    pad_ref[...] = jnp.zeros((LANES, LANES), F32)
    pad_ref[0 : s.span, 0 : s.span] = k_ref[:, c, :].astype(F32)
    return pad_ref[...].T


def main_tables(k_ref, t_ref, pad_ref, s):
    for c in range(2):
        turned = turn(k_ref, pad_ref, c, s)
        for r in range(2 * s.pairs):
            p, at = divmod(r, 2)
            for q in range(3):
                if r < s.group:
                    b = s.group * q + r
                    row = jnp.broadcast_to(turned[b : b + 1, :], (96, LANES))
                    band = pltpu.roll(row, 0, 1, stride=1, stride_axis=0).astype(BF16)
                else:
                    band = jnp.zeros((96, LANES), BF16)
                t_ref[c, p, q * 96 : (q + 1) * 96, at * LANES : (at + 1) * LANES] = band


def border_tables(t_ref, e_ref, s):
    window = 5 * TILE
    over = 2 * window - LANES
    for c in range(2):
        n = border_rows(c)
        late = 1 - c
        lane = lane_of((n, LANES))
        for g in range(s.span3):
            for q in range(3):
                def piece(at):
                    p, half = divmod(3 * g + at, 2)
                    return t_ref[c, p, 96 * q : 96 * q + n, half * LANES : (half + 1) * LANES]

                first = rolled(piece(0), (-late) % LANES).astype(F32)
                second = rolled(piece(1), window - late).astype(F32)
                third = rolled(piece(2), over - late).astype(F32)
                low = jnp.where(lane < window, first, second)
                high = jnp.where(lane < over, second, third)
                if late:
                    later = row_of(lane.shape) > 0
                    last = s.span - 2
                    low = jnp.where(later | (lane == last) | (lane == last + window), low, 0.0)
                    high = jnp.where(later | (lane == last + over), high, 0.0)
                e_ref[c, g, q * n : (q + 1) * n, :LANES] = low.astype(BF16)
                e_ref[c, g, q * n : (q + 1) * n, LANES:] = high.astype(BF16)


def quarter_tables(t_ref, e_ref, start, stop, offset, kept, s):
    n = stop - start
    lane = lane_of((n, LANES))
    half = LANES // 2
    for c in range(2):
        for g in range(s.quads):
            for q in range(3):
                pieces = []
                for at in range(4):
                    p, side = divmod(4 * g + at, 2)
                    x = t_ref[c, p, 96 * q + start : 96 * q + stop, side * LANES : (side + 1) * LANES]
                    pieces.append(rolled(x, (half * side - offset) % LANES).astype(F32))
                for h in range(2):
                    x = jnp.where(lane < half, pieces[2 * h], pieces[2 * h + 1])
                    if kept < half:
                        x = jnp.where((lane < kept) | ((lane >= half) & (lane < half + kept)), x, 0.0)
                    e_ref[c, g, q * n : (q + 1) * n, h * LANES : (h + 1) * LANES] = x.astype(BF16)


def load_of(tap, wave, s):
    total = jnp.zeros(tap.shape, F32)
    for n in range(s.waves):
        total = jnp.where(tap == n, wave(n), total)
    return total


def first_kernel(v_hbm, i_hbm, r_hbm, cap_hbm, shunt_hbm, tap_hbm, pad_hbm, wave_hbm, k_hbm,
                 one_ref, two_ref, v_ref, i_ref, r_ref, cap_ref, shunt_ref, tap_ref, pad_ref, k_ref, w_ref,
                 wave_ref, sems, *, s):
    sources = (v_hbm, r_hbm, i_hbm, wave_hbm, tap_hbm, pad_hbm, cap_hbm, shunt_hbm, k_hbm)
    targets = (v_ref, r_ref, i_ref, wave_ref, tap_ref, pad_ref, cap_ref, shunt_ref, k_ref)
    copies = [pltpu.make_async_copy(x, y, sems.at[n]) for n, (x, y) in enumerate(zip(sources, targets))]
    for copy in copies:
        copy.start()
    even = lax.rem(lax.axis_index("col"), 2) == 0
    rows, cols = s.rows, s.cols
    shape = (rows, LANES)
    lane, row = lane_of(shape), row_of(shape)

    def ends(ref):
        return jnp.where(lane < LANES // 2, ref[:, :LANES], ref[:, cols - LANES :])

    for copy in copies[:3]:
        copy.wait()
    volt = ends(v_ref)
    i0, i1, r0, r1 = ends(i_ref.at[0]), ends(i_ref.at[1]), ends(r_ref.at[0]), ends(r_ref.at[1])
    below = jnp.where(row == rows - 1, 0.0, pltpu.roll(volt, rows - 1, 0))
    beside = jnp.where(lane == LANES - 1, 0.0, pltpu.roll(volt, LANES - 1, 1))
    d0 = (volt - below) - r0 * i0
    d1 = (volt - beside) - r1 * i1
    half = rows // 2

    def put(start, left, right):
        at = slice(start, start + left.shape[0])
        one_ref[at, :] = jnp.where(even, right, left).astype(BF16)
        two_ref[at, :] = jnp.where(even, left, right).astype(BF16)

    def slotted(slots, fields):
        left = jnp.zeros(shape, F32)
        right = jnp.zeros(shape, F32)
        for (n, off, back), field in zip(slots, fields):
            x = rolled(field, off)
            left = jnp.where((lane >= off) & (lane < off + n), x, left)
            if n > 1:
                x = x if back == off else rolled(field, back)
                right = jnp.where(before(lane, n, back), x, right)
        return left, right

    put(0, *slotted(s.slots[0], (d0, d1, i0, i1, r0)))
    put(rows + half, v_ref[:TILE, :LANES], v_ref[:TILE, cols - LANES :])
    for copy in copies[3:]:
        copy.wait()
    for step in range(2):
        for n in range(s.waves):
            w_ref[step, n : n + 1, :] = jnp.full((1, LANES), wave_ref[step, n], F32)
    load = load_of(ends(tap_ref), lambda n: wave_ref[0, n], s)
    keep = ends(pad_ref) != 1
    b = jnp.where(keep, ends(cap_ref), 0.0)
    c = jnp.where(keep, 1.0, 0.0) - b * ends(shunt_ref)
    volt = ends(v_ref)
    a = b * load + c * volt
    folded = [x[:half] + pltpu.roll(x[half:], LANES // 2, 1)
              for x in slotted(s.slots[1], (ends(r_ref.at[1]), a, b, volt))]
    put(rows, *folded)


def before(lane, n, off):
    if off >= n:
        return (lane >= off - n) & (lane < off)
    return (lane < off) | (lane >= LANES + off - n)


def own_kernel(v_ref, i_ref, r_ref, cap_ref, shunt_ref, tap_ref, pad_ref, k_ref, w_ref,
               d_ref, a_ref, b_ref, c_ref, e_ref, t_ref, bor_ref, mid_ref, up_ref, down_ref, square_ref, *, s):
    main_tables(k_ref, t_ref, square_ref, s)
    border_tables(t_ref, bor_ref, s)
    quarter_tables(t_ref, mid_ref, 0, 96, 32, 64, s)
    quarter_tables(t_ref, up_ref, 16, 80, 16, 64, s)
    quarter_tables(t_ref, down_ref, 48, 96, 80, 48, s)
    volt = v_ref[...]
    rows, cols = volt.shape
    below = jnp.where(row_of(volt.shape) == rows - 1, 0.0, pltpu.roll(volt, rows - 1, 0))
    beside = jnp.where(lane_of(volt.shape) == cols - 1, 0.0, pltpu.roll(volt, cols - 1, 1))
    d_ref[0] = ((volt - below) - r_ref[0] * i_ref[0]).astype(BF16)
    d_ref[1] = ((volt - beside) - r_ref[1] * i_ref[1]).astype(BF16)
    keep = pad_ref[...] != 1
    b = jnp.where(keep, cap_ref[...], 0.0)
    c = jnp.where(keep, 1.0, 0.0) - b * shunt_ref[...]
    b_ref[...], c_ref[...] = b, c
    for at in range(0, cols, LANES):
        at = slice(at, at + LANES)
        first, second = [load_of(tap_ref[:, at], lambda n: w_ref[step, n : n + 1, :], s) for step in range(2)]
        a_ref[:, at] = c[:, at] * volt[:, at] + b[:, at] * first
        e_ref[:, at] = b[:, at] * second


def second_kernel(d_ref, v_ref, i_ref, r_ref, a_ref, b_ref, one_ref, two_ref,
                  df_ref, t_ref, up_ref, down_ref, *, s):
    even = lax.rem(lax.axis_index("col"), 2) == 0
    rows, cols = v_ref.shape
    lane = lane_of((rows, LANES))
    half = rows // 2
    index, count = lax.axis_index("col"), lax.axis_size("col")

    def get(start, size):
        at = slice(start, start + size)
        one, two = one_ref[at, :].astype(F32), two_ref[at, :].astype(F32)
        right, left = jnp.where(even, one, two), jnp.where(even, two, one)
        return jnp.where(index < count - 1, right, 0.0), jnp.where(index > 0, left, 0.0)

    sides = []
    for tile, slots in enumerate(s.slots):
        if tile == 0:
            pair = get(0, rows)
        else:
            pair = [jnp.concatenate([x, pltpu.roll(x, LANES // 2, 1)], 0) for x in get(rows, half)]
        for n, off, back in slots:
            if back == off:
                x = jnp.where((lane >= off) & (lane < off + n), pair[0], pair[1])
                x = rolled(x, (LANES - off) % LANES)
                sides.append(jnp.where((lane < n) | (lane >= LANES - n), x, 0.0))
            else:
                x, y = rolled(pair[0], LANES - off), rolled(pair[1], LANES - back)
                sides.append(jnp.where(lane < n, x, jnp.where(lane >= LANES - n, y, 0.0)))
    d0s, d1s, i0s, i1s, r0s, r1s, as_, bs, vs = sides
    x, y = get(rows + half, TILE)
    first = lane_of((TILE, LANES))
    corner = jnp.where(first < s.far, x, jnp.where(first >= LANES - s.far, y, 0.0))
    edge = lane == LANES - 1
    next_side = pltpu.roll(vs, LANES - 1, 1)
    next_own = pltpu.roll(v_ref[:, :LANES], LANES - 1, 1)
    d1 = d_ref[1]
    tail = d1[:, cols - LANES :].astype(F32)
    tail = jnp.where(edge, tail - next_side, tail).astype(BF16)
    d1s = jnp.where(edge, jnp.where(r1s > 0, d1s - next_own, 0.0), d1s).astype(BF16)
    df_ref[0, :, :cols] = d_ref[0]
    df_ref[0, :, cols:] = d0s.astype(BF16)
    df_ref[1, :, : cols - LANES] = d1[:, : cols - LANES]
    df_ref[1, :, cols - LANES : cols] = tail
    df_ref[1, :, cols:] = d1s
    for n, x in enumerate((i0s, i1s, r0s, r1s, as_, bs)):
        t_ref[n] = x.astype(BF16)
    t_ref[6, :TILE, :] = corner.astype(BF16)
    above = lax.rem(lax.axis_index("row"), 2) == 0

    own = (i_ref.at[0], i_ref.at[1], r_ref.at[0], r_ref.at[1], a_ref, b_ref)

    def rows_of(n, start, size):
        if n < 2:
            at = start // TILE * TILE
            x = df_ref[n, at : at + TILE, :].astype(F32)
            return x[start - at : start - at + size]
        source = v_ref if n == 8 else own[n - 2]
        at = start // TILE * TILE
        x = t_ref[n - 2, at : at + TILE, :].astype(F32)
        return jnp.concatenate([source[start : start + size, :], x[start - at : start - at + size]], 1)

    lane16 = lane_of((TILE, LANES))
    wide = (lane16 < s.far) | (lane16 >= LANES - s.far)

    def pack(ref, down):
        at = 0
        dstart = rows - s.up_d if down else 0
        fstart = rows - s.up_f if down else 0

        def corner(k, x):
            ref[s.main + k // 2 * TILE : s.main + (k // 2 + 1) * TILE, k % 2 * LANES : (k % 2 + 1) * LANES] = x.astype(BF16)

        def field_side(n):
            return t_ref[n, fstart : fstart + s.up_f, :].astype(F32)

        for c in range(2):
            ref[at : at + s.up_d, :] = df_ref[c, dstart : dstart + s.up_d, :cols]
            at += s.up_d
            for h in range(2):
                x = df_ref[c, dstart + h * TILE : dstart + (h + 1) * TILE, cols:].astype(F32)
                corner(2 * c + h, jnp.where(wide, x, pltpu.roll(field_side(2 * c + h), s.slide, 1)))
        for field in own:
            ref[at : at + s.up_f, :] = field[fstart : fstart + s.up_f, :].astype(BF16)
            at += s.up_f
        corner(4, jnp.where(wide, field_side(4), pltpu.roll(field_side(5), s.slide, 1)))
        eight = row_of((8, s.lanes))
        halves = [jnp.zeros((8, s.lanes), F32), jnp.zeros((8, s.lanes), F32)]
        for n in range(8):
            width = s.up_d if n < 2 else s.up_f
            slot = 2 * n % 8
            if down:
                x = pltpu.roll(rows_of(n, rows - width - 8, 8), (slot + 2) % 8, 0)
            else:
                x = pltpu.roll(rows_of(n, width, 8), slot, 0)
            keep = (eight == slot) | (eight == slot + 1)
            halves[n // 4] = jnp.where(keep, x, halves[n // 4])
        if not down:
            x = pltpu.roll(rows_of(8, 0, 8), 1, 0)
            halves[0] = jnp.where(eight == 1, x, halves[0])
        extra = jnp.concatenate(halves, 0)
        ref[at : at + TILE, :] = extra[:, :cols].astype(BF16)
        corner(5, extra[:, cols:])

    @pl.when(above)
    def _():
        pack(up_ref, True)
        pack(down_ref, False)

    @pl.when(jnp.logical_not(above))
    def _():
        pack(up_ref, False)
        pack(down_ref, True)


class Convolution:
    def __init__(self, d_ref, up_ref, down_ref, c, s):
        self.s, self.c, self.down_ref = s, c, down_ref
        self.acc = [None] * 4
        tiles = s.frame // TILE
        above = [tiles - 2, tiles - 1, 0, 1]
        last = s.rows // TILE
        below = [last - 2, last - 1, last, last]
        self.late = []
        for g in range(s.quads):
            upper, lower = [], []
            for at in range(4):
                shift = s.turn(4 * g + at)
                upper += [rolled(d_ref[c, t * TILE : (t + 1) * TILE, :], shift) for t in above]
                x = [rolled(d_ref[c, t * TILE : (t + 1) * TILE, :], shift) for t in below[:3]]
                lower += x + x[2:]
            upper, lower = jnp.concatenate(upper, 0), jnp.concatenate(lower, 0)
            lhs = up_ref[c, g]
            self.add(0, lhs, upper[:, : s.cols])
            self.add(1, lhs, upper[:, s.cols :])
            self.late.append(lower)

    def add(self, n, lhs, rhs):
        x = jnp.dot(lhs, rhs, preferred_element_type=F32)
        self.acc[n] = x if self.acc[n] is None else self.acc[n] + x

    def finish(self):
        for g, lower in enumerate(self.late):
            lhs = self.down_ref[self.c, g]
            self.add(2, lhs, lower[:, : self.s.cols])
            self.add(3, lhs, lower[:, self.s.cols :])

    def total(self, n):
        acc = [self.acc[2 * n], None, self.acc[2 * n + 1]]
        size = acc[0].shape[0] // 3
        return gather(acc, 0, size, 0, size, self.s)


def rolled(x, shift):
    return pltpu.roll(x, shift, 1) if shift else x


def gather(acc, n, high, start, stop, s):
    parts = []
    for q in range(3):
        at = slice(high * q + start, high * q + stop)
        side = acc[2][at, n * LANES : (n + 1) * LANES]
        parts.append(rolled(jnp.concatenate([acc[n][at], side], 1), (s.group - s.group * q) % s.lanes))
    return parts[0] + parts[1] + parts[2]


def middle_kernel(df_ref, i_ref, r_ref, a_ref, b_ref, side_ref, tab_ref, mid_ref,
                  if_ref, rf_ref, af_ref, bf_ref, x_ref, vm_ref, part_ref, z_ref, *, s):
    rows, cols, lanes = s.rows, s.cols, s.lanes
    own = (i_ref.at[0], i_ref.at[1], r_ref.at[0], r_ref.at[1], a_ref, b_ref)
    frames = (if_ref.at[0], if_ref.at[1], rf_ref.at[0], rf_ref.at[1], af_ref, bf_ref)
    for n, (src, dst) in enumerate(zip(own, frames)):
        dst[0:rows, :cols] = src[...]
        dst[0:rows, cols:] = side_ref[n].astype(F32)
    z_ref[...] = df_ref[...]
    end = z_ref[0, rows - TILE :, :]
    z_ref[0, rows - TILE :, :] = jnp.where(row_of(end.shape) == TILE - 1, 0.0, end.astype(F32)).astype(BF16)
    for c in range(2):
        acc = [jnp.zeros((288, cols), F32), None, jnp.zeros((288, LANES), F32)]
        for p in range(s.pairs):
            pieces = []
            for r in (2 * p, 2 * p + 1):
                if r < s.group:
                    x = rolled(z_ref[c], (s.half - s.group - r) % lanes)
                    x_ref[c, r, 0 : 2 * TILE, :] = x[0 : 2 * TILE]
                    x_ref[c, r, 2 * TILE :, :] = x[rows - 2 * TILE :]
                pieces.append(x)
            rhs = jnp.concatenate(pieces, 0)
            acc[0] = acc[0] + jnp.dot(tab_ref[c, p], rhs[:, :cols], preferred_element_type=F32)
            acc[2] = acc[2] + jnp.dot(tab_ref[c, p], rhs[:, cols:], preferred_element_type=F32)
        at = slice(s.half, rows - s.half)
        total = gather(acc, 0, 96, 0, 96, s)
        if_ref[c, at, :] = jnp.where(rf_ref[c, at, :] > 0, if_ref[c, at, :] + total, 0.0)
    at = slice(2 * TILE - 8, rows - 2 * TILE + 8)
    size = rows - 4 * TILE
    i = [if_ref[c, at, :] for c in range(2)]
    r = [rf_ref[c, at, :] for c in range(2)]
    volt, drive = advance(i, r, af_ref[at, :], bf_ref[at, :])
    vm_ref[...] = volt[8 : 8 + size, :cols]
    for c in range(2):
        x = drive[c][8 : 8 + size].astype(BF16)
        acc = [jnp.zeros((288, cols), F32), None, jnp.zeros((288, LANES), F32)]
        for g in range(s.quads):
            pieces = [rolled(x, s.turn(4 * g + at)) for at in range(4)]
            rhs = jnp.concatenate(pieces, 0)
            acc[0] = acc[0] + jnp.dot(mid_ref[c, g], rhs[:, :cols], preferred_element_type=F32)
            acc[2] = acc[2] + jnp.dot(mid_ref[c, g], rhs[:, cols:], preferred_element_type=F32)
        part_ref[c] = gather(acc, 0, 96, 0, 96, s)


def advance(i, r, a, b):
    rows, lanes = a.shape
    volt = a - b * (i[0] - pltpu.roll(i[0], 1, 0) + i[1] - pltpu.roll(i[1], 1, 1))
    drops = volt - pltpu.roll(volt, rows - 1, 0), volt - pltpu.roll(volt, lanes - 1, 1)
    return volt, [jnp.where(r[c] > 0, drops[c] - r[c] * i[c], 0.0) for c in range(2)]


def border(d_ref, x_ref, e_ref, c, s):
    n = border_rows(c)
    acc = [jnp.zeros((3 * n, 2 * LANES), F32) for _ in range(3)]
    rows, lanes, cols = s.rows, s.lanes, s.cols
    for g in range(s.span3):
        tops, bottoms = [], []
        for at in range(3):
            r = 3 * g + at
            r = r if r < s.group else 0
            shift = (s.half - s.group - r) % lanes
            outer = rolled(d_ref[c, rows : s.frame, :], shift)
            start, stop = x_ref[c, r, 0 : 2 * TILE, :], x_ref[c, r, 2 * TILE :, :]
            if c == 0:
                stop = jnp.concatenate([stop[:TILE], rolled(d_ref[c, rows - TILE : rows, :], shift)], 0)
            top = jnp.concatenate([outer[2 * TILE :], start], 0)
            bottom = jnp.concatenate([stop, outer[: 3 * TILE]], 0)
            tops.append(top)
            bottoms.append(bottom)
        tops.append(tops[0][:TILE])
        bottoms.append(bottoms[0][:TILE])
        top, bottom = jnp.concatenate(tops, 0), jnp.concatenate(bottoms, 0)
        strip = jnp.concatenate([top[:, cols:], bottom[:, cols:]], 1)
        lhs = e_ref[c, g, 0 : 3 * n, :]
        for k, rhs in enumerate((top[:, :cols], bottom[:, :cols], strip)):
            acc[k] = acc[k] + jnp.dot(lhs, rhs, preferred_element_type=F32)
    return [gather(acc, k, n, 0, n, s) for k in range(2)]


def last_kernel(df_ref, v_ref, b_ref, c_ref, e_ref, side_ref, up_ref, down_ref, bor_ref, x_ref, vm_ref, part_ref,
                one_ref, two_ref,
                if_in, rf_in, af_in, bf_in, vo_hbm, io_hbm, if_ref, rf_ref, af_ref, bf_ref,
                d_ref, vf_ref, vo_ref, io_ref, sems, *, s):
    even = lax.rem(lax.axis_index("row"), 2) == 0
    rows, cols, frame, lanes = s.rows, s.cols, s.frame, s.lanes
    index = lax.axis_index("row")
    low = jnp.where(even, one_ref[...], two_ref[...])
    high = jnp.where(even, two_ref[...], one_ref[...])
    low = jnp.where(index < lax.axis_size("row") - 1, low, jnp.zeros_like(low))
    high = jnp.where(index > 0, high, jnp.zeros_like(high))
    ud, uf, full = s.up_d, s.up_f, s.fields
    lane = lane_of((TILE, LANES))

    def corner(x, k):
        return x[s.main + k // 2 * TILE : s.main + (k // 2 + 1) * TILE, k % 2 * LANES : (k % 2 + 1) * LANES].astype(F32)

    def rest(x):
        return jnp.concatenate([x[s.tail : s.main, :].astype(F32), corner(x, 5)], 1)

    def field(x, n):
        at = 2 * ud + n * uf
        side = corner(x, min(n, 4))
        if n != 4:
            side = pltpu.roll(side, LANES - s.slide, 1)
        side = jnp.where((lane < s.near) | (lane >= LANES - s.near), side, 0.0)
        return jnp.concatenate([x[at : at + uf, :].astype(F32), side], 1)

    def driving(x, c):
        sides = [jnp.where((lane < s.far) | (lane >= LANES - s.far), corner(x, 2 * c + h), 0.0) for h in range(2)]
        return jnp.concatenate([x[c * ud : (c + 1) * ud, :], jnp.concatenate(sides, 0).astype(BF16)], 1)

    low_rest, high_rest = rest(low), rest(high)
    eight = row_of((8, lanes))
    frames = (if_ref.at[0], if_ref.at[1], rf_ref.at[0], rf_ref.at[1], af_ref, bf_ref)
    for n, dst in enumerate(frames):
        half, slot = divmod(4 + 2 * n, 8)
        extra_low = pltpu.roll(low_rest[8 * half : 8 * half + 8], (8 - slot) % 8, 0)
        extra_high = pltpu.roll(high_rest[8 * half : 8 * half + 8], 6 - slot, 0)
        dst[rows : rows + uf, :] = field(low, n)
        dst[rows + uf : rows + uf + 8, :] = jnp.where(eight == 0, extra_low, 0.0)
        dst[full - uf - 8 : full - uf, :] = jnp.where(eight >= 6, extra_high, 0.0)
        dst[full - uf : full, :] = field(high, n)
    v_next = low_rest[1:2, :]
    v_first = jnp.concatenate([v_ref[0:8, :][0:1, :], side_ref[6, 0:TILE, :].astype(F32)[0:1, :]], 1)
    gap = rows + ud
    shape = (TILE, lanes)
    for c in range(2):
        d_ref[c, rows - TILE : rows, :] = df_ref[c, rows - TILE : rows, :]
        d_ref[c, rows:gap, :] = driving(low, c)
        d_ref[c, gap + TILE :, :] = driving(high, c)
        extra_low = pltpu.roll(low_rest[0:8], (8 - 2 * c) % 8, 0)
        extra_high = pltpu.roll(high_rest[0:8], 6 - 2 * c, 0)
        d_ref[c, gap : gap + TILE, :] = jnp.concatenate(
            [jnp.where(eight == 0, extra_low, 0.0), jnp.where(eight >= 6, extra_high, 0.0)], 0).astype(BF16)
    last = row_of(shape) == TILE - 1
    x = d_ref[0, rows - TILE : rows, :].astype(F32)
    d_ref[0, rows - TILE : rows, :] = jnp.where(last, x - v_next, x).astype(BF16)
    x = d_ref[0, frame - TILE :, :].astype(F32)
    inside = rf_ref[0, full - TILE :, :] > 0
    d_ref[0, frame - TILE :, :] = jnp.where(last, jnp.where(inside, x - v_first, 0.0), x).astype(BF16)

    for c in range(2):
        top, bottom = border(d_ref, x_ref, bor_ref, c, s)
        n = border_rows(c)
        pieces = []
        if c == 0:
            pieces.append((rows - 24, jnp.where(eight == 7, jnp.broadcast_to(bottom[0:1], (8, lanes)), 0.0)))
            top, bottom = pltpu.roll(top, n - 1, 0), pltpu.roll(bottom, n - 1, 0)
        pieces += [(full - 24, top[8:32]), (0, top[32:48]), (rows - TILE, bottom[0:40])]
        for dst, add in pieces:
            at = slice(dst, dst + add.shape[0])
            if_ref[c, at, :] = jnp.where(rf_ref[c, at, :] > 0, if_ref[c, at, :] + add, 0.0)
    inset = 2 * TILE
    vf_ref[inset : rows - inset, :] = vm_ref[...]

    def upper(ref):
        return jnp.concatenate([ref[full - 24 : full, :], ref[0 : inset + 8, :]], 0)

    def lower(ref):
        return ref[rows - inset - 8 : rows + 24, :]

    for part in (upper, lower):
        volt, drive = advance([part(if_ref.at[c]) for c in range(2)], [part(rf_ref.at[c]) for c in range(2)],
                              part(af_ref), part(bf_ref))
        if part is upper:
            vf_ref[0:inset, :] = volt[24 : 24 + inset, :cols]
        else:
            vf_ref[rows - inset : rows, :] = volt[8 : 8 + inset, :cols]
        for c in range(2):
            if part is upper:
                x = jnp.concatenate([jnp.zeros((8, lanes), F32), drive[c][: 24 + inset]], 0).astype(BF16)
                d_ref[c, frame - 2 * TILE :, :] = x[: 2 * TILE]
                d_ref[c, 0:inset, :] = x[2 * TILE :]
            else:
                d_ref[c, rows - inset : rows + TILE, :] = drive[c][8 : 8 + inset + TILE].astype(BF16)

    copies = []

    def send(src, dst):
        copies.append(pltpu.make_async_copy(src, dst, sems.at[len(copies)]))
        copies[-1].start()

    def emit(n, above, adds):
        size = rows // 2
        at = slice(size * n, size * n + size)
        i0 = (if_ref[0, at, :] + adds[0])[:, :cols]
        io_ref[0, at, :] = i0
        send(io_ref.at[0, at], io_hbm.at[0, at])
        ends = jnp.where(rf_ref[1, at, :] > 0, if_ref[1, at, :] + adds[1], 0.0)
        i1 = ends[:, :cols]
        io_ref[1, at, :] = i1
        send(io_ref.at[1, at], io_hbm.at[1, at])
        left = pltpu.roll(ends, 1, 1)[:, :cols]
        up = jnp.where(row_of(i0.shape) == 0, above, pltpu.roll(i0, 1, 0))
        div = i0 - up + i1 - left
        vo_ref[at, :] = c_ref[at, :] * vf_ref[at, :] + e_ref[at, :] - b_ref[at, :] * div
        send(vo_ref.at[at], vo_hbm.at[at])

    parts = [Convolution(d_ref, up_ref, down_ref, c, s) for c in range(2)]
    tops = [part.total(0) for part in parts]
    above = if_ref[0, full - 8 :, :] + tops[0][8:16]
    above = jnp.where(rf_ref[0, full - 8 :, :] > 0, above, 0.0)[7:8, :cols]
    parts[0].finish()
    emit(0, above, [jnp.concatenate([tops[c][16:32], tops[c][32:64] + part_ref[c, 0:32, :], part_ref[c, 32:48, :]], 0)
                    for c in range(2)])
    parts[1].finish()
    ends = [part.total(1) for part in parts]
    emit(1, io_ref[0, rows // 2 - 8 : rows // 2, :][7:8],
         [jnp.concatenate([part_ref[c, 48:64, :], part_ref[c, 64:96, :] + ends[c][0:32], ends[c][32:48]], 0)
          for c in range(2)])
    for copy in copies:
        copy.wait()


def swapped(x, axis, odd):
    sizes = lax.axis_size("row"), lax.axis_size("col")
    main = ("row", "col").index(axis)
    to = {}
    for at in itertools.product(range(sizes[0]), range(sizes[1])):
        along, other = at[main], at[1 - main]
        if along >= odd and (along ^ 1 if not odd else ((along - 1) ^ 1) + 1) < sizes[main]:
            along = along ^ 1 if not odd else ((along - 1) ^ 1) + 1
        elif main == 0 and other ^ 2 < sizes[1]:
            other = other ^ 2
        elif main == 1 and other ^ 1 < sizes[0]:
            other = other ^ 1
        else:
            continue
        there = (along, other) if main == 0 else (other, along)
        to[at[0] * sizes[1] + at[1]] = there[0] * sizes[1] + there[1]
    return lax.ppermute(x, ("row", "col"), list(to.items()))


def near(x):
    return pltpu.with_memory_space_constraint(x, pltpu.VMEM)


def call(kernel, outs, ins, scratch=(), specs=None, limit=16, out_specs=None, aliases=None):
    return pl.pallas_call(
        kernel,
        compiler_params=pltpu.CompilerParams(vmem_limit_bytes=limit << 20),
        out_shape=outs,
        in_specs=specs or [VMEM] * len(ins),
        out_specs=out_specs or jax.tree.map(lambda _: VMEM, outs),
        scratch_shapes=scratch,
        input_output_aliases=aliases or {},
    )(*ins)


def local(voltage, currents, resistance, inverse_cap, shunt, tap, pad, waveforms, k_window):
    rows, cols = voltage.shape
    s = Sizes(rows, cols, k_window.shape[1], waveforms.shape[1])
    sds = pltpu.VMEM
    k_window = k_window.transpose(1, 0, 2)
    block = sds((rows, cols), F32)
    half = sds((s.edge, LANES), BF16)
    pair = sds((2, rows, cols), F32)
    whole = sds((rows, cols), jnp.int32)
    one, two, v_near, i_near, r_near, cap_near, shunt_near, tap_near, pad_near, k_near, w_near = call(
        functools.partial(first_kernel, s=s),
        (half, half, block, pair, pair, block, block, whole, whole, sds(k_window.shape, BF16),
         sds((2, s.waves, LANES), F32)),
        [pltpu.with_memory_space_constraint(x, pltpu.HBM)
         for x in (voltage, currents, resistance, inverse_cap, shunt, tap, pad, waveforms, k_window)],
        specs=[FAR] * 9,
        scratch=[pltpu.SMEM(waveforms.shape, F32), pltpu.SemaphoreType.DMA((9,))])
    square = pltpu.VMEM((LANES, LANES), F32)
    d, a, b, c, e, tables, borders, mids, uppers, lowers = call(
        functools.partial(own_kernel, s=s),
        (sds((2, rows, cols), BF16), block, block, block, block, sds((2, s.pairs, 288, 2 * LANES), BF16),
         sds((2, s.span3, 192, 2 * LANES), BF16), *[sds((2, s.quads, 3 * n, 2 * LANES), BF16) for n in (96, 64, 48)]),
        (v_near, i_near, r_near, cap_near, shunt_near, tap_near, pad_near, k_near, w_near),
        scratch=[square])
    one, two = near(swapped(one, "col", 0)), near(swapped(two, "col", 1))
    pay = sds((s.payload, cols), BF16)
    df, side, one, two = call(
        functools.partial(second_kernel, s=s),
        (sds((2, rows, s.lanes), BF16), sds((7, rows, LANES), BF16), pay, pay),
        (d, v_near, i_near, r_near, a, b, one, two))
    one, two = swapped(one, "row", 0), swapped(two, "row", 1)
    f = sds((s.fields, s.lanes), F32)
    f2 = sds((2, s.fields, s.lanes), F32)
    i_frame, r_frame, a_frame, b_frame, shifted, v_inner, partial = call(
        functools.partial(middle_kernel, s=s),
        (f2, f2, f, f, sds((2, s.group, 4 * TILE, s.lanes), BF16),
         sds((rows - 4 * TILE, cols), F32), sds((2, 96, s.lanes), F32)),
        (df, i_near, r_near, a, b, side, tables, mids),
        scratch=[pltpu.VMEM((2, rows, s.lanes), BF16)])
    outs = call(
        functools.partial(last_kernel, s=s),
        (jax.ShapeDtypeStruct((rows, cols), F32), jax.ShapeDtypeStruct((2, rows, cols), F32), f2, f2, f, f),
        (df, v_near, b, c, e, side, uppers, lowers, borders, shifted, v_inner, partial, near(one), near(two), i_frame, r_frame, a_frame, b_frame),
        scratch=[pltpu.VMEM((2, s.frame, s.lanes), BF16), pltpu.VMEM((rows, cols), F32),
                 pltpu.VMEM((rows, cols), F32), pltpu.VMEM((2, rows, cols), F32), pltpu.SemaphoreType.DMA((6,))],
        out_specs=(FAR, FAR, VMEM, VMEM, VMEM, VMEM), aliases={14: 2, 15: 3, 16: 4, 17: 5})
    return outs[0], outs[1]


def solution(mesh):
    grid = P("row", "col")
    pair = P(None, "row", "col")

    return jax.shard_map(
        local,
        mesh=mesh,
        in_specs=(grid, pair, pair, grid, grid, grid, grid, P(), P()),
        out_specs=(grid, pair),
        check_vma=False,
    )
```
